128 devices in a mesh: ga: 32 (over z, y, core), ba: 4 (over x).
Axes of the slice: x: 4, y: 4, z: 4, core: 2. Of those that a mesh axis runs over, the one named last changes fastest.
Arguments:
- coefficients: bfloat16 [40960, 6144], P('ga', 'ba')
- rotation: bfloat16 [6144, 6144], P('ga', 'ba'), may hold values from -0.078125 to 0.078125
Outputs:
- new_coefficients: bfloat16 [40960, 6144], P('ga', 'ba')
- band_rms: float32 [6144], P('ba')
The draws below stay inside these ranges and needn't reach their ends.
All inputs are finite; a program needn't handle non-finite values.
Results may differ from the reference program's by a relative error of at most 0.0004.
Values may be sent and summed in bfloat16 or wider, within the bound.
A program may use at most 128 MiB of HBM per device.

```python
import math
import jax
import jax.numpy as jnp
from jax import lax

NB = 6144
NG = 40960


def draw_coefficients(key, part):
    first, second, third = jax.random.split(jax.random.fold_in(key, 11), 3)
    positions = jnp.arange(NG, dtype=jnp.float32)[:, None]
    row_scale = jnp.exp(positions / NG * math.log(3.0)) * jnp.exp(jax.random.uniform(first, (NG, 1), jnp.float32) * math.log(3.3))
    col_scale = jnp.exp(jax.random.uniform(second, (1, NB), jnp.float32) * math.log(10.0))
    base = jnp.clip(jax.random.normal(third, (NG, NB), jnp.float32), -6.0, 6.0)
    return (base * row_scale * col_scale).astype(jnp.bfloat16)


def steps_of(own_key, shape, shards, least, largest):
    loudness = 1.0
    for axis_at, parts in shards:
        heights = jax.random.uniform(jax.random.fold_in(jax.random.fold_in(own_key, 6), axis_at), (parts,), jnp.float32, least / len(shards), largest / len(shards))
        loudness = loudness * jnp.repeat(jnp.exp(heights), shape[axis_at] // parts).reshape((-1,) + (1,) * (len(shape) - 1 - axis_at))
    return loudness


def normal_values(own_key, shape, deviation, limit, shards=(), kind=jnp.bfloat16):
    drawn = jax.random.normal(own_key, shape, jnp.float32) * deviation
    if len(shards) > 0:
        drawn = steps_of(own_key, shape, shards, -0.22, 0.18) * drawn
    return jnp.clip(drawn, min=-limit, max=limit).astype(kind)


def setup_inputs(seed: int = 0) -> dict:
    seeds = jax.random.split(jax.random.key(seed), 3)
    coefficients = draw_coefficients(jax.random.fold_in(seeds[2], 71), 0)
    rotation = normal_values(seeds[1], (NB, NB), NB ** -0.5, 0.078125, ((0, 32), (1, 4)))
    return {"coefficients": coefficients, "rotation": rotation}


def reference(coefficients, rotation):
    rotated = jnp.dot(coefficients, rotation, preferred_element_type=jnp.float32)
    sums = lax.optimization_barrier(jnp.sum(rotated * rotated, axis=0))
    band_rms = jnp.sqrt(sums / NG + 1e-06)
    return ((rotated / band_rms).astype(jnp.bfloat16), band_rms)
```

```python
import functools

import jax
import jax.numpy as jnp
from jax import lax
from jax.experimental import pallas as pl
from jax.experimental.pallas import tpu as pltpu
from jax.sharding import PartitionSpec as P

MESH = pl.DeviceIdType.MESH
SIDE = 4
CHUNKS = 8
TILE_M = 320
TILE_N = 512
TOTAL_ROWS = 40960


def kernel(
    coef, rot, out, rms_out, a_buf, r_buf, c_buf, sq_sum, sq_buf,
    load_sem, a_send, a_recv, r_send, r_recv, p_send, p_recv, s_send, s_recv, out_sem,
):
    rows, depth = coef.shape
    piece, cols = rot.shape
    peers = 2 * SIDE * SIDE
    chunk = rows // CHUNKS
    half_chunk = chunk // 2
    half = piece // 2
    quarter = half // 2

    g = lax.axis_index("ga")
    x = lax.axis_index("ba")
    core = g % 2
    y = (g // 2) % SIDE
    z = g // (2 * SIDE)
    sends = []

    def shift(value, by):
        return (value + by + SIDE) % SIDE

    def a_rows(block, start, size):
        return a_buf.at[block, pl.ds(start, size), :]

    def r_rows(zz, yy, cc, start, size):
        return r_buf.at[zz, pl.ds(pl.multiple_of((yy * 2 + cc) * piece + start, 16), size), :]

    own_rot = pltpu.make_async_copy(rot, r_rows(z, y, core, 0, piece), load_sem.at[CHUNKS])
    own_rot.start()
    own_coef = []
    for c in range(CHUNKS):
        copy = pltpu.make_async_copy(
            coef.at[pl.ds(c * chunk, chunk), :], a_rows(x, c * chunk, chunk), load_sem.at[c]
        )
        copy.start()
        own_coef.append(copy)

    barrier = pltpu.get_barrier_semaphore()

    def greet(step, carry):
        pl.semaphore_signal(
            barrier, inc=1, device_id={"ga": (g + step) % peers, "ba": x}, device_id_type=MESH
        )
        return carry

    lax.fori_loop(1, peers, greet, 0)
    for by in (1, -1):
        pl.semaphore_signal(
            barrier, inc=1, device_id={"ga": g, "ba": shift(x, by)}, device_id_type=MESH
        )
    pl.semaphore_wait(barrier, peers + 1)

    def remote(ref, send, recv, ga, ba):
        return pltpu.make_async_remote_copy(
            src_ref=ref, dst_ref=ref, send_sem=send, recv_sem=recv,
            device_id={"ga": ga, "ba": ba}, device_id_type=MESH,
        )

    def launch(copy):
        copy.start()
        sends.append(copy)

    def a_copy(direction, kind, c):
        by = 1 if direction == 0 else -1
        if kind == 0:
            ref = a_rows(x, c * chunk, chunk)
        else:
            ref = a_rows(shift(x, -by), c * chunk + direction * half_chunk, half_chunk)
        return remote(ref, a_send.at[direction, kind, c], a_recv.at[direction, kind, c], g, shift(x, by))

    def a_arrived(direction, kind, c):
        by = 1 if direction == 0 else -1
        if kind == 0:
            ref = a_rows(shift(x, -by), c * chunk, chunk)
        else:
            ref = a_rows(shift(x, 2), c * chunk + direction * half_chunk, half_chunk)
        remote(ref, a_send.at[direction, kind, c], a_recv.at[direction, kind, c], g, shift(x, by)).wait_recv()

    def a_relay(c):
        for direction in (0, 1):
            a_arrived(direction, 0, c)
            launch(a_copy(direction, 1, c))

    n_sent = [0]

    def place(h, first, second):
        return (shift(z, second), shift(y, first)) if h == 0 else (shift(z, first), shift(y, second))

    def device_of(zz, yy, cc):
        return (zz * SIDE + yy) * 2 + cc

    def r_ref(h, at, part):
        start, size = h * half, half
        if part is not None:
            start, size = start + part * quarter, quarter
        return r_rows(at[0], at[1], core, start, size)

    def r_copy(h, at, part, to):
        slot = n_sent[0]
        n_sent[0] += 1
        launch(remote(
            r_ref(h, at, part), r_send.at[slot], r_recv.at[h, at[0] * SIDE + at[1], part or 0],
            device_of(to[0], to[1], core), x,
        ))

    def r_arrived(h, at, part):
        remote(
            r_ref(h, at, part), r_send.at[0], r_recv.at[h, at[0] * SIDE + at[1], part or 0], device_of(z, y, 1 - core), x
        ).wait_recv()

    def to_partner(h, at):
        index = at[0] * SIDE + at[1]
        launch(remote(r_ref(h, at, None), p_send.at[h, index], p_recv.at[h, index], device_of(z, y, 1 - core), x))

    def along_second(h, at):
        for by in (1, -1):
            r_copy(h, at, None, place(h, 0, by))

    own_rot.wait()
    for h in (0, 1):
        at = place(h, 0, 0)
        for by in (1, -1):
            r_copy(h, at, None, place(h, by, 0))
    for c in range(CHUNKS):
        own_coef[c].wait()
        for direction in (0, 1):
            launch(a_copy(direction, 0, c))
    for h in (0, 1):
        at = place(h, 0, 0)
        along_second(h, at)
        to_partner(h, at)
    for direction in (0, 1):
        by = 1 if direction == 0 else -1
        for h in (0, 1):
            at = place(h, -by, 0)
            r_arrived(h, at, None)
            r_copy(h, at, direction, place(h, by, 0))
            along_second(h, at)
            to_partner(h, at)
    for h in (0, 1):
        at = place(h, 2, 0)
        r_arrived(h, at, 0)
        r_arrived(h, at, 1)
        along_second(h, at)
        to_partner(h, at)
    for first in (0, -1, 1, 2):
        for direction in (0, 1):
            by = 1 if direction == 0 else -1
            for h in (0, 1):
                at = place(h, first, -by)
                r_arrived(h, at, None)
                r_copy(h, at, direction, place(h, 0, by))
                to_partner(h, at)
        if first == 0:
            a_relay(0)
        if first == 1:
            a_relay(1)
    for first in (0, -1, 1, 2):
        for h in (0, 1):
            at = place(h, first, 2)
            r_arrived(h, at, 0)
            r_arrived(h, at, 1)
            to_partner(h, at)
    a_relay(2)
    for h in (0, 1):
        def partner_arrived(index, carry):
            zz, yy = index // SIDE, index % SIDE
            remote(
                r_rows(zz, yy, 1 - core, h * half, half), p_send.at[h, index], p_recv.at[h, index],
                device_of(z, y, 1 - core), x,
            ).wait_recv()
            return carry

        lax.fori_loop(0, SIDE * SIDE, partner_arrived, 0)

    def product(block, start, m, j):
        columns = pl.ds(pl.multiple_of(j * TILE_N, TILE_N), TILE_N)
        return columns, jnp.dot(
            a_buf[block, pl.ds(start, m), :], r_buf[block, :, columns], preferred_element_type=jnp.float32
        )

    n_tiles = cols // TILE_N
    m_tiles = rows // TILE_M

    def own_step(step, carry):
        start = pl.multiple_of((step % m_tiles) * TILE_M, 16)
        columns, value = product(x, start, TILE_M, step // m_tiles)
        c_buf[pl.ds(start, TILE_M), columns] = value
        return carry

    lax.fori_loop(0, n_tiles * m_tiles, own_step, 0)
    for c in range(3, CHUNKS):
        a_relay(c)

    def next_step(step, carry):
        start = pl.multiple_of((step % m_tiles) * TILE_M, 16)
        for by in (1, -1):
            columns, value = product(shift(x, by), start, TILE_M, step // m_tiles)
            c_buf[pl.ds(start, TILE_M), columns] += value
        return carry

    lax.fori_loop(0, n_tiles * m_tiles, next_step, 0)
    sq_sum[...] = jnp.zeros_like(sq_sum)
    for c in range(CHUNKS):
        a_arrived(0, 1, c)
        a_arrived(1, 1, c)

        def last_step(j, carry):
            columns, value = product(shift(x, 2), c * chunk, chunk, j)
            total = c_buf[c * chunk:(c + 1) * chunk, columns] + value
            c_buf[c * chunk:(c + 1) * chunk, columns] = total
            sq_sum[:, columns] += jnp.sum(total * total, axis=0, keepdims=True)
            return carry

        lax.fori_loop(0, n_tiles, last_step, 0)

    sq_buf[g] = sq_sum[...]

    def square_copy(source, target, sem):
        return remote(sq_buf.at[source], s_send.at[sem], s_recv.at[source], target, x)

    def send_squares(step, carry):
        square_copy(g, (g + step) % peers, step).start()
        return carry

    def squares_arrived(step, carry):
        source = (g + step) % peers
        square_copy(source, source, step).wait_recv()
        return carry

    def squares_sent(step, carry):
        square_copy(g, (g + step) % peers, step).wait_send()
        return carry

    lax.fori_loop(1, peers, send_squares, 0)
    for copy in sends:
        copy.wait_send()
    lax.fori_loop(1, peers, squares_sent, 0)
    lax.fori_loop(1, peers, squares_arrived, 0)

    total = sq_buf[0]
    for i in range(1, peers):
        total = total + sq_buf[i]
    rms = jnp.sqrt(total / TOTAL_ROWS + 1e-06)
    rms_out[...] = rms
    sq_sum[...] = 1.0 / rms

    def out_copy(i):
        start = i * chunk
        return pltpu.make_async_copy(a_rows(x, start, chunk), out.at[pl.ds(start, chunk), :], out_sem.at[i])

    for c in range(CHUNKS):
        a_buf[x, c * chunk:(c + 1) * chunk, :] = (
            c_buf[c * chunk:(c + 1) * chunk, :] * sq_sum[...]
        ).astype(jnp.bfloat16)
        out_copy(c).start()
    for c in range(CHUNKS):
        out_copy(c).wait()


def body(coefficients, rotation):
    rows, depth = coefficients.shape
    piece, cols = rotation.shape
    peers = lax.axis_size("ga")
    dma = pltpu.SemaphoreType.DMA
    out, rms = pl.pallas_call(
        kernel,
        out_shape=(
            jax.ShapeDtypeStruct((rows, cols), jnp.bfloat16),
            jax.ShapeDtypeStruct((1, cols), jnp.float32),
        ),
        in_specs=[pl.BlockSpec(memory_space=pl.ANY)] * 2,
        out_specs=(pl.BlockSpec(memory_space=pl.ANY), pl.BlockSpec(memory_space=pltpu.VMEM)),
        scratch_shapes=[
            pltpu.VMEM((SIDE, rows, depth), jnp.bfloat16),
            pltpu.VMEM((SIDE, depth, cols), jnp.bfloat16),
            pltpu.VMEM((rows, cols), jnp.float32),
            pltpu.VMEM((1, cols), jnp.float32),
            pltpu.VMEM((peers, 1, cols), jnp.float32),
            dma((CHUNKS + 1,)),
            dma((2, 2, CHUNKS)),
            dma((2, 2, CHUNKS)),
            dma((40,)),
            dma((2, 16, 2)),
            dma((2, 16)),
            dma((2, 16)),
            dma((peers,)),
            dma((peers,)),
            dma((CHUNKS,)),
        ],
        compiler_params=pltpu.CompilerParams(
            collective_id=0, has_side_effects=True, vmem_limit_bytes=64 * 1024 * 1024 - 65536
        ),
        cost_estimate=pl.CostEstimate(
            flops=2 * rows * depth * SIDE * cols, bytes_accessed=4 * rows * depth, transcendentals=0
        ),
    )(coefficients, rotation)
    return out, rms.reshape(cols)


def solution(mesh):
    return jax.shard_map(
        body, mesh=mesh, in_specs=(P("ga", "ba"), P("ga", "ba")), out_specs=(P("ga", "ba"), P("ba")), check_vma=False
    )
```

```python
import functools

import jax
import jax.numpy as jnp
from jax import lax
from jax.experimental import pallas as pl
from jax.experimental.pallas import tpu as pltpu
from jax.sharding import PartitionSpec as P

MESH = pl.DeviceIdType.MESH
SIDE = 4
SIZES = (192, 192, 192, 192, 192, 192, 64, 64)
CHUNKS = 8
TILE_M = 320
TILE_N = 512
TOTAL_ROWS = 40960


def gather_multiply(
    coef, rot, c_buf, sq_buf, a_buf, r_buf, sq_sum,
    load_sem, a_send, a_recv, r_send, r_recv, p_send, p_recv, s_send, s_recv,
):
    rows, depth = coef.shape
    piece, cols = rot.shape
    peers = 2 * SIDE * SIDE
    starts = [sum(SIZES[:c]) for c in range(len(SIZES))]
    half = piece // 2
    quarter = half // 2

    g = lax.axis_index("ga")
    x = lax.axis_index("ba")
    core = g % 2
    y = (g // 2) % SIDE
    z = g // (2 * SIDE)
    sends = []

    def shift(value, by):
        return (value + by + SIDE) % SIDE

    def device_of(zz, yy, cc):
        return (zz * SIDE + yy) * 2 + cc

    def a_rows(block, start, size):
        return a_buf.at[block, pl.ds(start, size), :]

    def r_rows(zz, yy, cc, start, size):
        return r_buf.at[zz, pl.ds(pl.multiple_of((yy * 2 + cc) * piece + start, 16), size), :]

    own_rot = pltpu.make_async_copy(rot, r_rows(z, y, core, 0, piece), load_sem.at[len(SIZES)])
    own_rot.start()
    own_coef = []
    for c, (start, size) in enumerate(zip(starts, SIZES)):
        copy = pltpu.make_async_copy(coef.at[pl.ds(start, size), :], a_rows(x, start, size), load_sem.at[c])
        copy.start()
        own_coef.append(copy)

    barrier = pltpu.get_barrier_semaphore()

    near = [(device_of(shift(z, by), y, core), x) for by in (1, -1)]
    near += [(device_of(z, shift(y, by), core), x) for by in (1, -1)]
    near += [(g, shift(x, by)) for by in (1, -1)]
    near += [(device_of(z, y, 1 - core), x)]
    for ga, ba in near:
        pl.semaphore_signal(barrier, inc=1, device_id={"ga": ga, "ba": ba}, device_id_type=MESH)
    pl.semaphore_wait(barrier, len(near))

    def remote(ref, send, recv, ga, ba):
        return pltpu.make_async_remote_copy(
            src_ref=ref, dst_ref=ref, send_sem=send, recv_sem=recv,
            device_id={"ga": ga, "ba": ba}, device_id_type=MESH,
        )

    def launch(copy):
        copy.start()
        sends.append(copy)

    def a_copy(direction, kind, c):
        by = 1 if direction == 0 else -1
        if kind == 0:
            ref = a_rows(x, starts[c], SIZES[c])
        else:
            ref = a_rows(shift(x, -by), starts[c] + direction * (SIZES[c] // 2), SIZES[c] // 2)
        return remote(ref, a_send.at[direction, kind, c], a_recv.at[direction, kind, c], g, shift(x, by))

    def a_arrived(direction, kind, c):
        by = 1 if direction == 0 else -1
        if kind == 0:
            ref = a_rows(shift(x, -by), starts[c], SIZES[c])
        else:
            ref = a_rows(shift(x, 2), starts[c] + direction * (SIZES[c] // 2), SIZES[c] // 2)
        remote(ref, a_send.at[direction, kind, c], a_recv.at[direction, kind, c], g, shift(x, by)).wait_recv()

    def a_relay(c):
        for direction in (0, 1):
            a_arrived(direction, 0, c)
            launch(a_copy(direction, 1, c))

    n_sent = [0]

    def place(h, first, second):
        return (shift(z, second), shift(y, first)) if h == 0 else (shift(z, first), shift(y, second))

    def r_ref(h, at, part):
        start, size = h * half, half
        if part is not None:
            start, size = start + part * quarter, quarter
        return r_rows(at[0], at[1], core, start, size)

    def r_copy(h, at, part, to):
        slot = n_sent[0]
        n_sent[0] += 1
        launch(remote(
            r_ref(h, at, part), r_send.at[slot], r_recv.at[h, at[0] * SIDE + at[1], part or 0],
            device_of(to[0], to[1], core), x,
        ))

    def r_arrived(h, at, part):
        remote(
            r_ref(h, at, part), r_send.at[0], r_recv.at[h, at[0] * SIDE + at[1], part or 0], device_of(z, y, 1 - core), x
        ).wait_recv()

    def to_partner(h, at):
        index = at[0] * SIDE + at[1]
        launch(remote(r_ref(h, at, None), p_send.at[h, index], p_recv.at[h, index], device_of(z, y, 1 - core), x))

    def along_second(h, at):
        for by in (1, -1):
            r_copy(h, at, None, place(h, 0, by))

    own_rot.wait()
    for h in (0, 1):
        at = place(h, 0, 0)
        for by in (1, -1):
            r_copy(h, at, None, place(h, by, 0))
    for c in range(len(SIZES)):
        own_coef[c].wait()
        for direction in (0, 1):
            launch(a_copy(direction, 0, c))
    for h in (0, 1):
        at = place(h, 0, 0)
        along_second(h, at)
        to_partner(h, at)
    for direction in (0, 1):
        by = 1 if direction == 0 else -1
        for h in (0, 1):
            at = place(h, -by, 0)
            r_arrived(h, at, None)
            r_copy(h, at, direction, place(h, by, 0))
            along_second(h, at)
            to_partner(h, at)
    for h in (0, 1):
        at = place(h, 2, 0)
        r_arrived(h, at, 0)
        r_arrived(h, at, 1)
        along_second(h, at)
        to_partner(h, at)
    for first in (0, -1, 1, 2):
        for direction in (0, 1):
            by = 1 if direction == 0 else -1
            for h in (0, 1):
                at = place(h, first, -by)
                r_arrived(h, at, None)
                r_copy(h, at, direction, place(h, 0, by))
                to_partner(h, at)
        if first == 0:
            a_relay(0)
        if first == 1:
            a_relay(1)
    for first in (0, -1, 1, 2):
        for h in (0, 1):
            at = place(h, first, 2)
            r_arrived(h, at, 0)
            r_arrived(h, at, 1)
            to_partner(h, at)
    a_relay(2)
    for h in (0, 1):
        def partner_arrived(index, carry):
            zz, yy = index // SIDE, index % SIDE
            remote(
                r_rows(zz, yy, 1 - core, h * half, half), p_send.at[h, index], p_recv.at[h, index],
                device_of(z, y, 1 - core), x,
            ).wait_recv()
            return carry

        lax.fori_loop(0, SIDE * SIDE, partner_arrived, 0)

    def product(block, start, m, j):
        columns = pl.ds(pl.multiple_of(j * TILE_N, TILE_N), TILE_N)
        return columns, jnp.dot(
            a_buf[block, pl.ds(start, m), :], r_buf[block, :, columns], preferred_element_type=jnp.float32
        )

    n_tiles = cols // TILE_N
    m_tiles = rows // TILE_M

    def own_step(step, carry):
        start = pl.multiple_of((step % m_tiles) * TILE_M, 16)
        columns, value = product(x, start, TILE_M, step // m_tiles)
        c_buf[pl.ds(start, TILE_M), columns] = value
        return carry

    lax.fori_loop(0, n_tiles * m_tiles, own_step, 0)
    for c in range(3, len(SIZES)):
        a_relay(c)

    def next_step(step, carry):
        start = pl.multiple_of((step % m_tiles) * TILE_M, 16)
        for by in (1, -1):
            columns, value = product(shift(x, by), start, TILE_M, step // m_tiles)
            c_buf[pl.ds(start, TILE_M), columns] += value
        return carry

    lax.fori_loop(0, n_tiles * m_tiles, next_step, 0)
    sq_sum[...] = jnp.zeros_like(sq_sum)
    for c in range(len(SIZES)):
        a_arrived(0, 1, c)
        a_arrived(1, 1, c)

        def last_step(j, carry):
            columns, value = product(shift(x, 2), starts[c], SIZES[c], j)
            total = c_buf[starts[c]:starts[c] + SIZES[c], columns] + value
            c_buf[starts[c]:starts[c] + SIZES[c], columns] = total
            sq_sum[:, columns] += jnp.sum(total * total, axis=0, keepdims=True)
            return carry

        lax.fori_loop(0, n_tiles, last_step, 0)

    sq_buf[g] = sq_sum[...]

    def square_copy(source, target, sem):
        return remote(sq_buf.at[source], s_send.at[sem], s_recv.at[source], target, x)

    def send_squares(step, carry):
        square_copy(g, (g + step) % peers, step).start()
        return carry

    def squares_arrived(step, carry):
        source = (g + step) % peers
        square_copy(source, source, step).wait_recv()
        return carry

    def squares_sent(step, carry):
        square_copy(g, (g + step) % peers, step).wait_send()
        return carry

    lax.fori_loop(1, peers, send_squares, 0)
    for copy in sends:
        copy.wait_send()
    lax.fori_loop(1, peers, squares_sent, 0)
    lax.fori_loop(1, peers, squares_arrived, 0)


def normalize(c_buf, sq_buf, out, rms_out, scale, staged, out_sem):
    rows, cols = c_buf.shape
    chunk = rows // CHUNKS
    total = sq_buf[0]
    for i in range(1, sq_buf.shape[0]):
        total = total + sq_buf[i]
    rms = jnp.sqrt(total / TOTAL_ROWS + 1e-06)
    rms_out[...] = rms.reshape(cols)
    scale[...] = 1.0 / rms

    def out_copy(c):
        part = pl.ds(c * chunk, chunk)
        return pltpu.make_async_copy(staged.at[part, :], out.at[part, :], out_sem.at[c])

    for c in range(CHUNKS):
        part = pl.ds(c * chunk, chunk)
        staged[part, :] = (c_buf[part, :] * scale[...]).astype(jnp.bfloat16)
        out_copy(c).start()
    for c in range(CHUNKS):
        out_copy(c).wait()


def body(coefficients, rotation):
    rows, depth = coefficients.shape
    piece, cols = rotation.shape
    peers = lax.axis_size("ga")
    dma = pltpu.SemaphoreType.DMA
    rotated, squares = pl.pallas_call(
        gather_multiply,
        out_shape=(pltpu.VMEM((rows, cols), jnp.float32), pltpu.VMEM((peers, 1, cols), jnp.float32)),
        in_specs=[pl.BlockSpec(memory_space=pl.ANY)] * 2,
        out_specs=(pl.BlockSpec(memory_space=pltpu.VMEM), pl.BlockSpec(memory_space=pltpu.VMEM)),
        scratch_shapes=[
            pltpu.VMEM((SIDE, rows, depth), jnp.bfloat16),
            pltpu.VMEM((SIDE, depth, cols), jnp.bfloat16),
            pltpu.VMEM((1, cols), jnp.float32),
            dma((len(SIZES) + 1,)),
            dma((2, 2, len(SIZES))),
            dma((2, 2, len(SIZES))),
            dma((40,)),
            dma((2, 16, 2)),
            dma((2, 16)),
            dma((2, 16)),
            dma((peers,)),
            dma((peers,)),
        ],
        compiler_params=pltpu.CompilerParams(
            collective_id=0, has_side_effects=True, vmem_limit_bytes=50 * 1024 * 1024
        ),
        cost_estimate=pl.CostEstimate(
            flops=2 * rows * depth * SIDE * cols, bytes_accessed=4 * rows * depth, transcendentals=0
        ),
    )(coefficients, rotation)
    return pl.pallas_call(
        normalize,
        out_shape=(
            jax.ShapeDtypeStruct((rows, cols), jnp.bfloat16),
            jax.ShapeDtypeStruct((cols,), jnp.float32),
        ),
        in_specs=[pl.BlockSpec(memory_space=pltpu.VMEM)] * 2,
        out_specs=(pl.BlockSpec(memory_space=pl.ANY), pl.BlockSpec(memory_space=pltpu.VMEM)),
        scratch_shapes=[
            pltpu.VMEM((1, cols), jnp.float32),
            pltpu.VMEM((rows, cols), jnp.bfloat16),
            dma((CHUNKS,)),
        ],
        compiler_params=pltpu.CompilerParams(vmem_limit_bytes=20 * 1024 * 1024),
        cost_estimate=pl.CostEstimate(flops=rows * cols, bytes_accessed=6 * rows * cols, transcendentals=0),
    )(rotated, squares)


def solution(mesh):
    return jax.shard_map(
        body, mesh=mesh, in_specs=(P("ga", "ba"), P("ga", "ba")), out_specs=(P("ga", "ba"), P("ba")), check_vma=False
    )
```

```python
import functools

import jax
import jax.numpy as jnp
from jax import lax
from jax.experimental import pallas as pl
from jax.experimental.pallas import tpu as pltpu
from jax.sharding import PartitionSpec as P

MESH = pl.DeviceIdType.MESH
SIDE = 4
SIZES = (256, 256, 256, 256, 192, 64)
CHUNKS = 8
TILE_M = 320
TILE_N = 512
TOTAL_ROWS = 40960


def gather_multiply(
    coef, rot, c_buf, sq_buf, a_buf, r_buf, sq_sum,
    load_sem, a_sem, relay_sem, r_sem, sem,
):
    rows, depth = coef.shape
    piece, cols = rot.shape
    peers = 2 * SIDE * SIDE
    starts = [sum(SIZES[:c]) for c in range(len(SIZES))]
    half = piece // 2
    quarter = half // 2

    g = lax.axis_index("ga")
    x = lax.axis_index("ba")
    core = g % 2
    y = (g // 2) % SIDE
    z = g // (2 * SIDE)
    a_send, r_send, p_send, p_recv, s_send, s_recv = (sem.at[i] for i in range(6))

    def shift(value, by):
        return (value + by + SIDE) % SIDE

    def device_of(zz, yy, cc):
        return (zz * SIDE + yy) * 2 + cc

    def a_rows(block, start, size):
        return a_buf.at[block, pl.ds(start, size), :]

    def r_rows(zz, yy, cc, start, size):
        return r_buf.at[pl.ds(pl.multiple_of(device_of(zz, yy, cc) * piece + start, 16), size), :]

    own_rot = pltpu.make_async_copy(rot, r_rows(z, y, core, 0, piece), load_sem.at[1])
    own_rot.start()
    own_coef = pltpu.make_async_copy(coef, a_buf.at[x], load_sem.at[0])
    own_coef.start()

    barrier = pltpu.get_barrier_semaphore()

    near = [(device_of(shift(z, by), y, core), x) for by in (1, -1)]
    near += [(device_of(z, shift(y, by), core), x) for by in (1, -1)]
    near += [(g, shift(x, by)) for by in (1, -1)]
    near += [(device_of(z, y, 1 - core), x)]
    for ga, ba in near:
        pl.semaphore_signal(barrier, inc=1, device_id={"ga": ga, "ba": ba}, device_id_type=MESH)
    pl.semaphore_wait(barrier, len(near))

    def remote(ref, send, recv, ga, ba):
        return pltpu.make_async_remote_copy(
            src_ref=ref, dst_ref=ref, send_sem=send, recv_sem=recv,
            device_id={"ga": ga, "ba": ba}, device_id_type=MESH,
        )

    def half_rows(block, direction, c):
        return a_rows(block, starts[c] + direction * (SIZES[c] // 2), SIZES[c] // 2)

    def a_start(direction, c):
        to = shift(x, 1 - 2 * direction)
        remote(a_rows(x, starts[c], SIZES[c]), a_send, a_sem.at[direction, c], g, to).start()

    def a_wait(direction, c):
        origin = shift(x, 2 * direction - 1)
        remote(a_rows(origin, starts[c], SIZES[c]), a_send, a_sem.at[direction, c], g, origin).wait_recv()

    def relay_start(direction, c):
        origin, to = shift(x, 2 * direction - 1), shift(x, 1 - 2 * direction)
        remote(half_rows(origin, direction, c), a_send, relay_sem.at[c], g, to).start()

    def relay_wait(c):
        origin = shift(x, 2)
        remote(a_rows(origin, starts[c], SIZES[c]), a_send, relay_sem.at[c], g, shift(x, 1)).wait_recv()

    def a_relay(c):
        for direction in (0, 1):
            a_wait(direction, c)
            relay_start(direction, c)

    def place(h, first, second):
        return (shift(z, second), shift(y, first)) if h == 0 else (shift(z, first), shift(y, second))

    def r_ref(h, at, part):
        if part is None:
            return r_rows(at[0], at[1], core, h * half, half)
        return r_rows(at[0], at[1], core, h * half + part * quarter, quarter)

    def r_start(h, at, part, slot, to):
        remote(r_ref(h, at, part), r_send, r_sem.at[h, slot], device_of(to[0], to[1], core), x).start()

    def r_wait(h, at, slot):
        remote(r_ref(h, at, None), r_send, r_sem.at[h, slot], device_of(z, y, 1 - core), x).wait_recv()

    def to_partner(h, at):
        remote(r_ref(h, at, None), p_send, p_recv, device_of(z, y, 1 - core), x).start()

    places = {0: 0, -1: 1, 1: 2, 2: 3}

    def slot_of(first, kind):
        return 3 + 3 * places[first] + kind

    def along_second(h, at, first):
        for direction in (0, 1):
            r_start(h, at, None, slot_of(first, direction), place(h, 0, 1 - 2 * direction))

    own_rot.wait()
    for h in (0, 1):
        for direction in (0, 1):
            r_start(h, (z, y), None, direction, place(h, 1 - 2 * direction, 0))
    own_coef.wait()
    for c in range(len(SIZES)):
        for direction in (0, 1):
            a_start(direction, c)
    for h in (0, 1):
        along_second(h, (z, y), 0)
        to_partner(h, (z, y))
    for direction in (0, 1):
        by = 1 - 2 * direction
        for h in (0, 1):
            at = place(h, -by, 0)
            r_wait(h, at, direction)
            r_start(h, at, direction, 2, place(h, by, 0))
            along_second(h, at, -by)
            to_partner(h, at)
    for h in (0, 1):
        at = place(h, 2, 0)
        r_wait(h, at, 2)
        along_second(h, at, 2)
        to_partner(h, at)
    for first in (0, -1, 1, 2):
        for direction in (0, 1):
            by = 1 - 2 * direction
            for h in (0, 1):
                at = place(h, first, -by)
                r_wait(h, at, slot_of(first, direction))
                r_start(h, at, direction, slot_of(first, 2), place(h, 0, by))
                to_partner(h, at)
        if first == 0:
            a_relay(0)
    for first in (0, -1, 1, 2):
        for h in (0, 1):
            at = place(h, first, 2)
            r_wait(h, at, slot_of(first, 2))
            to_partner(h, at)
    a_relay(1)
    pieces = SIDE * SIDE * piece
    remote(r_buf.at[pl.ds(0, pieces), :], p_send, p_recv, device_of(z, y, 1 - core), x).wait()

    def product(block, start, m, j):
        columns = pl.ds(pl.multiple_of(j * TILE_N, TILE_N), TILE_N)
        return columns, jnp.dot(
            a_buf[block, pl.ds(start, m), :], r_buf[pl.ds(pl.multiple_of(block * depth, depth), depth), columns], preferred_element_type=jnp.float32
        )

    n_tiles = cols // TILE_N
    m_tiles = rows // TILE_M

    def own_step(step, carry):
        start = pl.multiple_of((step % m_tiles) * TILE_M, 16)
        columns, value = product(x, start, TILE_M, step // m_tiles)
        c_buf[pl.ds(start, TILE_M), columns] = value
        return carry

    lax.fori_loop(0, n_tiles * m_tiles, own_step, 0)
    for c in range(2, len(SIZES)):
        a_relay(c)

    def next_step(step, carry):
        start = pl.multiple_of((step % m_tiles) * TILE_M, 16)
        for by in (1, -1):
            columns, value = product(shift(x, by), start, TILE_M, step // m_tiles)
            c_buf[pl.ds(start, TILE_M), columns] += value
        return carry

    lax.fori_loop(0, n_tiles * m_tiles, next_step, 0)
    sq_sum[...] = jnp.zeros_like(sq_sum)
    for c in range(len(SIZES)):
        relay_wait(c)

        def last_step(j, carry):
            columns, value = product(shift(x, 2), starts[c], SIZES[c], j)
            total = c_buf[starts[c]:starts[c] + SIZES[c], columns] + value
            c_buf[starts[c]:starts[c] + SIZES[c], columns] = total
            sq_sum[:, columns] += jnp.sum(total * total, axis=0, keepdims=True)
            return carry

        lax.fori_loop(0, n_tiles, last_step, 0)

    sq_buf[g] = sq_sum[...]
    others = [(dz, dy, dc) for dz in range(-1, 3) for dy in range(-1, 3) for dc in (0, 1) if (dz, dy, dc) != (0, 0, 0)]
    for dz, dy, dc in sorted(others, key=lambda by: -(abs(by[0]) + abs(by[1]))):
        peer = device_of(shift(z, dz), shift(y, dy), (core + dc) % 2)
        remote(sq_buf.at[g], s_send, s_recv, peer, x).start()
    remote(a_buf.at[pl.ds(0, 3)], a_send, a_sem.at[0, 0], g, shift(x, 1)).wait_send()
    sent = 15 * piece
    remote(r_buf.at[pl.ds(0, sent), :], r_send, r_sem.at[0, 0], device_of(z, y, 1 - core), x).wait_send()
    remote(sq_buf.at[pl.ds(0, peers - 1)], s_send, s_recv, device_of(z, y, 1 - core), x).wait()


def normalize(c_buf, sq_buf, out, rms_out, scale, staged, out_sem):
    rows, cols = c_buf.shape
    chunk = rows // CHUNKS
    total = sq_buf[0]
    for i in range(1, sq_buf.shape[0]):
        total = total + sq_buf[i]
    rms = jnp.sqrt(total / TOTAL_ROWS + 1e-06)
    rms_out[...] = rms.reshape(cols)
    scale[...] = 1.0 / rms

    def out_copy(c):
        part = pl.ds(c * chunk, chunk)
        return pltpu.make_async_copy(staged.at[part, :], out.at[part, :], out_sem.at[c])

    for c in range(CHUNKS):
        part = pl.ds(c * chunk, chunk)
        staged[part, :] = (c_buf[part, :] * scale[...]).astype(jnp.bfloat16)
        out_copy(c).start()
    for c in range(CHUNKS):
        out_copy(c).wait()


def body(coefficients, rotation):
    rows, depth = coefficients.shape
    piece, cols = rotation.shape
    peers = lax.axis_size("ga")
    dma = pltpu.SemaphoreType.DMA
    rotated, squares = pl.pallas_call(
        gather_multiply,
        out_shape=(pltpu.VMEM((rows, cols), jnp.float32), pltpu.VMEM((peers, 1, cols), jnp.float32)),
        in_specs=[pl.BlockSpec(memory_space=pl.ANY)] * 2,
        out_specs=(pl.BlockSpec(memory_space=pltpu.VMEM), pl.BlockSpec(memory_space=pltpu.VMEM)),
        scratch_shapes=[
            pltpu.VMEM((SIDE, rows, depth), jnp.bfloat16),
            pltpu.VMEM((SIDE * depth, cols), jnp.bfloat16),
            pltpu.VMEM((1, cols), jnp.float32),
            dma((2,)),
            dma((2, len(SIZES))),
            dma((len(SIZES),)),
            dma((2, 15)),
            dma((6,)),
        ],
        compiler_params=pltpu.CompilerParams(
            collective_id=0, has_side_effects=True, vmem_limit_bytes=50 * 1024 * 1024
        ),
        cost_estimate=pl.CostEstimate(
            flops=2 * rows * depth * SIDE * cols, bytes_accessed=4 * rows * depth, transcendentals=0
        ),
    )(coefficients, rotation)
    return pl.pallas_call(
        normalize,
        out_shape=(
            jax.ShapeDtypeStruct((rows, cols), jnp.bfloat16),
            jax.ShapeDtypeStruct((cols,), jnp.float32),
        ),
        in_specs=[pl.BlockSpec(memory_space=pltpu.VMEM)] * 2,
        out_specs=(pl.BlockSpec(memory_space=pl.ANY), pl.BlockSpec(memory_space=pltpu.VMEM)),
        scratch_shapes=[
            pltpu.VMEM((1, cols), jnp.float32),
            pltpu.VMEM((rows, cols), jnp.bfloat16),
            dma((CHUNKS,)),
        ],
        compiler_params=pltpu.CompilerParams(vmem_limit_bytes=20 * 1024 * 1024),
        cost_estimate=pl.CostEstimate(flops=rows * cols, bytes_accessed=6 * rows * cols, transcendentals=0),
    )(rotated, squares)


def solution(mesh):
    return jax.shard_map(
        body, mesh=mesh, in_specs=(P("ga", "ba"), P("ga", "ba")), out_specs=(P("ga", "ba"), P("ba")), check_vma=False
    )
```

```python
import jax
import jax.numpy as jnp
from jax import lax
from jax.experimental import pallas as pl
from jax.experimental.pallas import tpu as pltpu
from jax.sharding import PartitionSpec as P

MESH = pl.DeviceIdType.MESH
SIDE = 4
LAST = (256, 64)
CHUNKS = 8
TILE_N = 512
TOTAL_ROWS = 40960
SENDS = ("a_send", "r_send", "s_send", "p_send", "x_send", "e_send", "q_send", "t_send")
ARRIVALS = ("x_recv", "e_recv", "q_recv", "t_recv", "p_recv", "p_recv00", "p_recv01", "p_recv10", "p_recv11")
SEMS = {name: i for i, name in enumerate(SENDS + ARRIVALS)}


def gather_multiply(
    coef, rot, c_buf, sq_buf, a_buf, r_buf, r2_buf, ext, sq_sum, sq_out, sq_in,
    load_sem, a_sem, relay_sem, last_sem, r_sem, r2_sem, sems,
):
    rows, depth = coef.shape
    piece, cols = rot.shape
    peers = 2 * SIDE * SIDE
    quarter = rows // SIDE
    side_cols = cols // 2
    k_all = peers * piece
    chip = 2 * piece

    g = lax.axis_index("ga")
    x = lax.axis_index("ba")
    core = g % 2
    y = (g // 2) % SIDE
    z = g // (2 * SIDE)
    sem = {name: sems.at[i] for name, i in SEMS.items()}

    def shift(value, by):
        return (value + by + SIDE) % SIDE

    def device_of(zz, yy, cc):
        return (zz * SIDE + yy) * 2 + cc

    partner = device_of(z, y, 1 - core)

    def rows_at(start, size, align=16):
        return pl.ds(pl.multiple_of(start, align), size)

    def a_part(block, by, start=0, size=None):
        at = block * rows + shift(x, by) * quarter + start
        return rows_at(at, quarter if size is None else size, 32)

    def piece_rows(at, cc, start=0, size=None):
        return rows_at(device_of(at[0], at[1], cc) * piece + start, piece if size is None else size)

    own = (z, y)

    own_rot = pltpu.make_async_copy(rot, r_buf.at[piece_rows(own, core), :], load_sem.at[1])
    own_rot.start()
    own_coef = pltpu.make_async_copy(coef, a_buf.at[rows_at(x * rows, rows), :], load_sem.at[0])
    own_coef.start()

    barrier = pltpu.get_barrier_semaphore()
    near = [(device_of(shift(z, by), y, core), x) for by in (1, -1)]
    near += [(device_of(z, shift(y, by), core), x) for by in (1, -1)]
    near += [(g, shift(x, by)) for by in (1, -1)]
    near += [(partner, x)]
    for ga, ba in near:
        pl.semaphore_signal(barrier, inc=1, device_id={"ga": ga, "ba": ba}, device_id_type=MESH)
    pl.semaphore_wait(barrier, len(near))

    def remote(src, dst, send, recv, ga, ba):
        return pltpu.make_async_remote_copy(
            src_ref=src, dst_ref=dst, send_sem=send, recv_sem=recv,
            device_id={"ga": ga, "ba": ba}, device_id_type=MESH,
        )

    order = lambda by: (by, 2, 0)

    def a_move(part, recv, to):
        ref = a_buf.at[part, :]
        return remote(ref, ref, sem["a_send"], recv, g, to)

    def a_start(direction, i):
        by = 1 - 2 * direction
        a_move(a_part(x, order(by)[i]), a_sem.at[direction, i], shift(x, by)).start()

    def a_wait(direction, i):
        by = 1 - 2 * direction
        a_move(a_part(shift(x, -by), order(by)[i] - by), a_sem.at[direction, i], shift(x, by)).wait_recv()

    def relay_start(direction):
        by = 1 - 2 * direction
        a_move(a_part(shift(x, -by), 0), relay_sem.at[direction], shift(x, by)).start()

    def relay_wait(direction):
        by = 1 - 2 * direction
        a_move(a_part(shift(x, 2), -by), relay_sem.at[direction], shift(x, by)).wait_recv()

    last_starts = [sum(LAST[:c]) for c in range(len(LAST))]

    def last_start(direction, c):
        by = 1 - 2 * direction
        size = LAST[c] // 2
        part = a_part(shift(x, -by), by, last_starts[c] + direction * size, size)
        a_move(part, last_sem.at[c], shift(x, by)).start()

    def last_wait(c):
        a_move(a_part(shift(x, 2), 0, last_starts[c], LAST[c]), last_sem.at[c], shift(x, 1)).wait_recv()

    def place(h, first, second):
        return (shift(z, second), shift(y, first)) if h == 0 else (shift(z, first), shift(y, second))

    def r_ref(q, h, at, part, cc):
        if q == 0:
            size = piece // 2
            start = h * size
            ref = r_buf
            if part is not None:
                size = size // 2
                start = start + part * size
            return ref.at[piece_rows(at, cc, start, size), :]
        size, start = piece, h * k_all
        if part is not None:
            size = size // 2
            start = start + part * size
        return r2_buf.at[piece_rows(at, cc, start, size), :]

    def r_start(q, h, at, part, slot, to):
        ref = r_ref(q, h, at, part, core)
        recv = (r_sem if q == 0 else r2_sem).at[h, slot]
        remote(ref, ref, sem["r_send"] if q == 0 else sem["s_send"], recv, device_of(to[0], to[1], core), x).start()

    def r_wait(q, h, at, slot):
        ref = r_ref(q, h, at, None, core)
        recv = (r_sem if q == 0 else r2_sem).at[h, slot]
        remote(ref, ref, sem["r_send"], recv, partner, x).wait_recv()

    def to_partner(q, h, at, late):
        ref = r_ref(q, h, at, None, core)
        recv = sem["p_recv"] if q == 0 else sem["p_recv%d%d" % (h, late)]
        remote(ref, ref, sem["p_send"] if q == 0 else sem["t_send"], recv, partner, x).start()

    places = {0: 0, -1: 1, 1: 2, 2: 3}

    def slot_of(first, kind):
        return 3 + 3 * places[first] + kind

    def late_of(first):
        return 0

    def along_second(q, h, at, first):
        for direction in (0, 1):
            r_start(q, h, at, None, slot_of(first, direction), place(h, 0, 1 - 2 * direction))

    def r_own_first(q):
        for h in (0, 1):
            for direction in (0, 1):
                r_start(q, h, own, None, direction, place(h, 1 - 2 * direction, 0))

    def r_own_second(q):
        for h in (0, 1):
            along_second(q, h, own, 0)
            to_partner(q, h, own, 0)

    def r_first(q, direction, h):
        by = 1 - 2 * direction
        at = place(h, -by, 0)
        r_wait(q, h, at, direction)
        r_start(q, h, at, direction, 2, place(h, by, 0))
        along_second(q, h, at, -by)
        to_partner(q, h, at, 0)

    def r_opposite(q, h):
        at = place(h, 2, 0)
        r_wait(q, h, at, 2)
        along_second(q, h, at, 2)
        to_partner(q, h, at, 0)

    def r_second(q, first, direction, h):
        by = 1 - 2 * direction
        at = place(h, first, -by)
        r_wait(q, h, at, slot_of(first, direction))
        r_start(q, h, at, direction, slot_of(first, 2), place(h, 0, by))
        to_partner(q, h, at, 0)

    def r_second_opposite(q, first, h):
        at = place(h, first, 2)
        r_wait(q, h, at, slot_of(first, 2))
        to_partner(q, h, at, 1)

    FIRSTS = (0, -1, 1, 2)

    def product(k, by, start, size, columns):
        return jnp.dot(
            a_buf[a_part(shift(x, k), by, start, size), :],
            r_buf[rows_at(shift(x, k) * depth, depth), columns],
            preferred_element_type=jnp.float32,
        )

    def unit(k, by, mode, start=0, size=None):
        size = quarter if size is None else size
        out_rows = rows_at(shift(x, by) * quarter + start, size, 32)

        def step(j, carry):
            columns = pl.ds(pl.multiple_of(j * TILE_N, TILE_N), TILE_N)
            value = product(k, by, start, size, columns)
            if mode != "set":
                value = value + c_buf[out_rows, columns]
            c_buf[out_rows, columns] = value
            if mode == "last":
                sq_sum[:, columns] += jnp.sum(value * value, axis=0, keepdims=True)
            return carry

        lax.fori_loop(0, cols // TILE_N, step, 0)

    def ext_value(h, mt, k):
        half_rows = quarter // 2
        if h == 0:
            block = shift(z, k)
            return jnp.dot(
                a_buf[a_part(block, -1, mt * half_rows, half_rows), :],
                r2_buf[rows_at(block * depth, depth), :],
                preferred_element_type=jnp.float32,
            )
        yy = shift(y, k)
        total = None
        for zz in range(SIDE):
            value = jnp.dot(
                a_buf[a_part(zz, 1, mt * half_rows, half_rows), pl.ds(pl.multiple_of(yy * chip, 128), chip)],
                r2_buf[rows_at(k_all + (zz * SIDE + yy) * chip, chip), :],
                preferred_element_type=jnp.float32,
            )
            total = value if total is None else total + value
        return total

    def ext_unit(h, k, mode):
        half_rows = quarter // 2

        def step(mt, carry):
            part = rows_at(mt * half_rows, half_rows)
            value = ext_value(h, mt, k)
            if mode != "set":
                value = value + ext[h, part, :]
            ext[h, part, :] = value
            if mode == "last":
                columns = pl.ds(h * side_cols, side_cols)
                sq_out[:, columns] += jnp.sum(value * value, axis=0, keepdims=True)
            return carry

        lax.fori_loop(0, 2, step, 0)

    def ext_copy(h):
        by = 1 - 2 * h
        dst = c_buf.at[rows_at(shift(x, -by) * quarter, quarter, 64), pl.ds(h * side_cols, side_cols)]
        return remote(ext.at[h], dst, sem["e_send"], sem["e_recv"], g, shift(x, by))

    def sq_ext_copy(h):
        columns = pl.ds(h * side_cols, side_cols)
        return remote(
            sq_out.at[:, columns], sq_in.at[:, columns], sem["q_send"], sem["q_recv"], g, shift(x, 1 - 2 * h)
        )

    own_rot.wait()
    for h in (0, 1):
        remote(
            r_buf.at[piece_rows(own, core), pl.ds(h * side_cols, side_cols)], r_ref(1, h, own, None, core),
            sem["x_send"], sem["x_recv"], g, shift(x, 2 * h - 1),
        ).start()
    r_own_first(0)
    own_coef.wait()
    for i in range(3):
        for direction in (0, 1):
            a_start(direction, i)
    r_own_second(0)
    sq_sum[...] = jnp.zeros_like(sq_sum)
    sq_out[...] = jnp.zeros_like(sq_out)
    for direction in (0, 1):
        for h in (0, 1):
            r_first(0, direction, h)
    for h in (0, 1):
        r_opposite(0, h)
    two = r2_buf.at[pl.ds(0, 2 * piece), :]
    remote(two, two, sem["x_send"], sem["x_recv"], g, shift(x, 1)).wait()
    r_own_first(1)
    r_own_second(1)
    for first in FIRSTS:
        for direction in (0, 1):
            for h in (0, 1):
                r_second(0, first, direction, h)
    for direction in (0, 1):
        a_wait(direction, 0)
        relay_start(direction)
    for first in FIRSTS:
        for h in (0, 1):
            r_second_opposite(0, first, h)
    pieces = SIDE * SIDE * piece
    ref = r_buf.at[pl.ds(0, pieces), :]
    remote(ref, ref, sem["p_send"], sem["p_recv"], partner, x).wait()
    for direction in (0, 1):
        for h in (0, 1):
            r_first(1, direction, h)
    for direction in (0, 1):
        a_wait(direction, 1)
        for c in range(len(LAST)):
            last_start(direction, c)

    unit(0, 0, "set")
    r_opposite(1, 0)
    unit(0, 1, "set")
    r_opposite(1, 1)
    unit(0, -1, "set")
    events = [(first, direction, h) for first in FIRSTS for direction in (0, 1) for h in (0, 1)]
    units = [(-1, 0), (1, 0), (-1, 1), (1, -1), None, (-1, -1), (1, 1)]
    for i, event in enumerate(events):
        r_second(1, *event)
        if i % 2 == 1 and i // 2 < len(units):
            if units[i // 2] is None:
                for direction in (0, 1):
                    a_wait(direction, 2)
            else:
                unit(*units[i // 2], "add")
    for direction in (0, 1):
        relay_wait(direction)
        unit(2, -1 if direction == 0 else 1, "last")
    early = r2_buf.at[pl.ds(0, 12 * piece), :]
    for h in (0, 1):
        remote(early, early, sem["t_send"], sem["p_recv%d0" % h], partner, x).wait_recv()
        for k in (0, -1, 1):
            ext_unit(h, k, "set" if k == 0 else "add")
        for first in FIRSTS[2 * h:2 * h + 2]:
            for hh in (0, 1):
                r_second_opposite(1, first, hh)
    late = r2_buf.at[pl.ds(0, 4 * piece), :]
    for h in (0, 1):
        remote(late, late, sem["t_send"], sem["p_recv%d1" % h], partner, x).wait_recv()
        ext_unit(h, 2, "last")
    for h in (0, 1):
        sq_ext_copy(h).start()
    for h in (0, 1):
        ext_copy(h).start()
    for c in range(len(LAST)):
        last_wait(c)
        unit(2, 0, "last", last_starts[c], LAST[c])
    remote(sq_out, sq_in, sem["q_send"], sem["q_recv"], g, shift(x, 1)).wait()

    sq_buf[g] = sq_sum[...] + sq_in[...]
    others = [(dz, dy, dc) for dz in range(-1, 3) for dy in range(-1, 3) for dc in (0, 1) if (dz, dy, dc) != (0, 0, 0)]
    for dz, dy, dc in sorted(others, key=lambda by: -(abs(by[0]) + abs(by[1]))):
        peer = device_of(shift(z, dz), shift(y, dy), (core + dc) % 2)
        remote(sq_buf.at[g], sq_buf.at[g], sem["s_send"] if False else load_sem.at[2], sem["t_recv"], peer, x).start()
    ref = a_buf.at[pl.ds(0, 9 * quarter), :]
    remote(ref, ref, sem["a_send"], sem["e_recv"], g, shift(x, 1)).wait_send()
    ref = r_buf.at[pl.ds(0, 15 * piece), :]
    remote(ref, ref, sem["r_send"], sem["e_recv"], partner, x).wait_send()
    ref = r2_buf.at[pl.ds(0, 30 * piece), :]
    remote(ref, ref, sem["s_send"], sem["e_recv"], partner, x).wait_send()
    ref = r2_buf.at[pl.ds(0, 32 * piece), :]
    remote(ref, ref, sem["t_send"], sem["e_recv"], partner, x).wait_send()
    ref = sq_buf.at[pl.ds(0, peers - 1)]
    remote(ref, ref, load_sem.at[2], sem["t_recv"], partner, x).wait()
    remote(ext, ext, sem["e_send"], sem["e_recv"], g, shift(x, 1)).wait()


def normalize(c_buf, sq_buf, out, rms_out, scale, staged, out_sem):
    rows, cols = c_buf.shape
    chunk = rows // CHUNKS
    total = sq_buf[0]
    for i in range(1, sq_buf.shape[0]):
        total = total + sq_buf[i]
    rms = jnp.sqrt(total / TOTAL_ROWS + 1e-06)
    rms_out[...] = rms.reshape(cols)
    scale[...] = 1.0 / rms

    def out_copy(c):
        part = pl.ds(c * chunk, chunk)
        return pltpu.make_async_copy(staged.at[part, :], out.at[part, :], out_sem.at[c])

    for c in range(CHUNKS):
        part = pl.ds(c * chunk, chunk)
        staged[part, :] = (c_buf[part, :] * scale[...]).astype(jnp.bfloat16)
        out_copy(c).start()
    for c in range(CHUNKS):
        out_copy(c).wait()


def body(coefficients, rotation):
    rows, depth = coefficients.shape
    piece, cols = rotation.shape
    peers = lax.axis_size("ga")
    dma = pltpu.SemaphoreType.DMA
    rotated, squares = pl.pallas_call(
        gather_multiply,
        out_shape=(pltpu.VMEM((rows, cols), jnp.float32), pltpu.VMEM((peers, 1, cols), jnp.float32)),
        in_specs=[pl.BlockSpec(memory_space=pl.ANY)] * 2,
        out_specs=(pl.BlockSpec(memory_space=pltpu.VMEM), pl.BlockSpec(memory_space=pltpu.VMEM)),
        scratch_shapes=[
            pltpu.VMEM((SIDE * rows, depth), jnp.bfloat16),
            pltpu.VMEM((SIDE * depth, cols), jnp.bfloat16),
            pltpu.VMEM((2 * SIDE * depth, cols // 2), jnp.bfloat16),
            pltpu.VMEM((2, rows // SIDE, cols // 2), jnp.float32),
            pltpu.VMEM((1, cols), jnp.float32),
            pltpu.VMEM((1, cols), jnp.float32),
            pltpu.VMEM((1, cols), jnp.float32),
            dma((3,)),
            dma((2, 3)),
            dma((2,)),
            dma((len(LAST),)),
            dma((2, 15)),
            dma((2, 15)),
            dma((len(SEMS),)),
        ],
        compiler_params=pltpu.CompilerParams(
            collective_id=0, has_side_effects=True, vmem_limit_bytes=55 * 1024 * 1024
        ),
        cost_estimate=pl.CostEstimate(
            flops=2 * rows * depth * SIDE * cols, bytes_accessed=4 * rows * depth, transcendentals=0
        ),
    )(coefficients, rotation)
    return pl.pallas_call(
        normalize,
        out_shape=(
            jax.ShapeDtypeStruct((rows, cols), jnp.bfloat16),
            jax.ShapeDtypeStruct((cols,), jnp.float32),
        ),
        in_specs=[pl.BlockSpec(memory_space=pltpu.VMEM)] * 2,
        out_specs=(pl.BlockSpec(memory_space=pl.ANY), pl.BlockSpec(memory_space=pltpu.VMEM)),
        scratch_shapes=[
            pltpu.VMEM((1, cols), jnp.float32),
            pltpu.VMEM((rows, cols), jnp.bfloat16),
            dma((CHUNKS,)),
        ],
        compiler_params=pltpu.CompilerParams(vmem_limit_bytes=20 * 1024 * 1024),
        cost_estimate=pl.CostEstimate(flops=rows * cols, bytes_accessed=6 * rows * cols, transcendentals=0),
    )(rotated, squares)


def solution(mesh):
    return jax.shard_map(
        body, mesh=mesh, in_specs=(P("ga", "ba"), P("ga", "ba")), out_specs=(P("ga", "ba"), P("ba")), check_vma=False
    )
```

```python
import jax
import jax.numpy as jnp
from jax import lax
from jax.experimental import pallas as pl
from jax.experimental.pallas import tpu as pltpu
from jax.sharding import PartitionSpec as P

MESH = pl.DeviceIdType.MESH
SIDE = 4
LAST = (256, 64)
CHUNKS = 8
TILE_N = 768
TOTAL_ROWS = 40960
SENDS = ("a_send", "r_send", "r2_send", "p_send", "p2_send", "x_send", "e_send", "q_send", "s_send")
ARRIVALS = ("x_recv", "e_recv", "q_recv", "s_recv", "p_recv", "p_recv00", "p_recv01", "p_recv10", "p_recv11")
SEMS = {name: i for i, name in enumerate(SENDS + ARRIVALS)}


def gather_multiply(
    coef, rot, c_buf, sq_buf, a_buf, r_buf, r2_buf, ext, sq_sum, sq_out, sq_in,
    load_sem, a_sem, relay_sem, last_sem, r_sem, r2_sem, sems,
):
    rows, depth = coef.shape
    piece, cols = rot.shape
    peers = 2 * SIDE * SIDE
    quarter = rows // SIDE
    side_cols = cols // 2
    k_all = peers * piece
    chip = 2 * piece

    g = lax.axis_index("ga")
    x = lax.axis_index("ba")
    core = g % 2
    y = (g // 2) % SIDE
    z = g // (2 * SIDE)
    sem = {name: sems.at[i] for name, i in SEMS.items()}

    def shift(value, by):
        return (value + by + SIDE) % SIDE

    def device_of(zz, yy, cc):
        return (zz * SIDE + yy) * 2 + cc

    partner = device_of(z, y, 1 - core)

    def rows_at(start, size, align=16):
        return pl.ds(pl.multiple_of(start, align), size)

    def a_part(block, by, start=0, size=None):
        at = block * rows + shift(x, by) * quarter + start
        return rows_at(at, quarter if size is None else size, 32)

    def piece_rows(at, cc, start=0, size=None):
        return rows_at(device_of(at[0], at[1], cc) * piece + start, piece if size is None else size)

    own = (z, y)

    own_rot = pltpu.make_async_copy(rot, r_buf.at[piece_rows(own, core), :], load_sem.at[1])
    own_rot.start()
    own_coef = pltpu.make_async_copy(coef, a_buf.at[rows_at(x * rows, rows), :], load_sem.at[0])
    own_coef.start()

    barrier = pltpu.get_barrier_semaphore()
    near = [(device_of(shift(z, by), y, core), x) for by in (1, -1)]
    near += [(device_of(z, shift(y, by), core), x) for by in (1, -1)]
    near += [(g, shift(x, by)) for by in (1, -1)]
    near += [(partner, x)]
    for ga, ba in near:
        pl.semaphore_signal(barrier, inc=1, device_id={"ga": ga, "ba": ba}, device_id_type=MESH)
    pl.semaphore_wait(barrier, len(near))

    def remote(src, dst, send, recv, ga, ba):
        return pltpu.make_async_remote_copy(
            src_ref=src, dst_ref=dst, send_sem=send, recv_sem=recv,
            device_id={"ga": ga, "ba": ba}, device_id_type=MESH,
        )

    order = lambda by: (by, 2, 0)

    def a_move(part, recv, to):
        ref = a_buf.at[part, :]
        return remote(ref, ref, sem["a_send"], recv, g, to)

    def a_start(direction, i):
        by = 1 - 2 * direction
        a_move(a_part(x, order(by)[i]), a_sem.at[direction, i], shift(x, by)).start()

    def a_wait(direction, i):
        by = 1 - 2 * direction
        a_move(a_part(shift(x, -by), order(by)[i] - by), a_sem.at[direction, i], shift(x, by)).wait_recv()

    def relay_start(direction):
        by = 1 - 2 * direction
        a_move(a_part(shift(x, -by), 0), relay_sem.at[direction], shift(x, by)).start()

    def relay_wait(direction):
        by = 1 - 2 * direction
        a_move(a_part(shift(x, 2), -by), relay_sem.at[direction], shift(x, by)).wait_recv()

    last_starts = [sum(LAST[:c]) for c in range(len(LAST))]

    def last_start(direction, c):
        by = 1 - 2 * direction
        size = LAST[c] // 2
        part = a_part(shift(x, -by), by, last_starts[c] + direction * size, size)
        a_move(part, last_sem.at[c], shift(x, by)).start()

    def last_wait(c):
        a_move(a_part(shift(x, 2), 0, last_starts[c], LAST[c]), last_sem.at[c], shift(x, 1)).wait_recv()

    def place(h, first, second):
        return (shift(z, second), shift(y, first)) if h == 0 else (shift(z, first), shift(y, second))

    def r_ref(q, h, at, part, cc):
        if q == 0:
            size = piece // 2
            start = h * size
            ref = r_buf
            if part is not None:
                size = size // 2
                start = start + part * size
            return ref.at[piece_rows(at, cc, start, size), :]
        size, start = piece, h * k_all
        if part is not None:
            size = size // 2
            start = start + part * size
        return r2_buf.at[piece_rows(at, cc, start, size), :]

    def r_start(q, h, at, part, slot, to):
        ref = r_ref(q, h, at, part, core)
        recv = (r_sem if q == 0 else r2_sem).at[h, slot]
        remote(ref, ref, sem["r_send"] if q == 0 else sem["r2_send"], recv, device_of(to[0], to[1], core), x).start()

    def r_wait(q, h, at, slot):
        ref = r_ref(q, h, at, None, core)
        recv = (r_sem if q == 0 else r2_sem).at[h, slot]
        remote(ref, ref, sem["r_send"], recv, partner, x).wait_recv()

    def to_partner(q, h, at, late):
        ref = r_ref(q, h, at, None, core)
        recv = sem["p_recv"] if q == 0 else sem["p_recv%d%d" % (h, late)]
        remote(ref, ref, sem["p_send"] if q == 0 else sem["p2_send"], recv, partner, x).start()

    places = {0: 0, -1: 1, 1: 2, 2: 3}

    def slot_of(first, kind):
        return 3 + 3 * places[first] + kind

    def along_second(q, h, at, first):
        for direction in (0, 1):
            r_start(q, h, at, None, slot_of(first, direction), place(h, 0, 1 - 2 * direction))

    def r_own_first(q):
        for h in (0, 1):
            for direction in (0, 1):
                r_start(q, h, own, None, direction, place(h, 1 - 2 * direction, 0))

    def r_own_second(q):
        for h in (0, 1):
            along_second(q, h, own, 0)
            to_partner(q, h, own, 0)

    def r_first(q):
        for direction in (0, 1):
            by = 1 - 2 * direction
            for h in (0, 1):
                at = place(h, -by, 0)
                r_wait(q, h, at, direction)
                r_start(q, h, at, direction, 2, place(h, by, 0))
        for by in (1, -1):
            for h in (0, 1):
                at = place(h, -by, 0)
                along_second(q, h, at, -by)
                to_partner(q, h, at, 0)

    def r_opposite(q, h):
        at = place(h, 2, 0)
        r_wait(q, h, at, 2)
        along_second(q, h, at, 2)
        to_partner(q, h, at, 0)

    def r_second(q, first, direction, h):
        by = 1 - 2 * direction
        at = place(h, first, -by)
        r_wait(q, h, at, slot_of(first, direction))
        r_start(q, h, at, direction, slot_of(first, 2), place(h, 0, by))
        to_partner(q, h, at, 0)

    def r_second_opposite(q, first, h):
        at = place(h, first, 2)
        r_wait(q, h, at, slot_of(first, 2))
        to_partner(q, h, at, 1)

    FIRSTS = (0, -1, 1, 2)

    def product(k, by, start, size, columns):
        return jnp.dot(
            a_buf[a_part(shift(x, k), by, start, size), :],
            r_buf[rows_at(shift(x, k) * depth, depth), columns],
            preferred_element_type=jnp.float32,
        )

    def unit(k, by, mode, start=0, size=None):
        size = quarter if size is None else size
        out_rows = rows_at(shift(x, by) * quarter + start, size, 32)

        def step(j, carry):
            columns = pl.ds(pl.multiple_of(j * TILE_N, TILE_N), TILE_N)
            value = product(k, by, start, size, columns)
            if mode != "set":
                value = value + c_buf[out_rows, columns]
            c_buf[out_rows, columns] = value
            if mode == "last":
                sq_sum[:, columns] += jnp.sum(value * value, axis=0, keepdims=True)
            return carry

        lax.fori_loop(0, cols // TILE_N, step, 0)

    def ext_value(h, mt, k):
        half_rows = quarter // 2
        if h == 0:
            block = shift(z, k)
            return jnp.dot(
                a_buf[a_part(block, -1, mt * half_rows, half_rows), :],
                r2_buf[rows_at(block * depth, depth), :],
                preferred_element_type=jnp.float32,
            )
        yy = shift(y, k)
        total = None
        for zz in range(SIDE):
            value = jnp.dot(
                a_buf[a_part(zz, 1, mt * half_rows, half_rows), pl.ds(pl.multiple_of(yy * chip, 128), chip)],
                r2_buf[rows_at(k_all + (zz * SIDE + yy) * chip, chip), :],
                preferred_element_type=jnp.float32,
            )
            total = value if total is None else total + value
        return total

    def ext_unit(h, k, mode):
        half_rows = quarter // 2

        def step(mt, carry):
            part = rows_at(mt * half_rows, half_rows)
            value = ext_value(h, mt, k)
            if mode != "set":
                value = value + ext[h, part, :]
            ext[h, part, :] = value
            if mode == "last":
                columns = pl.ds(h * side_cols, side_cols)
                sq_out[:, columns] += jnp.sum(value * value, axis=0, keepdims=True)
            return carry

        lax.fori_loop(0, 2, step, 0)

    def ext_copy(h):
        by = 1 - 2 * h
        dst = c_buf.at[rows_at(shift(x, -by) * quarter, quarter, 64), pl.ds(h * side_cols, side_cols)]
        return remote(ext.at[h], dst, sem["e_send"], sem["e_recv"], g, shift(x, by))

    def sq_ext_copy(h):
        columns = pl.ds(h * side_cols, side_cols)
        return remote(
            sq_out.at[:, columns], sq_in.at[:, columns], sem["q_send"], sem["q_recv"], g, shift(x, 1 - 2 * h)
        )

    own_rot.wait()
    for h in (0, 1):
        remote(
            r_buf.at[piece_rows(own, core), pl.ds(h * side_cols, side_cols)], r_ref(1, h, own, None, core),
            sem["x_send"], sem["x_recv"], g, shift(x, 2 * h - 1),
        ).start()
    r_own_first(0)
    own_coef.wait()
    for i in range(3):
        for direction in (0, 1):
            a_start(direction, i)
    r_own_second(0)
    sq_sum[...] = jnp.zeros_like(sq_sum)
    sq_out[...] = jnp.zeros_like(sq_out)
    r_first(0)
    for h in (0, 1):
        r_opposite(0, h)
    for first in FIRSTS:
        for direction in (0, 1):
            for h in (0, 1):
                r_second(0, first, direction, h)
    two = r2_buf.at[pl.ds(0, 2 * piece), :]
    remote(two, two, sem["x_send"], sem["x_recv"], g, shift(x, 1)).wait()
    r_own_first(1)
    r_own_second(1)
    for direction in (0, 1):
        a_wait(direction, 0)
        relay_start(direction)
    for first in FIRSTS:
        for h in (0, 1):
            r_second_opposite(0, first, h)
    for direction in (0, 1):
        a_wait(direction, 1)
        for c in range(len(LAST)):
            last_start(direction, c)
    pieces = SIDE * SIDE * piece
    ref = r_buf.at[pl.ds(0, pieces), :]
    remote(ref, ref, sem["p_send"], sem["p_recv"], partner, x).wait()

    unit(0, 0, "set")
    unit(0, 1, "set")
    r_first(1)
    unit(0, -1, "set")
    for k in (-1, 1):
        unit(k, 0, "add")
    r_opposite(1, 0)
    for k in (-1, 1):
        unit(k, -k, "add")
    r_opposite(1, 1)
    for first in FIRSTS:
        for direction in (0, 1):
            for h in (0, 1):
                r_second(1, first, direction, h)
        if first == 0:
            for direction, k in enumerate((-1, 1)):
                a_wait(direction, 2)
                unit(k, k, "add")
    for direction in (0, 1):
        relay_wait(direction)
    early = r2_buf.at[pl.ds(0, 12 * piece), :]
    for h in (0, 1):
        remote(early, early, sem["p2_send"], sem["p_recv%d0" % h], partner, x).wait_recv()
        for k in (0, -1, 1):
            ext_unit(h, k, "set" if k == 0 else "add")
    for h in (0, 1):
        for first in FIRSTS:
            r_second_opposite(1, first, h)
    late = r2_buf.at[pl.ds(0, 4 * piece), :]
    for h in (0, 1):
        remote(late, late, sem["p2_send"], sem["p_recv%d1" % h], partner, x).wait_recv()
        ext_unit(h, 2, "last")
    for h in (0, 1):
        sq_ext_copy(h).start()
    for h in (0, 1):
        ext_copy(h).start()
    for by in (-1, 1):
        unit(2, by, "last")
    for c in range(len(LAST)):
        last_wait(c)
        unit(2, 0, "last", last_starts[c], LAST[c])
    remote(sq_out, sq_in, sem["q_send"], sem["q_recv"], g, shift(x, 1)).wait()

    sq_buf[g] = sq_sum[...] + sq_in[...]
    others = [(dz, dy, dc) for dz in range(-1, 3) for dy in range(-1, 3) for dc in (0, 1) if (dz, dy, dc) != (0, 0, 0)]
    for dz, dy, dc in sorted(others, key=lambda by: -(abs(by[0]) + abs(by[1]))):
        peer = device_of(shift(z, dz), shift(y, dy), (core + dc) % 2)
        remote(sq_buf.at[g], sq_buf.at[g], sem["s_send"], sem["s_recv"], peer, x).start()
    ref = a_buf.at[pl.ds(0, 9 * quarter), :]
    remote(ref, ref, sem["a_send"], sem["e_recv"], g, shift(x, 1)).wait_send()
    ref = r_buf.at[pl.ds(0, 15 * piece), :]
    remote(ref, ref, sem["r_send"], sem["e_recv"], partner, x).wait_send()
    ref = r2_buf.at[pl.ds(0, 30 * piece), :]
    remote(ref, ref, sem["r2_send"], sem["e_recv"], partner, x).wait_send()
    ref = r2_buf.at[pl.ds(0, 32 * piece), :]
    remote(ref, ref, sem["p2_send"], sem["e_recv"], partner, x).wait_send()
    ref = sq_buf.at[pl.ds(0, peers - 1)]
    remote(ref, ref, sem["s_send"], sem["s_recv"], partner, x).wait()
    remote(ext, ext, sem["e_send"], sem["e_recv"], g, shift(x, 1)).wait()


def normalize(c_buf, sq_buf, out, rms_out, scale, staged, out_sem):
    rows, cols = c_buf.shape
    chunk = rows // CHUNKS
    total = sq_buf[0]
    for i in range(1, sq_buf.shape[0]):
        total = total + sq_buf[i]
    rms = jnp.sqrt(total / TOTAL_ROWS + 1e-06)
    rms_out[...] = rms.reshape(cols)
    scale[...] = 1.0 / rms

    def out_copy(c):
        part = pl.ds(c * chunk, chunk)
        return pltpu.make_async_copy(staged.at[part, :], out.at[part, :], out_sem.at[c])

    for c in range(CHUNKS):
        part = pl.ds(c * chunk, chunk)
        staged[part, :] = (c_buf[part, :] * scale[...]).astype(jnp.bfloat16)
        out_copy(c).start()
    for c in range(CHUNKS):
        out_copy(c).wait()


def body(coefficients, rotation):
    rows, depth = coefficients.shape
    piece, cols = rotation.shape
    peers = lax.axis_size("ga")
    dma = pltpu.SemaphoreType.DMA
    rotated, squares = pl.pallas_call(
        gather_multiply,
        out_shape=(pltpu.VMEM((rows, cols), jnp.float32), pltpu.VMEM((peers, 1, cols), jnp.float32)),
        in_specs=[pl.BlockSpec(memory_space=pl.ANY)] * 2,
        out_specs=(pl.BlockSpec(memory_space=pltpu.VMEM), pl.BlockSpec(memory_space=pltpu.VMEM)),
        scratch_shapes=[
            pltpu.VMEM((SIDE * rows, depth), jnp.bfloat16),
            pltpu.VMEM((SIDE * depth, cols), jnp.bfloat16),
            pltpu.VMEM((2 * SIDE * depth, cols // 2), jnp.bfloat16),
            pltpu.VMEM((2, rows // SIDE, cols // 2), jnp.float32),
            pltpu.VMEM((1, cols), jnp.float32),
            pltpu.VMEM((1, cols), jnp.float32),
            pltpu.VMEM((1, cols), jnp.float32),
            dma((2,)),
            dma((2, 3)),
            dma((2,)),
            dma((len(LAST),)),
            dma((2, 15)),
            dma((2, 15)),
            dma((len(SEMS),)),
        ],
        compiler_params=pltpu.CompilerParams(
            collective_id=0, has_side_effects=True, vmem_limit_bytes=55 * 1024 * 1024
        ),
        cost_estimate=pl.CostEstimate(
            flops=2 * rows * depth * SIDE * cols, bytes_accessed=4 * rows * depth, transcendentals=0
        ),
    )(coefficients, rotation)
    return pl.pallas_call(
        normalize,
        out_shape=(
            jax.ShapeDtypeStruct((rows, cols), jnp.bfloat16),
            jax.ShapeDtypeStruct((cols,), jnp.float32),
        ),
        in_specs=[pl.BlockSpec(memory_space=pltpu.VMEM)] * 2,
        out_specs=(pl.BlockSpec(memory_space=pl.ANY), pl.BlockSpec(memory_space=pltpu.VMEM)),
        scratch_shapes=[
            pltpu.VMEM((1, cols), jnp.float32),
            pltpu.VMEM((rows, cols), jnp.bfloat16),
            dma((CHUNKS,)),
        ],
        compiler_params=pltpu.CompilerParams(vmem_limit_bytes=20 * 1024 * 1024),
        cost_estimate=pl.CostEstimate(flops=rows * cols, bytes_accessed=6 * rows * cols, transcendentals=0),
    )(rotated, squares)


def solution(mesh):
    return jax.shard_map(
        body, mesh=mesh, in_specs=(P("ga", "ba"), P("ga", "ba")), out_specs=(P("ga", "ba"), P("ba")), check_vma=False
    )
```

```python
import jax
import jax.numpy as jnp
from jax import lax
from jax.experimental import pallas as pl
from jax.experimental.pallas import tpu as pltpu
from jax.sharding import PartitionSpec as P

MESH = pl.DeviceIdType.MESH
SIDE = 4
LAST = (320,)
WIDE = 128
TILE_N = 768
EXT_M = 160
TOTAL_ROWS = 40960
SENDS = ("a_send", "r_send", "r2_send", "p_send", "p2_send", "x_send", "e_send", "q_send", "s_send", "n_send", "b_send")
ARRIVALS = ("x_recv", "e_recv", "q_recv", "s_recv", "n_recv", "b_recv", "p_recv", "p_recv00", "p_recv01", "p_recv10", "p_recv11")
SEMS = {name: i for i, name in enumerate(SENDS + ARRIVALS)}


def gather_multiply(
    coef, rot, c_buf, rms_out, scale, narrow, a_buf, r_buf, r2_buf, ext, sq_buf, sq_sum, sq_out, sq_in, scale_in,
    load_sem, a_sem, relay_sem, last_sem, r_sem, r2_sem, sems,
):
    rows, depth = coef.shape
    piece, cols = rot.shape
    peers = 2 * SIDE * SIDE
    quarter = rows // SIDE
    side_cols = cols // 2
    k_all = peers * piece
    chip = 2 * piece

    g = lax.axis_index("ga")
    x = lax.axis_index("ba")
    core = g % 2
    y = (g // 2) % SIDE
    z = g // (2 * SIDE)
    sem = {name: sems.at[i] for name, i in SEMS.items()}

    def shift(value, by):
        return (value + by + SIDE) % SIDE

    def device_of(zz, yy, cc):
        return (zz * SIDE + yy) * 2 + cc

    partner = device_of(z, y, 1 - core)

    def rows_at(start, size, align=16):
        return pl.ds(pl.multiple_of(start, align), size)

    def a_part(block, by, start=0, size=None):
        at = block * rows + shift(x, by) * quarter + start
        return rows_at(at, quarter if size is None else size, 32)

    def piece_rows(at, cc, start=0, size=None):
        return rows_at(device_of(at[0], at[1], cc) * piece + start, piece if size is None else size)

    own = (z, y)

    own_rot = pltpu.make_async_copy(rot, r_buf.at[piece_rows(own, core), :], load_sem.at[1])
    own_rot.start()
    own_coef = pltpu.make_async_copy(coef, a_buf.at[rows_at(x * rows, rows), :], load_sem.at[0])
    own_coef.start()

    barrier = pltpu.get_barrier_semaphore()
    near = [(device_of(shift(z, by), y, core), x) for by in (1, -1)]
    near += [(device_of(z, shift(y, by), core), x) for by in (1, -1)]
    near += [(g, shift(x, by)) for by in (1, -1)]
    near += [(partner, x)]
    for ga, ba in near:
        pl.semaphore_signal(barrier, inc=1, device_id={"ga": ga, "ba": ba}, device_id_type=MESH)
    pl.semaphore_wait(barrier, len(near))

    def remote(src, dst, send, recv, ga, ba):
        return pltpu.make_async_remote_copy(
            src_ref=src, dst_ref=dst, send_sem=send, recv_sem=recv,
            device_id={"ga": ga, "ba": ba}, device_id_type=MESH,
        )

    order = lambda by: (by, 2, 0)

    def a_move(part, recv, to):
        ref = a_buf.at[part, :]
        return remote(ref, ref, sem["a_send"], recv, g, to)

    def a_start(direction, i):
        by = 1 - 2 * direction
        a_move(a_part(x, order(by)[i]), a_sem.at[direction, i], shift(x, by)).start()

    def a_wait(direction, i):
        by = 1 - 2 * direction
        a_move(a_part(shift(x, -by), order(by)[i] - by), a_sem.at[direction, i], shift(x, by)).wait_recv()

    def relay_start(direction):
        by = 1 - 2 * direction
        a_move(a_part(shift(x, -by), 0), relay_sem.at[direction], shift(x, by)).start()

    def relay_wait(direction):
        by = 1 - 2 * direction
        a_move(a_part(shift(x, 2), -by), relay_sem.at[direction], shift(x, by)).wait_recv()

    last_starts = [sum(LAST[:c]) for c in range(len(LAST))]

    def last_start(direction, c):
        by = 1 - 2 * direction
        size = LAST[c] // 2
        part = a_part(shift(x, -by), by, last_starts[c] + direction * size, size)
        a_move(part, last_sem.at[c], shift(x, by)).start()

    def last_wait(c):
        a_move(a_part(shift(x, 2), 0, last_starts[c], LAST[c]), last_sem.at[c], shift(x, 1)).wait_recv()

    def place(h, first, second):
        return (shift(z, second), shift(y, first)) if h == 0 else (shift(z, first), shift(y, second))

    def r_ref(q, h, at, part, cc):
        if q == 0:
            size = piece // 2
            start = h * size
            ref = r_buf
            if part is not None:
                size = size // 2
                start = start + part * size
            return ref.at[piece_rows(at, cc, start, size), :]
        size, start = piece, h * k_all
        if part is not None:
            size = size // 2
            start = start + part * size
        return r2_buf.at[piece_rows(at, cc, start, size), :]

    def r_start(q, h, at, part, slot, to):
        ref = r_ref(q, h, at, part, core)
        recv = (r_sem if q == 0 else r2_sem).at[h, slot]
        remote(ref, ref, sem["r_send"] if q == 0 else sem["r2_send"], recv, device_of(to[0], to[1], core), x).start()

    def r_wait(q, h, at, slot):
        ref = r_ref(q, h, at, None, core)
        recv = (r_sem if q == 0 else r2_sem).at[h, slot]
        remote(ref, ref, sem["r_send"], recv, partner, x).wait_recv()

    def to_partner(q, h, at, late):
        ref = r_ref(q, h, at, None, core)
        recv = sem["p_recv"] if q == 0 else sem["p_recv%d%d" % (h, late)]
        remote(ref, ref, sem["p_send"] if q == 0 else sem["p2_send"], recv, partner, x).start()

    places = {0: 0, -1: 1, 1: 2, 2: 3}

    def slot_of(first, kind):
        return 3 + 3 * places[first] + kind

    def along_second(q, h, at, first):
        for direction in (0, 1):
            r_start(q, h, at, None, slot_of(first, direction), place(h, 0, 1 - 2 * direction))

    def r_own_first(q):
        for h in (0, 1):
            for direction in (0, 1):
                r_start(q, h, own, None, direction, place(h, 1 - 2 * direction, 0))

    def r_own_second(q):
        for h in (0, 1):
            along_second(q, h, own, 0)
            to_partner(q, h, own, 0)

    def r_first(q):
        for direction in (0, 1):
            by = 1 - 2 * direction
            for h in (0, 1):
                at = place(h, -by, 0)
                r_wait(q, h, at, direction)
                r_start(q, h, at, direction, 2, place(h, by, 0))
        for by in (1, -1):
            for h in (0, 1):
                at = place(h, -by, 0)
                along_second(q, h, at, -by)
                to_partner(q, h, at, 0)

    def r_opposite(q, h):
        at = place(h, 2, 0)
        r_wait(q, h, at, 2)
        along_second(q, h, at, 2)
        to_partner(q, h, at, 0)

    def r_second(q, first, direction, h):
        by = 1 - 2 * direction
        at = place(h, first, -by)
        r_wait(q, h, at, slot_of(first, direction))
        r_start(q, h, at, direction, slot_of(first, 2), place(h, 0, by))
        to_partner(q, h, at, 0)

    def r_second_opposite(q, first, h):
        at = place(h, first, 2)
        r_wait(q, h, at, slot_of(first, 2))
        to_partner(q, h, at, 1)

    FIRSTS = (0, -1, 1, 2)

    def product(k, by, start, size, columns):
        return jnp.dot(
            a_buf[a_part(shift(x, k), by, start, size), :],
            r_buf[rows_at(shift(x, k) * depth, depth), columns],
            preferred_element_type=jnp.float32,
        )

    def unit(k, by, mode, start=0, size=None):
        size = quarter if size is None else size
        out_rows = rows_at(shift(x, by) * quarter + start, size, 32)

        def step(j, carry):
            columns = pl.ds(pl.multiple_of(j * TILE_N, TILE_N), TILE_N)
            value = product(k, by, start, size, columns)
            if mode != "set":
                value = value + c_buf[out_rows, columns]
            c_buf[out_rows, columns] = value
            if mode == "last":
                sq_sum[:, columns] += jnp.sum(value * value, axis=0, keepdims=True)
            return carry

        lax.fori_loop(0, cols // TILE_N, step, 0)

    delta = (x + 2 - z + SIDE) % SIDE
    low = 1 - delta // 2
    early_blocks = ((3 - delta) // 3, 1 + 2 * low)
    late_blocks = (delta * low + 3 * (1 - low), 2)

    def ext_dot_0(start, block):
        return jnp.dot(
            a_buf[a_part(block, -1, start, EXT_M), :],
            r2_buf[rows_at(block * depth, depth), :],
            preferred_element_type=jnp.float32,
        )

    def ext_dot_1(start, pairs):
        total = None
        for zz, yy in pairs:
            value = jnp.dot(
                a_buf[a_part(zz, 1, start, EXT_M), pl.ds(pl.multiple_of(yy * chip, 128), chip)],
                r2_buf[rows_at(k_all + (zz * SIDE + yy) * chip, chip), :],
                preferred_element_type=jnp.float32,
            )
            total = value if total is None else total + value
        return total

    def ext_unit(h, dot, what, mode):
        def step(i, carry):
            start = pl.multiple_of(i * EXT_M, EXT_M)
            part = pl.ds(start, EXT_M)
            value = dot(start, what)
            if mode != "set":
                value = value + ext[h, part, :]
            ext[h, part, :] = value
            if mode == "last":
                columns = pl.ds(h * side_cols, side_cols)
                sq_out[:, columns] += jnp.sum(value * value, axis=0, keepdims=True)
            return carry

        lax.fori_loop(0, quarter // EXT_M, step, 0)

    def ext_early(h):
        if h == 0:
            for i, k in enumerate(early_blocks):
                ext_unit(0, ext_dot_0, shift(z, k), "set" if i == 0 else "add")
        else:
            for i, k in enumerate((0, -1, 1)):
                pairs = [(shift(x, b), shift(y, k)) for b in (0, -1, 1)]
                ext_unit(1, ext_dot_1, pairs, "set" if i == 0 else "add")

    def ext_late(h):
        if h == 0:
            for i, k in enumerate(late_blocks):
                ext_unit(0, ext_dot_0, shift(z, k), "add" if i == 0 else "last")
        else:
            pairs = [(shift(x, 2), shift(y, k)) for k in (0, -1, 1)] + [(zz, shift(y, 2)) for zz in range(SIDE)]
            ext_unit(1, ext_dot_1, pairs, "last")

    def ext_copy(h):
        by = 1 - 2 * h
        dst = c_buf.at[rows_at(shift(x, -by) * quarter, WIDE, 64), pl.ds(h * side_cols, side_cols)]
        return remote(ext.at[h, pl.ds(0, WIDE), :], dst, sem["e_send"], sem["e_recv"], g, shift(x, by))

    def rounded(h, count=1):
        return r2_buf.at[pl.ds(h * (quarter - WIDE), count * (quarter - WIDE)), :]

    def rounded_copy(h):
        dst = narrow.at[:, pl.ds(h * side_cols, side_cols)]
        return remote(rounded(h), dst, sem["b_send"], sem["b_recv"], g, shift(x, 1 - 2 * h))

    def scale_copy(h):
        columns = pl.ds(h * side_cols, side_cols)
        return remote(
            scale.at[:, columns], scale_in.at[:, columns], sem["n_send"], sem["n_recv"], g, shift(x, 2 * h - 1)
        )

    def sq_ext_copy(h):
        columns = pl.ds(h * side_cols, side_cols)
        return remote(
            sq_out.at[:, columns], sq_in.at[:, columns], sem["q_send"], sem["q_recv"], g, shift(x, 1 - 2 * h)
        )

    own_rot.wait()
    for h in (0, 1):
        remote(
            r_buf.at[piece_rows(own, core), pl.ds(h * side_cols, side_cols)], r_ref(1, h, own, None, core),
            sem["x_send"], sem["x_recv"], g, shift(x, 2 * h - 1),
        ).start()
    r_own_first(0)
    own_coef.wait()
    for i in range(3):
        for direction in (0, 1):
            a_start(direction, i)
    r_own_second(0)
    sq_sum[...] = jnp.zeros_like(sq_sum)
    sq_out[...] = jnp.zeros_like(sq_out)
    r_first(0)
    for h in (0, 1):
        r_opposite(0, h)
    for first in FIRSTS:
        for direction in (0, 1):
            for h in (0, 1):
                r_second(0, first, direction, h)
    two = r2_buf.at[pl.ds(0, 2 * piece), :]
    remote(two, two, sem["x_send"], sem["x_recv"], g, shift(x, 1)).wait()
    r_own_first(1)
    r_own_second(1)
    for direction in (0, 1):
        a_wait(direction, 0)
        relay_start(direction)
    for first in FIRSTS:
        for h in (0, 1):
            r_second_opposite(0, first, h)
    for direction in (0, 1):
        a_wait(direction, 1)
        for c in range(len(LAST)):
            last_start(direction, c)
    pieces = SIDE * SIDE * piece
    ref = r_buf.at[pl.ds(0, pieces), :]
    remote(ref, ref, sem["p_send"], sem["p_recv"], partner, x).wait()

    unit(0, 0, "set")
    unit(0, 1, "set")
    r_first(1)
    unit(0, -1, "set")
    for k in (-1, 1):
        unit(k, 0, "add")
    r_opposite(1, 0)
    for k in (-1, 1):
        unit(k, -k, "add")
    r_opposite(1, 1)
    for first in FIRSTS:
        for direction in (0, 1):
            for h in (0, 1):
                r_second(1, first, direction, h)
        if first == 0:
            for direction, k in enumerate((-1, 1)):
                a_wait(direction, 2)
                unit(k, k, "add")
    early = r2_buf.at[pl.ds(0, 12 * piece), :]
    for h in (0, 1):
        remote(early, early, sem["p2_send"], sem["p_recv%d0" % h], partner, x).wait_recv()
        ext_early(h)
    for direction, by in enumerate((-1, 1)):
        relay_wait(direction)
        unit(2, by, "last")
        for first in FIRSTS[2 * direction:2 * direction + 2]:
            for h in (0, 1):
                r_second_opposite(1, first, h)
    late = r2_buf.at[pl.ds(0, 4 * piece), :]
    for h in (0, 1):
        remote(late, late, sem["p2_send"], sem["p_recv%d1" % h], partner, x).wait_recv()
        ext_late(h)
        sq_ext_copy(h).start()
    for h in (0, 1):
        ext_copy(h).start()
    for c in range(len(LAST)):
        last_wait(c)
        unit(2, 0, "last", last_starts[c], LAST[c])
    remote(sq_out, sq_in, sem["q_send"], sem["q_recv"], g, shift(x, 1)).wait()

    sq_buf[g] = sq_sum[...] + sq_in[...]
    others = [(dz, dy, dc) for dz in range(-1, 3) for dy in range(-1, 3) for dc in (0, 1) if (dz, dy, dc) != (0, 0, 0)]
    for dz, dy, dc in sorted(others, key=lambda by: -(abs(by[0]) + abs(by[1]))):
        peer = device_of(shift(z, dz), shift(y, dy), (core + dc) % 2)
        remote(sq_buf.at[g], sq_buf.at[g], sem["s_send"], sem["s_recv"], peer, x).start()
    ref = a_buf.at[pl.ds(0, 9 * quarter), :]
    remote(ref, ref, sem["a_send"], sem["e_recv"], g, shift(x, 1)).wait_send()
    ref = r_buf.at[pl.ds(0, 15 * piece), :]
    remote(ref, ref, sem["r_send"], sem["e_recv"], partner, x).wait_send()
    ref = r2_buf.at[pl.ds(0, 30 * piece), :]
    remote(ref, ref, sem["r2_send"], sem["e_recv"], partner, x).wait_send()
    ref = r2_buf.at[pl.ds(0, 32 * piece), :]
    remote(ref, ref, sem["p2_send"], sem["e_recv"], partner, x).wait_send()
    ref = sq_buf.at[pl.ds(0, peers - 1)]
    remote(ref, ref, sem["s_send"], sem["s_recv"], partner, x).wait()
    total = sq_buf[0]
    for i in range(1, peers):
        total = total + sq_buf[i]
    rms = jnp.sqrt(total / TOTAL_ROWS + 1e-06)
    rms_out[...] = rms
    scale[...] = 1.0 / rms
    for h in (0, 1):
        scale_copy(h).start()
    remote(scale, scale_in, sem["n_send"], sem["n_recv"], g, shift(x, 1)).wait()
    for h in (0, 1):
        rounded(h)[...] = (ext[h, WIDE:, :] * scale_in[:, h * side_cols:(h + 1) * side_cols]).astype(jnp.bfloat16)
        rounded_copy(h).start()
    ref = ext.at[:, pl.ds(0, WIDE), :]
    remote(ref, ref, sem["e_send"], sem["e_recv"], g, shift(x, 1)).wait()
    remote(rounded(0, 2), rounded(0, 2), sem["b_send"], sem["b_recv"], g, shift(x, 1)).wait()


def normalize(c_buf, rms_in, scale, narrow, out, rms_out, staged, out_sem):
    rows, cols = c_buf.shape
    quarter = rows // SIDE
    x = lax.axis_index("ba")
    rms_out[...] = rms_in[...].reshape(cols)
    copies = []

    def put(src, start, size):
        part = pl.ds(pl.multiple_of(start, 64), size)
        copy = pltpu.make_async_copy(src, out.at[part, :], out_sem.at[len(copies)])
        copy.start()
        copies.append(copy)

    def opposite(by):
        return (x + by) % SIDE * quarter

    put(narrow, opposite(2) + WIDE, quarter - WIDE)
    at = 0
    for by, start, size in [(2, 0, WIDE)] + [(by, start, 64) for by in (0, 1, 3) for start in range(0, quarter, 64)]:
        part = pl.ds(pl.multiple_of(opposite(by) + start, 64), size)
        staged[pl.ds(at, size), :] = (c_buf[part, :] * scale[...]).astype(jnp.bfloat16)
        put(staged.at[pl.ds(at, size), :], opposite(by) + start, size)
        at += size
    for copy in copies:
        copy.wait()


def body(coefficients, rotation):
    rows, depth = coefficients.shape
    piece, cols = rotation.shape
    peers = lax.axis_size("ga")
    dma = pltpu.SemaphoreType.DMA
    row = pltpu.VMEM((1, cols), jnp.float32)
    parts = pl.pallas_call(
        gather_multiply,
        out_shape=(
            pltpu.VMEM((rows, cols), jnp.float32), row, row,
            pltpu.VMEM((rows // SIDE - WIDE, cols), jnp.bfloat16),
        ),
        in_specs=[pl.BlockSpec(memory_space=pl.ANY)] * 2,
        out_specs=(pl.BlockSpec(memory_space=pltpu.VMEM),) * 4,
        scratch_shapes=[
            pltpu.VMEM((SIDE * rows, depth), jnp.bfloat16),
            pltpu.VMEM((SIDE * depth, cols), jnp.bfloat16),
            pltpu.VMEM((2 * SIDE * depth, cols // 2), jnp.bfloat16),
            pltpu.VMEM((2, rows // SIDE, cols // 2), jnp.float32),
            pltpu.VMEM((peers, 1, cols), jnp.float32),
            row,
            row,
            row,
            row,
            dma((2,)),
            dma((2, 3)),
            dma((2,)),
            dma((len(LAST),)),
            dma((2, 15)),
            dma((2, 15)),
            dma((len(SEMS),)),
        ],
        compiler_params=pltpu.CompilerParams(
            collective_id=0, has_side_effects=True, vmem_limit_bytes=55 * 1024 * 1024
        ),
        cost_estimate=pl.CostEstimate(
            flops=2 * rows * depth * SIDE * cols, bytes_accessed=4 * rows * depth, transcendentals=0
        ),
    )(coefficients, rotation)
    return pl.pallas_call(
        normalize,
        out_shape=(
            jax.ShapeDtypeStruct((rows, cols), jnp.bfloat16),
            jax.ShapeDtypeStruct((cols,), jnp.float32),
        ),
        in_specs=[pl.BlockSpec(memory_space=pltpu.VMEM)] * 4,
        out_specs=(pl.BlockSpec(memory_space=pl.ANY), pl.BlockSpec(memory_space=pltpu.VMEM)),
        scratch_shapes=[
            pltpu.VMEM((rows, cols), jnp.bfloat16),
            dma((20,)),
        ],
        compiler_params=pltpu.CompilerParams(vmem_limit_bytes=20 * 1024 * 1024),
        cost_estimate=pl.CostEstimate(flops=rows * cols, bytes_accessed=6 * rows * cols, transcendentals=0),
    )(*parts)


def solution(mesh):
    return jax.shard_map(
        body, mesh=mesh, in_specs=(P("ga", "ba"), P("ga", "ba")), out_specs=(P("ga", "ba"), P("ba")), check_vma=False
    )
```

```python
import jax
import jax.numpy as jnp
from jax import lax
from jax.experimental import pallas as pl
from jax.experimental.pallas import tpu as pltpu
from jax.sharding import PartitionSpec as P

MESH = pl.DeviceIdType.MESH
SIDE = 4
LAST = (320,)
FIRST_WIDE, WIDE = 128, 176
TILE_N = 768
EXT_M = 160
TOTAL_ROWS = 40960
SENDS = ("a_send", "r_send", "r2_send", "p_send", "p2_send", "x_send", "e_send", "q_send", "s_send", "n_send", "b_send")
ARRIVALS = ("x_recv", "e_recv", "q_recv", "s_recv", "n_recv", "b_recv", "p_recv", "p_recv00", "p_recv01", "p_recv10", "p_recv11")
SEMS = {name: i for i, name in enumerate(SENDS + ARRIVALS)}


def gather_multiply(
    coef, rot, c_buf, rms_out, scale, narrow, a_buf, r_buf, r2_buf, ext, sq_buf, sq_sum, sq_out, sq_in, scale_in,
    load_sem, a_sem, relay_sem, last_sem, r_sem, r2_sem, sems,
):
    rows, depth = coef.shape
    piece, cols = rot.shape
    peers = 2 * SIDE * SIDE
    quarter = rows // SIDE
    side_cols = cols // 2
    k_all = peers * piece
    chip = 2 * piece

    g = lax.axis_index("ga")
    x = lax.axis_index("ba")
    core = g % 2
    y = (g // 2) % SIDE
    z = g // (2 * SIDE)
    sem = {name: sems.at[i] for name, i in SEMS.items()}

    def shift(value, by):
        return (value + by + SIDE) % SIDE

    def device_of(zz, yy, cc):
        return (zz * SIDE + yy) * 2 + cc

    partner = device_of(z, y, 1 - core)

    def rows_at(start, size, align=16):
        return pl.ds(pl.multiple_of(start, align), size)

    def a_part(block, by, start=0, size=None):
        at = block * rows + shift(x, by) * quarter + start
        return rows_at(at, quarter if size is None else size, 32)

    def piece_rows(at, cc, start=0, size=None):
        return rows_at(device_of(at[0], at[1], cc) * piece + start, piece if size is None else size)

    own = (z, y)

    own_rot = pltpu.make_async_copy(rot, r_buf.at[piece_rows(own, core), :], load_sem.at[1])
    own_rot.start()
    own_coef = pltpu.make_async_copy(coef, a_buf.at[rows_at(x * rows, rows), :], load_sem.at[0])
    own_coef.start()

    barrier = pltpu.get_barrier_semaphore()
    near = [(device_of(shift(z, by), y, core), x) for by in (1, -1)]
    near += [(device_of(z, shift(y, by), core), x) for by in (1, -1)]
    near += [(g, shift(x, by)) for by in (1, -1)]
    near += [(partner, x)]
    for ga, ba in near:
        pl.semaphore_signal(barrier, inc=1, device_id={"ga": ga, "ba": ba}, device_id_type=MESH)
    pl.semaphore_wait(barrier, len(near))

    def remote(src, dst, send, recv, ga, ba):
        return pltpu.make_async_remote_copy(
            src_ref=src, dst_ref=dst, send_sem=send, recv_sem=recv,
            device_id={"ga": ga, "ba": ba}, device_id_type=MESH,
        )

    order = lambda by: (by, 2, 0)

    def a_move(part, recv, to):
        ref = a_buf.at[part, :]
        return remote(ref, ref, sem["a_send"], recv, g, to)

    def a_start(direction, i):
        by = 1 - 2 * direction
        a_move(a_part(x, order(by)[i]), a_sem.at[direction, i], shift(x, by)).start()

    def a_wait(direction, i):
        by = 1 - 2 * direction
        a_move(a_part(shift(x, -by), order(by)[i] - by), a_sem.at[direction, i], shift(x, by)).wait_recv()

    def relay_start(direction):
        by = 1 - 2 * direction
        a_move(a_part(shift(x, -by), 0), relay_sem.at[direction], shift(x, by)).start()

    def relay_wait(direction):
        by = 1 - 2 * direction
        a_move(a_part(shift(x, 2), -by), relay_sem.at[direction], shift(x, by)).wait_recv()

    last_starts = [sum(LAST[:c]) for c in range(len(LAST))]

    def last_start(direction, c):
        by = 1 - 2 * direction
        size = LAST[c] // 2
        part = a_part(shift(x, -by), by, last_starts[c] + direction * size, size)
        a_move(part, last_sem.at[c], shift(x, by)).start()

    def last_wait(c):
        a_move(a_part(shift(x, 2), 0, last_starts[c], LAST[c]), last_sem.at[c], shift(x, 1)).wait_recv()

    def place(h, first, second):
        return (shift(z, second), shift(y, first)) if h == 0 else (shift(z, first), shift(y, second))

    def r_ref(q, h, at, part, cc):
        if q == 0:
            size = piece // 2
            start = h * size
            ref = r_buf
            if part is not None:
                size = size // 2
                start = start + part * size
            return ref.at[piece_rows(at, cc, start, size), :]
        size, start = piece, h * k_all
        if part is not None:
            size = size // 2
            start = start + part * size
        return r2_buf.at[piece_rows(at, cc, start, size), :]

    def r_start(q, h, at, part, slot, to):
        ref = r_ref(q, h, at, part, core)
        recv = (r_sem if q == 0 else r2_sem).at[h, slot]
        remote(ref, ref, sem["r_send"] if q == 0 else sem["r2_send"], recv, device_of(to[0], to[1], core), x).start()

    def r_wait(q, h, at, slot):
        ref = r_ref(q, h, at, None, core)
        recv = (r_sem if q == 0 else r2_sem).at[h, slot]
        remote(ref, ref, sem["r_send"], recv, partner, x).wait_recv()

    def to_partner(q, h, at, late):
        ref = r_ref(q, h, at, None, core)
        recv = sem["p_recv"] if q == 0 else sem["p_recv%d%d" % (h, late)]
        remote(ref, ref, sem["p_send"] if q == 0 else sem["p2_send"], recv, partner, x).start()

    places = {0: 0, -1: 1, 1: 2, 2: 3}

    def slot_of(first, kind):
        return 3 + 3 * places[first] + kind

    def along_second(q, h, at, first):
        for direction in (0, 1):
            r_start(q, h, at, None, slot_of(first, direction), place(h, 0, 1 - 2 * direction))

    def r_own_first(q):
        for h in (0, 1):
            for direction in (0, 1):
                r_start(q, h, own, None, direction, place(h, 1 - 2 * direction, 0))

    def r_own_second(q):
        for h in (0, 1):
            along_second(q, h, own, 0)
            to_partner(q, h, own, 0)

    def r_first(q):
        for direction in (0, 1):
            by = 1 - 2 * direction
            for h in (0, 1):
                at = place(h, -by, 0)
                r_wait(q, h, at, direction)
                r_start(q, h, at, direction, 2, place(h, by, 0))
        for by in (1, -1):
            for h in (0, 1):
                at = place(h, -by, 0)
                along_second(q, h, at, -by)
                to_partner(q, h, at, 0)

    def r_opposite(q, h):
        at = place(h, 2, 0)
        r_wait(q, h, at, 2)
        along_second(q, h, at, 2)
        to_partner(q, h, at, 0)

    def r_second(q, first, direction, h):
        by = 1 - 2 * direction
        at = place(h, first, -by)
        r_wait(q, h, at, slot_of(first, direction))
        r_start(q, h, at, direction, slot_of(first, 2), place(h, 0, by))
        to_partner(q, h, at, 0)

    def r_second_opposite(q, first, h):
        at = place(h, first, 2)
        r_wait(q, h, at, slot_of(first, 2))
        to_partner(q, h, at, 1)

    FIRSTS = (0, -1, 1, 2)

    def product(k, by, start, size, columns):
        return jnp.dot(
            a_buf[a_part(shift(x, k), by, start, size), :],
            r_buf[rows_at(shift(x, k) * depth, depth), columns],
            preferred_element_type=jnp.float32,
        )

    def unit(k, by, mode, start=0, size=None):
        size = quarter if size is None else size
        out_rows = rows_at(shift(x, by) * quarter + start, size, 32)

        def step(j, carry):
            columns = pl.ds(pl.multiple_of(j * TILE_N, TILE_N), TILE_N)
            value = product(k, by, start, size, columns)
            if mode != "set":
                value = value + c_buf[out_rows, columns]
            c_buf[out_rows, columns] = value
            if mode == "last":
                sq_sum[:, columns] += jnp.sum(value * value, axis=0, keepdims=True)
            return carry

        lax.fori_loop(0, cols // TILE_N, step, 0)

    delta = (x + 2 - z + SIDE) % SIDE
    low = 1 - delta // 2
    early_blocks = ((3 - delta) // 3, 1 + 2 * low)
    late_blocks = (delta * low + 3 * (1 - low), 2)

    def ext_dot_0(start, block):
        return jnp.dot(
            a_buf[a_part(block, -1, start, EXT_M), :],
            r2_buf[rows_at(block * depth, depth), :],
            preferred_element_type=jnp.float32,
        )

    def ext_dot_1(start, pairs):
        total = None
        for zz, yy in pairs:
            value = jnp.dot(
                a_buf[a_part(zz, 1, start, EXT_M), pl.ds(pl.multiple_of(yy * chip, 128), chip)],
                r2_buf[rows_at(k_all + (zz * SIDE + yy) * chip, chip), :],
                preferred_element_type=jnp.float32,
            )
            total = value if total is None else total + value
        return total

    def ext_unit(h, dot, what, mode):
        def step(i, carry):
            start = pl.multiple_of(i * EXT_M, EXT_M)
            part = pl.ds(start, EXT_M)
            value = dot(start, what)
            if mode != "set":
                value = value + ext[h, part, :]
            ext[h, part, :] = value
            if mode == "last":
                columns = pl.ds(h * side_cols, side_cols)
                sq_out[:, columns] += jnp.sum(value * value, axis=0, keepdims=True)
            return carry

        lax.fori_loop(0, quarter // EXT_M, step, 0)

    def ext_early(h):
        if h == 0:
            for i, k in enumerate(early_blocks):
                ext_unit(0, ext_dot_0, shift(z, k), "set" if i == 0 else "add")
        else:
            for i, k in enumerate((0, -1, 1)):
                pairs = [(shift(x, b), shift(y, k)) for b in (0, -1, 1)]
                ext_unit(1, ext_dot_1, pairs, "set" if i == 0 else "add")

    def ext_middle():
        ext_unit(0, ext_dot_0, shift(z, late_blocks[0]), "add")
        ext_unit(1, ext_dot_1, [(shift(x, 2), shift(y, k)) for k in (0, -1, 1)], "add")

    def ext_late(h):
        if h == 0:
            ext_unit(0, ext_dot_0, shift(z, late_blocks[1]), "last")
        else:
            ext_unit(1, ext_dot_1, [(zz, shift(y, 2)) for zz in range(SIDE)], "last")

    def ext_copy(h, start, stop):
        by = 1 - 2 * h
        dst = c_buf.at[rows_at(shift(x, -by) * quarter + start, stop - start, 64), pl.ds(h * side_cols, side_cols)]
        src = ext.at[h, pl.ds(start, stop - start), :]
        return remote(src, dst, sem["e_send"], sem["e_recv"], g, shift(x, by))

    def rounded(h, count=1):
        return r2_buf.at[pl.ds(h * (quarter - WIDE), count * (quarter - WIDE)), :]

    def rounded_copy(h):
        dst = narrow.at[:, pl.ds(h * side_cols, side_cols)]
        return remote(rounded(h), dst, sem["b_send"], sem["b_recv"], g, shift(x, 1 - 2 * h))

    def scale_copy(h):
        columns = pl.ds(h * side_cols, side_cols)
        return remote(
            scale.at[:, columns], scale_in.at[:, columns], sem["n_send"], sem["n_recv"], g, shift(x, 2 * h - 1)
        )

    def sq_ext_copy(h):
        columns = pl.ds(h * side_cols, side_cols)
        return remote(
            sq_out.at[:, columns], sq_in.at[:, columns], sem["q_send"], sem["q_recv"], g, shift(x, 1 - 2 * h)
        )

    own_rot.wait()
    for h in (0, 1):
        remote(
            r_buf.at[piece_rows(own, core), pl.ds(h * side_cols, side_cols)], r_ref(1, h, own, None, core),
            sem["x_send"], sem["x_recv"], g, shift(x, 2 * h - 1),
        ).start()
    r_own_first(0)
    own_coef.wait()
    for i in range(3):
        for direction in (0, 1):
            a_start(direction, i)
    r_own_second(0)
    sq_sum[...] = jnp.zeros_like(sq_sum)
    sq_out[...] = jnp.zeros_like(sq_out)
    r_first(0)
    for h in (0, 1):
        r_opposite(0, h)
    for first in FIRSTS:
        for direction in (0, 1):
            for h in (0, 1):
                r_second(0, first, direction, h)
    two = r2_buf.at[pl.ds(0, 2 * piece), :]
    remote(two, two, sem["x_send"], sem["x_recv"], g, shift(x, 1)).wait()
    r_own_first(1)
    r_own_second(1)
    for direction in (0, 1):
        a_wait(direction, 0)
        relay_start(direction)
    for first in FIRSTS:
        for h in (0, 1):
            r_second_opposite(0, first, h)
    for direction in (0, 1):
        a_wait(direction, 1)
        for c in range(len(LAST)):
            last_start(direction, c)
    pieces = SIDE * SIDE * piece
    ref = r_buf.at[pl.ds(0, pieces), :]
    remote(ref, ref, sem["p_send"], sem["p_recv"], partner, x).wait()

    unit(0, 0, "set")
    unit(0, 1, "set")
    r_first(1)
    unit(0, -1, "set")
    for k in (-1, 1):
        unit(k, 0, "add")
    r_opposite(1, 0)
    for k in (-1, 1):
        unit(k, -k, "add")
    r_opposite(1, 1)
    for first in FIRSTS:
        for direction in (0, 1):
            for h in (0, 1):
                r_second(1, first, direction, h)
        if first == 0:
            for direction, k in enumerate((-1, 1)):
                a_wait(direction, 2)
                unit(k, k, "add")
    early = r2_buf.at[pl.ds(0, 12 * piece), :]
    for h in (0, 1):
        remote(early, early, sem["p2_send"], sem["p_recv%d0" % h], partner, x).wait_recv()
        ext_early(h)
    for direction, by in enumerate((-1, 1)):
        relay_wait(direction)
        unit(2, by, "last")
        for first in FIRSTS[2 * direction:2 * direction + 2]:
            for h in (0, 1):
                r_second_opposite(1, first, h)
    ext_middle()
    late = r2_buf.at[pl.ds(0, 4 * piece), :]
    for h in (0, 1):
        remote(late, late, sem["p2_send"], sem["p_recv%d1" % h], partner, x).wait_recv()
        ext_late(h)
        sq_ext_copy(h).start()
        ext_copy(h, 0, FIRST_WIDE).start()
    for c in range(len(LAST)):
        last_wait(c)
        unit(2, 0, "last", last_starts[c], LAST[c])
    remote(sq_out, sq_in, sem["q_send"], sem["q_recv"], g, shift(x, 1)).wait()

    sq_buf[g] = sq_sum[...] + sq_in[...]
    others = [(dz, dy, dc) for dz in range(-1, 3) for dy in range(-1, 3) for dc in (0, 1) if (dz, dy, dc) != (0, 0, 0)]
    for dz, dy, dc in sorted(others, key=lambda by: -(abs(by[0]) + abs(by[1]))):
        peer = device_of(shift(z, dz), shift(y, dy), (core + dc) % 2)
        remote(sq_buf.at[g], sq_buf.at[g], sem["s_send"], sem["s_recv"], peer, x).start()
    ref = a_buf.at[pl.ds(0, 9 * quarter), :]
    remote(ref, ref, sem["a_send"], sem["e_recv"], g, shift(x, 1)).wait_send()
    ref = r_buf.at[pl.ds(0, 15 * piece), :]
    remote(ref, ref, sem["r_send"], sem["e_recv"], partner, x).wait_send()
    ref = r2_buf.at[pl.ds(0, 30 * piece), :]
    remote(ref, ref, sem["r2_send"], sem["e_recv"], partner, x).wait_send()
    ref = r2_buf.at[pl.ds(0, 32 * piece), :]
    remote(ref, ref, sem["p2_send"], sem["e_recv"], partner, x).wait_send()
    ref = sq_buf.at[pl.ds(0, peers - 1)]
    remote(ref, ref, sem["s_send"], sem["s_recv"], partner, x).wait()
    total = sq_buf[0]
    for i in range(1, peers):
        total = total + sq_buf[i]
    rms = jnp.sqrt(total / TOTAL_ROWS + 1e-06)
    rms_out[...] = rms
    scale[...] = 1.0 / rms
    for h in (0, 1):
        scale_copy(h).start()
        ext_copy(h, FIRST_WIDE, WIDE).start()
    remote(scale, scale_in, sem["n_send"], sem["n_recv"], g, shift(x, 1)).wait()
    for h in (0, 1):
        rounded(h)[...] = (ext[h, WIDE:, :] * scale_in[:, h * side_cols:(h + 1) * side_cols]).astype(jnp.bfloat16)
        rounded_copy(h).start()
    ref = ext.at[:, pl.ds(0, WIDE), :]
    remote(ref, ref, sem["e_send"], sem["e_recv"], g, shift(x, 1)).wait()
    remote(rounded(0, 2), rounded(0, 2), sem["b_send"], sem["b_recv"], g, shift(x, 1)).wait()


def normalize(c_buf, rms_in, scale, narrow, out, rms_out, staged, out_sem):
    rows, cols = c_buf.shape
    quarter = rows // SIDE
    x = lax.axis_index("ba")
    rms_out[...] = rms_in[...].reshape(cols)
    copies = []

    def put(src, start, size):
        part = pl.ds(pl.multiple_of(start, 16), size)
        copy = pltpu.make_async_copy(src, out.at[part, :], out_sem.at[len(copies)])
        copy.start()
        copies.append(copy)

    def opposite(by):
        return (x + by) % SIDE * quarter

    put(narrow, opposite(2) + WIDE, quarter - WIDE)
    at = 0
    for by, start, size in [(2, 0, WIDE)] + [(by, start, 64) for by in (0, 1, 3) for start in range(0, quarter, 64)]:
        part = pl.ds(pl.multiple_of(opposite(by) + start, 64), size)
        staged[pl.ds(at, size), :] = (c_buf[part, :] * scale[...]).astype(jnp.bfloat16)
        put(staged.at[pl.ds(at, size), :], opposite(by) + start, size)
        at += size
    for copy in copies:
        copy.wait()


def body(coefficients, rotation):
    rows, depth = coefficients.shape
    piece, cols = rotation.shape
    peers = lax.axis_size("ga")
    dma = pltpu.SemaphoreType.DMA
    row = pltpu.VMEM((1, cols), jnp.float32)
    parts = pl.pallas_call(
        gather_multiply,
        out_shape=(
            pltpu.VMEM((rows, cols), jnp.float32), row, row,
            pltpu.VMEM((rows // SIDE - WIDE, cols), jnp.bfloat16),
        ),
        in_specs=[pl.BlockSpec(memory_space=pl.ANY)] * 2,
        out_specs=(pl.BlockSpec(memory_space=pltpu.VMEM),) * 4,
        scratch_shapes=[
            pltpu.VMEM((SIDE * rows, depth), jnp.bfloat16),
            pltpu.VMEM((SIDE * depth, cols), jnp.bfloat16),
            pltpu.VMEM((2 * SIDE * depth, cols // 2), jnp.bfloat16),
            pltpu.VMEM((2, rows // SIDE, cols // 2), jnp.float32),
            pltpu.VMEM((peers, 1, cols), jnp.float32),
            row,
            row,
            row,
            row,
            dma((2,)),
            dma((2, 3)),
            dma((2,)),
            dma((len(LAST),)),
            dma((2, 15)),
            dma((2, 15)),
            dma((len(SEMS),)),
        ],
        compiler_params=pltpu.CompilerParams(
            collective_id=0, has_side_effects=True, vmem_limit_bytes=55 * 1024 * 1024
        ),
        cost_estimate=pl.CostEstimate(
            flops=2 * rows * depth * SIDE * cols, bytes_accessed=4 * rows * depth, transcendentals=0
        ),
    )(coefficients, rotation)
    return pl.pallas_call(
        normalize,
        out_shape=(
            jax.ShapeDtypeStruct((rows, cols), jnp.bfloat16),
            jax.ShapeDtypeStruct((cols,), jnp.float32),
        ),
        in_specs=[pl.BlockSpec(memory_space=pltpu.VMEM)] * 4,
        out_specs=(pl.BlockSpec(memory_space=pl.ANY), pl.BlockSpec(memory_space=pltpu.VMEM)),
        scratch_shapes=[
            pltpu.VMEM((rows, cols), jnp.bfloat16),
            dma((20,)),
        ],
        compiler_params=pltpu.CompilerParams(vmem_limit_bytes=20 * 1024 * 1024),
        cost_estimate=pl.CostEstimate(flops=rows * cols, bytes_accessed=6 * rows * cols, transcendentals=0),
    )(*parts)


def solution(mesh):
    return jax.shard_map(
        body, mesh=mesh, in_specs=(P("ga", "ba"), P("ga", "ba")), out_specs=(P("ga", "ba"), P("ba")), check_vma=False
    )
```

```python
import jax
import jax.numpy as jnp
from jax import lax
from jax.experimental import pallas as pl
from jax.experimental.pallas import tpu as pltpu
from jax.sharding import PartitionSpec as P

MESH = pl.DeviceIdType.MESH
SIDE = 4
LAST = (320,)
FIRST_WIDE, WIDE = 144, 144
TILE_N = 768
EXT_M = 160
TOTAL_ROWS = 40960
SENDS = ("a_send", "r_send", "r2_send", "p_send", "p2_send", "x_send", "e_send", "q_send", "s_send", "n_send", "b_send")
ARRIVALS = ("x_recv", "e_recv", "q_recv", "s_recv", "n_recv", "b_recv", "p_recv", "p_recv00", "p_recv01", "p_recv10", "p_recv11")
SEMS = {name: i for i, name in enumerate(SENDS + ARRIVALS)}


def gather_multiply(
    coef, rot, result, rms_out, c_buf, scale, a_buf, r_buf, r2_buf, ext, sq_buf, sq_sum, sq_out, sq_in, scale_in,
    load_sem, a_sem, relay_sem, last_sem, r_sem, r2_sem, sems,
):
    rows, depth = coef.shape
    piece, cols = rot.shape
    peers = 2 * SIDE * SIDE
    quarter = rows // SIDE
    side_cols = cols // 2
    k_all = peers * piece
    chip = 2 * piece

    g = lax.axis_index("ga")
    x = lax.axis_index("ba")
    core = g % 2
    y = (g // 2) % SIDE
    z = g // (2 * SIDE)
    sem = {name: sems.at[i] for name, i in SEMS.items()}

    def shift(value, by):
        return (value + by + SIDE) % SIDE

    def device_of(zz, yy, cc):
        return (zz * SIDE + yy) * 2 + cc

    partner = device_of(z, y, 1 - core)

    def rows_at(start, size, align=16):
        return pl.ds(pl.multiple_of(start, align), size)

    def a_part(block, by, start=0, size=None):
        at = (block * 3 + by + 1) * quarter + start
        return rows_at(at, quarter if size is None else size, 32)

    def piece_rows(at, cc, start=0, size=None):
        return rows_at(device_of(at[0], at[1], cc) * piece + start, piece if size is None else size)

    own = (z, y)

    own_rot = pltpu.make_async_copy(rot, r_buf.at[piece_rows(own, core), :], load_sem.at[1])
    own_rot.start()

    def own_part(by):
        return coef.at[rows_at(shift(x, by) * quarter, quarter, 32), :]

    for by in (-1, 0, 1):
        pltpu.make_async_copy(own_part(by), a_buf.at[a_part(x, by), :], load_sem.at[0]).start()

    barrier = pltpu.get_barrier_semaphore()
    near = [(device_of(shift(z, by), y, core), x) for by in (1, -1)]
    near += [(device_of(z, shift(y, by), core), x) for by in (1, -1)]
    near += [(g, shift(x, by)) for by in (1, -1)]
    near += [(partner, x)]
    for ga, ba in near:
        pl.semaphore_signal(barrier, inc=1, device_id={"ga": ga, "ba": ba}, device_id_type=MESH)
    pl.semaphore_wait(barrier, len(near))

    def remote(src, dst, send, recv, ga, ba):
        return pltpu.make_async_remote_copy(
            src_ref=src, dst_ref=dst, send_sem=send, recv_sem=recv,
            device_id={"ga": ga, "ba": ba}, device_id_type=MESH,
        )

    def a_move(src, dst, recv, to):
        src = src if isinstance(src, tuple) else (a_buf.at[src, :],)
        return remote(src[0], a_buf.at[dst, :], sem["a_send"], recv, g, to)

    def a_start(direction, i):
        by = 1 - 2 * direction
        src = (a_part(x, by), (own_part(2),), a_part(x, 0))[i]
        a_move(src, a_part(x, (0, by, -by)[i]), a_sem.at[direction, i], shift(x, by)).start()

    def a_wait(direction, i):
        by = 1 - 2 * direction
        part = a_part(shift(x, -by), (0, by, -by)[i])
        a_move(part, part, a_sem.at[direction, i], shift(x, by)).wait_recv()

    def relay_start(direction):
        by = 1 - 2 * direction
        origin = shift(x, -by)
        a_move(a_part(origin, 0), a_part(origin, -by), relay_sem.at[direction], shift(x, by)).start()

    def relay_wait(direction):
        by = 1 - 2 * direction
        part = a_part(shift(x, 2), -by)
        a_move(part, part, relay_sem.at[direction], shift(x, by)).wait_recv()

    last_starts = [sum(LAST[:c]) for c in range(len(LAST))]

    def last_start(direction, c):
        by = 1 - 2 * direction
        size = LAST[c] // 2
        start = last_starts[c] + direction * size
        origin = shift(x, -by)
        a_move(a_part(origin, by, start, size), a_part(origin, 0, start, size), last_sem.at[c], shift(x, by)).start()

    def last_wait(c):
        part = a_part(shift(x, 2), 0, last_starts[c], LAST[c])
        a_move(part, part, last_sem.at[c], shift(x, 1)).wait_recv()

    def place(h, first, second):
        return (shift(z, second), shift(y, first)) if h == 0 else (shift(z, first), shift(y, second))

    def r_ref(q, h, at, part, cc):
        if q == 0:
            size = piece // 2
            start = h * size
            ref = r_buf
            if part is not None:
                size = size // 2
                start = start + part * size
            return ref.at[piece_rows(at, cc, start, size), :]
        size, start = piece, h * k_all
        if part is not None:
            size = size // 2
            start = start + part * size
        return r2_buf.at[piece_rows(at, cc, start, size), :]

    def r_start(q, h, at, part, slot, to):
        ref = r_ref(q, h, at, part, core)
        recv = (r_sem if q == 0 else r2_sem).at[h, slot]
        remote(ref, ref, sem["r_send"] if q == 0 else sem["r2_send"], recv, device_of(to[0], to[1], core), x).start()

    def r_wait(q, h, at, slot):
        ref = r_ref(q, h, at, None, core)
        recv = (r_sem if q == 0 else r2_sem).at[h, slot]
        remote(ref, ref, sem["r_send"], recv, partner, x).wait_recv()

    def to_partner(q, h, at, late):
        ref = r_ref(q, h, at, None, core)
        recv = sem["p_recv"] if q == 0 else sem["p_recv%d%d" % (h, late)]
        remote(ref, ref, sem["p_send"] if q == 0 else sem["p2_send"], recv, partner, x).start()

    places = {0: 0, -1: 1, 1: 2, 2: 3}

    def slot_of(first, kind):
        return 3 + 3 * places[first] + kind

    def along_second(q, h, at, first):
        for direction in (0, 1):
            r_start(q, h, at, None, slot_of(first, direction), place(h, 0, 1 - 2 * direction))

    def r_own_first(q):
        for h in (0, 1):
            for direction in (0, 1):
                r_start(q, h, own, None, direction, place(h, 1 - 2 * direction, 0))

    def r_own_second(q):
        for h in (0, 1):
            along_second(q, h, own, 0)
            to_partner(q, h, own, 0)

    def r_first(q):
        for direction in (0, 1):
            by = 1 - 2 * direction
            for h in (0, 1):
                at = place(h, -by, 0)
                r_wait(q, h, at, direction)
                r_start(q, h, at, direction, 2, place(h, by, 0))
        for by in (1, -1):
            for h in (0, 1):
                at = place(h, -by, 0)
                along_second(q, h, at, -by)
                to_partner(q, h, at, 0)

    def r_opposite(q, h):
        at = place(h, 2, 0)
        r_wait(q, h, at, 2)
        along_second(q, h, at, 2)
        to_partner(q, h, at, 0)

    def r_second(q, first, direction, h):
        by = 1 - 2 * direction
        at = place(h, first, -by)
        r_wait(q, h, at, slot_of(first, direction))
        r_start(q, h, at, direction, slot_of(first, 2), place(h, 0, by))
        to_partner(q, h, at, 0)

    def r_second_opposite(q, first, h):
        at = place(h, first, 2)
        r_wait(q, h, at, slot_of(first, 2))
        to_partner(q, h, at, 1)

    FIRSTS = (0, -1, 1, 2)

    def product(k, by, start, size, columns):
        return jnp.dot(
            a_buf[a_part(shift(x, k), by, start, size), :],
            r_buf[rows_at(shift(x, k) * depth, depth), columns],
            preferred_element_type=jnp.float32,
        )

    def unit(k, by, mode, start=0, size=None):
        size = quarter if size is None else size
        out_rows = rows_at(shift(x, by) * quarter + start, size, 32)

        def step(j, carry):
            columns = pl.ds(pl.multiple_of(j * TILE_N, TILE_N), TILE_N)
            value = product(k, by, start, size, columns)
            if mode != "set":
                value = value + c_buf[out_rows, columns]
            c_buf[out_rows, columns] = value
            if mode == "last":
                sq_sum[:, columns] += jnp.sum(value * value, axis=0, keepdims=True)
            return carry

        lax.fori_loop(0, cols // TILE_N, step, 0)

    delta = (x + 2 - z + SIDE) % SIDE
    low = 1 - delta // 2
    early_blocks = ((3 - delta) // 3, 1 + 2 * low)
    late_blocks = (delta * low + 3 * (1 - low), 2)

    def ext_dot_0(start, block):
        return jnp.dot(
            a_buf[a_part(block, -1, start, EXT_M), :],
            r2_buf[rows_at(block * depth, depth), :],
            preferred_element_type=jnp.float32,
        )

    def ext_dot_1(start, pairs):
        total = None
        for zz, yy in pairs:
            value = jnp.dot(
                a_buf[a_part(zz, 1, start, EXT_M), pl.ds(pl.multiple_of(yy * chip, 128), chip)],
                r2_buf[rows_at(k_all + (zz * SIDE + yy) * chip, chip), :],
                preferred_element_type=jnp.float32,
            )
            total = value if total is None else total + value
        return total

    def ext_unit(h, dot, what, mode):
        def step(i, carry):
            start = pl.multiple_of(i * EXT_M, EXT_M)
            part = pl.ds(start, EXT_M)
            value = dot(start, what)
            if mode != "set":
                value = value + ext[h, part, :]
            ext[h, part, :] = value
            if mode == "last":
                columns = pl.ds(h * side_cols, side_cols)
                sq_out[:, columns] += jnp.sum(value * value, axis=0, keepdims=True)
            return carry

        lax.fori_loop(0, quarter // EXT_M, step, 0)

    def ext_early(h):
        if h == 0:
            for i, k in enumerate(early_blocks):
                ext_unit(0, ext_dot_0, shift(z, k), "set" if i == 0 else "add")
        else:
            for i, k in enumerate((0, -1, 1)):
                pairs = [(shift(x, b), shift(y, k)) for b in (0, -1, 1)]
                ext_unit(1, ext_dot_1, pairs, "set" if i == 0 else "add")

    def ext_middle():
        ext_unit(0, ext_dot_0, shift(z, late_blocks[0]), "add")
        ext_unit(1, ext_dot_1, [(shift(x, 2), shift(y, k)) for k in (0, -1, 1)], "add")

    def ext_late(h):
        if h == 0:
            ext_unit(0, ext_dot_0, shift(z, late_blocks[1]), "last")
        else:
            ext_unit(1, ext_dot_1, [(zz, shift(y, 2)) for zz in range(SIDE)], "last")

    def ext_copy(h, start, stop):
        by = 1 - 2 * h
        dst = c_buf.at[rows_at(shift(x, -by) * quarter + start, stop - start, 64), pl.ds(h * side_cols, side_cols)]
        src = ext.at[h, pl.ds(start, stop - start), :]
        return remote(src, dst, sem["e_send"], sem["e_recv"], g, shift(x, by))

    def rounded(h, count=1):
        return r2_buf.at[pl.ds(h * (quarter - WIDE), count * (quarter - WIDE)), :]

    def rounded_copy(h):
        by = 1 - 2 * h
        dst = result.at[rows_at(shift(x, -by) * quarter + WIDE, quarter - WIDE), pl.ds(h * side_cols, side_cols)]
        return remote(rounded(h), dst, sem["b_send"], sem["b_recv"], g, shift(x, 1 - 2 * h))

    def scale_copy(h):
        columns = pl.ds(h * side_cols, side_cols)
        return remote(
            scale.at[:, columns], scale_in.at[:, columns], sem["n_send"], sem["n_recv"], g, shift(x, 2 * h - 1)
        )

    def sq_ext_copy(h):
        columns = pl.ds(h * side_cols, side_cols)
        return remote(
            sq_out.at[:, columns], sq_in.at[:, columns], sem["q_send"], sem["q_recv"], g, shift(x, 1 - 2 * h)
        )

    own_rot.wait()
    for h in (0, 1):
        remote(
            r_buf.at[piece_rows(own, core), pl.ds(h * side_cols, side_cols)], r_ref(1, h, own, None, core),
            sem["x_send"], sem["x_recv"], g, shift(x, 2 * h - 1),
        ).start()
    r_own_first(0)
    loaded = a_buf.at[rows_at(x * 3 * quarter, 3 * quarter, 32), :]
    pltpu.make_async_copy(loaded, loaded, load_sem.at[0]).wait()
    for i in range(3):
        for direction in (0, 1):
            a_start(direction, i)
    r_own_second(0)
    sq_sum[...] = jnp.zeros_like(sq_sum)
    sq_out[...] = jnp.zeros_like(sq_out)
    r_first(0)
    for h in (0, 1):
        r_opposite(0, h)
    for first in FIRSTS:
        for direction in (0, 1):
            for h in (0, 1):
                r_second(0, first, direction, h)
    two = r2_buf.at[pl.ds(0, 2 * piece), :]
    remote(two, two, sem["x_send"], sem["x_recv"], g, shift(x, 1)).wait()
    r_own_first(1)
    r_own_second(1)
    for direction in (0, 1):
        a_wait(direction, 0)
        relay_start(direction)
    for first in FIRSTS:
        for h in (0, 1):
            r_second_opposite(0, first, h)
    for direction in (0, 1):
        a_wait(direction, 1)
        for c in range(len(LAST)):
            last_start(direction, c)
    pieces = SIDE * SIDE * piece
    ref = r_buf.at[pl.ds(0, pieces), :]
    remote(ref, ref, sem["p_send"], sem["p_recv"], partner, x).wait()

    unit(0, 0, "set")
    unit(0, 1, "set")
    r_first(1)
    unit(0, -1, "set")
    for k in (-1, 1):
        unit(k, 0, "add")
    r_opposite(1, 0)
    for k in (-1, 1):
        unit(k, -k, "add")
    r_opposite(1, 1)
    for first in FIRSTS:
        for direction in (0, 1):
            for h in (0, 1):
                r_second(1, first, direction, h)
        if first == 0:
            for direction, k in enumerate((-1, 1)):
                a_wait(direction, 2)
                unit(k, k, "add")
    early = r2_buf.at[pl.ds(0, 12 * piece), :]
    for h in (0, 1):
        remote(early, early, sem["p2_send"], sem["p_recv%d0" % h], partner, x).wait_recv()
        ext_early(h)
    for direction, by in enumerate((-1, 1)):
        relay_wait(direction)
        unit(2, by, "last")
        for first in FIRSTS[2 * direction:2 * direction + 2]:
            for h in (0, 1):
                r_second_opposite(1, first, h)
    ext_middle()
    late = r2_buf.at[pl.ds(0, 4 * piece), :]
    for h in (0, 1):
        remote(late, late, sem["p2_send"], sem["p_recv%d1" % h], partner, x).wait_recv()
        ext_late(h)
        sq_ext_copy(h).start()
        ext_copy(h, 0, FIRST_WIDE).start()
    for c in range(len(LAST)):
        last_wait(c)
        unit(2, 0, "last", last_starts[c], LAST[c])
    remote(sq_out, sq_in, sem["q_send"], sem["q_recv"], g, shift(x, 1)).wait()

    sq_buf[g] = sq_sum[...] + sq_in[...]
    others = [(dz, dy, dc) for dz in range(-1, 3) for dy in range(-1, 3) for dc in (0, 1) if (dz, dy, dc) != (0, 0, 0)]
    for dz, dy, dc in sorted(others, key=lambda by: -(abs(by[0]) + abs(by[1]))):
        peer = device_of(shift(z, dz), shift(y, dy), (core + dc) % 2)
        remote(sq_buf.at[g], sq_buf.at[g], sem["s_send"], sem["s_recv"], peer, x).start()
    ref = a_buf.at[pl.ds(0, 9 * quarter), :]
    remote(ref, ref, sem["a_send"], sem["e_recv"], g, shift(x, 1)).wait_send()
    ref = r_buf.at[pl.ds(0, 15 * piece), :]
    remote(ref, ref, sem["r_send"], sem["e_recv"], partner, x).wait_send()
    ref = r2_buf.at[pl.ds(0, 30 * piece), :]
    remote(ref, ref, sem["r2_send"], sem["e_recv"], partner, x).wait_send()
    ref = r2_buf.at[pl.ds(0, 32 * piece), :]
    remote(ref, ref, sem["p2_send"], sem["e_recv"], partner, x).wait_send()
    ref = sq_buf.at[pl.ds(0, peers - 1)]
    remote(ref, ref, sem["s_send"], sem["s_recv"], partner, x).wait()
    total = sq_buf[0]
    for i in range(1, peers):
        total = total + sq_buf[i]
    rms = jnp.sqrt(total / TOTAL_ROWS + 1e-06)
    rms_out[...] = rms
    scale[...] = 1.0 / rms
    for h in (0, 1):
        scale_copy(h).start()
        if FIRST_WIDE < WIDE:
            ext_copy(h, FIRST_WIDE, WIDE).start()
    remote(scale, scale_in, sem["n_send"], sem["n_recv"], g, shift(x, 1)).wait()
    for h in (0, 1):
        rounded(h)[...] = (ext[h, WIDE:, :] * scale_in[:, h * side_cols:(h + 1) * side_cols]).astype(jnp.bfloat16)
        rounded_copy(h).start()
    ref = ext.at[:, pl.ds(0, WIDE), :]
    remote(ref, ref, sem["e_send"], sem["e_recv"], g, shift(x, 1)).wait()

    def normalize(part):
        result[part, :] = (c_buf[part, :] * scale[...]).astype(jnp.bfloat16)

    normalize(rows_at(shift(x, 2) * quarter, WIDE))
    for by in (-1, 0, 1):
        normalize(rows_at(shift(x, by) * quarter, quarter))
    remote(rounded(0, 2), rounded(0, 2), sem["b_send"], sem["b_recv"], g, shift(x, 1)).wait()


def put(result, rms_in, out, rms_out, rms, out_sem):
    rows = result.shape[0]
    copies = []
    for i in range(4):
        part = pl.ds(i * rows // 4, rows // 4)
        copies.append(pltpu.make_async_copy(result.at[part, :], out.at[part, :], out_sem.at[i]))
        copies[-1].start()
    rms[...] = rms_in[...].reshape(rms.shape)
    copies.append(pltpu.make_async_copy(rms, rms_out, out_sem.at[4]))
    copies[-1].start()
    for copy in copies:
        copy.wait()


def body(coefficients, rotation):
    rows, depth = coefficients.shape
    piece, cols = rotation.shape
    peers = lax.axis_size("ga")
    dma = pltpu.SemaphoreType.DMA
    row = pltpu.VMEM((1, cols), jnp.float32)
    parts = pl.pallas_call(
        gather_multiply,
        out_shape=(pltpu.VMEM((rows, cols), jnp.bfloat16), row),
        in_specs=[pl.BlockSpec(memory_space=pl.ANY)] * 2,
        out_specs=(pl.BlockSpec(memory_space=pltpu.VMEM),) * 2,
        scratch_shapes=[
            pltpu.VMEM((rows, cols), jnp.float32),
            row,
            pltpu.VMEM((3 * rows, depth), jnp.bfloat16),
            pltpu.VMEM((SIDE * depth, cols), jnp.bfloat16),
            pltpu.VMEM((2 * SIDE * depth, cols // 2), jnp.bfloat16),
            pltpu.VMEM((2, rows // SIDE, cols // 2), jnp.float32),
            pltpu.VMEM((peers, 1, cols), jnp.float32),
            row,
            row,
            row,
            row,
            dma((2,)),
            dma((2, 3)),
            dma((2,)),
            dma((len(LAST),)),
            dma((2, 15)),
            dma((2, 15)),
            dma((len(SEMS),)),
        ],
        compiler_params=pltpu.CompilerParams(
            collective_id=0, has_side_effects=True, vmem_limit_bytes=60 * 1024 * 1024
        ),
        cost_estimate=pl.CostEstimate(
            flops=2 * rows * depth * SIDE * cols, bytes_accessed=4 * rows * depth, transcendentals=0
        ),
    )(coefficients, rotation)
    return pl.pallas_call(
        put,
        out_shape=(
            jax.ShapeDtypeStruct((rows, cols), jnp.bfloat16),
            jax.ShapeDtypeStruct((cols,), jnp.float32),
        ),
        in_specs=[pl.BlockSpec(memory_space=pltpu.VMEM)] * 2,
        out_specs=(pl.BlockSpec(memory_space=pl.ANY),) * 2,
        scratch_shapes=[
            pltpu.VMEM((cols,), jnp.float32),
            dma((5,)),
        ],
        compiler_params=pltpu.CompilerParams(vmem_limit_bytes=4 * 1024 * 1024),
        cost_estimate=pl.CostEstimate(flops=rows * cols, bytes_accessed=6 * rows * cols, transcendentals=0),
    )(*parts)


def solution(mesh):
    return jax.shard_map(
        body, mesh=mesh, in_specs=(P("ga", "ba"), P("ga", "ba")), out_specs=(P("ga", "ba"), P("ba")), check_vma=False
    )
```

```python
import jax
import jax.numpy as jnp
from jax import lax
from jax.experimental import pallas as pl
from jax.experimental.pallas import tpu as pltpu
from jax.sharding import PartitionSpec as P

MESH = pl.DeviceIdType.MESH
SIDE = 4
LAST = (320,)
FIRST_WIDE, WIDE = 144, 176
TILE_N = 768
EXT_M = 160
TOTAL_ROWS = 40960
SENDS = ("a_send", "r_send", "r2_send", "p_send", "p2_send", "x_send", "e_send", "q_send", "s_send", "n_send", "b_send")
ARRIVALS = ("x_recv", "e_recv", "q_recv", "s_recv", "n_recv", "b_recv", "p_recv", "p_recv00", "p_recv01", "p_recv10", "p_recv11")
SEMS = {name: i for i, name in enumerate(SENDS + ARRIVALS)}


def gather_multiply(
    coef, rot, result, rms_out, c_buf, scale, a_buf, r_buf, r2_buf, ext, sq_buf, sq_sum, sq_out, sq_in, scale_in,
    load_sem, a_sem, relay_sem, last_sem, r_sem, r2_sem, sems,
):
    rows, depth = coef.shape
    piece, cols = rot.shape
    peers = 2 * SIDE * SIDE
    quarter = rows // SIDE
    side_cols = cols // 2
    k_all = peers * piece
    chip = 2 * piece

    g = lax.axis_index("ga")
    x = lax.axis_index("ba")
    core = g % 2
    y = (g // 2) % SIDE
    z = g // (2 * SIDE)
    sem = {name: sems.at[i] for name, i in SEMS.items()}

    def shift(value, by):
        return (value + by + SIDE) % SIDE

    def device_of(zz, yy, cc):
        return (zz * SIDE + yy) * 2 + cc

    partner = device_of(z, y, 1 - core)

    def rows_at(start, size, align=16):
        return pl.ds(pl.multiple_of(start, align), size)

    def a_part(block, by, start=0, size=None):
        at = (block * 3 + by + 1) * quarter + start
        return rows_at(at, quarter if size is None else size, 32)

    def piece_rows(at, cc, start=0, size=None):
        return rows_at(device_of(at[0], at[1], cc) * piece + start, piece if size is None else size)

    own = (z, y)

    own_rot = pltpu.make_async_copy(rot, r_buf.at[piece_rows(own, core), :], load_sem.at[1])
    own_rot.start()

    def own_part(by):
        return coef.at[rows_at(shift(x, by) * quarter, quarter, 32), :]

    for by in (-1, 0, 1):
        pltpu.make_async_copy(own_part(by), a_buf.at[a_part(x, by), :], load_sem.at[0]).start()

    barrier = pltpu.get_barrier_semaphore()
    near = [(device_of(shift(z, by), y, core), x) for by in (1, -1)]
    near += [(device_of(z, shift(y, by), core), x) for by in (1, -1)]
    near += [(g, shift(x, by)) for by in (1, -1)]
    near += [(partner, x)]
    for ga, ba in near:
        pl.semaphore_signal(barrier, inc=1, device_id={"ga": ga, "ba": ba}, device_id_type=MESH)
    pl.semaphore_wait(barrier, len(near))

    def remote(src, dst, send, recv, ga, ba):
        return pltpu.make_async_remote_copy(
            src_ref=src, dst_ref=dst, send_sem=send, recv_sem=recv,
            device_id={"ga": ga, "ba": ba}, device_id_type=MESH,
        )

    def a_move(src, dst, recv, to):
        src = src if isinstance(src, tuple) else (a_buf.at[src, :],)
        return remote(src[0], a_buf.at[dst, :], sem["a_send"], recv, g, to)

    def a_start(direction, i):
        by = 1 - 2 * direction
        src = (a_part(x, by), (own_part(2),), a_part(x, 0))[i]
        a_move(src, a_part(x, (0, by, -by)[i]), a_sem.at[direction, i], shift(x, by)).start()

    def a_wait(direction, i):
        by = 1 - 2 * direction
        part = a_part(shift(x, -by), (0, by, -by)[i])
        a_move(part, part, a_sem.at[direction, i], shift(x, by)).wait_recv()

    def relay_start(direction):
        by = 1 - 2 * direction
        origin = shift(x, -by)
        a_move(a_part(origin, 0), a_part(origin, -by), relay_sem.at[direction], shift(x, by)).start()

    def relay_wait(direction):
        by = 1 - 2 * direction
        part = a_part(shift(x, 2), -by)
        a_move(part, part, relay_sem.at[direction], shift(x, by)).wait_recv()

    last_starts = [sum(LAST[:c]) for c in range(len(LAST))]

    def last_start(direction, c):
        by = 1 - 2 * direction
        size = LAST[c] // 2
        start = last_starts[c] + direction * size
        origin = shift(x, -by)
        a_move(a_part(origin, by, start, size), a_part(origin, 0, start, size), last_sem.at[c], shift(x, by)).start()

    def last_wait(c):
        part = a_part(shift(x, 2), 0, last_starts[c], LAST[c])
        a_move(part, part, last_sem.at[c], shift(x, 1)).wait_recv()

    def place(h, first, second):
        return (shift(z, second), shift(y, first)) if h == 0 else (shift(z, first), shift(y, second))

    def r_ref(q, h, at, part, cc):
        if q == 0:
            size = piece // 2
            start = h * size
            ref = r_buf
            if part is not None:
                size = size // 2
                start = start + part * size
            return ref.at[piece_rows(at, cc, start, size), :]
        size, start = piece, h * k_all
        if part is not None:
            size = size // 2
            start = start + part * size
        return r2_buf.at[piece_rows(at, cc, start, size), :]

    def r_start(q, h, at, part, slot, to):
        ref = r_ref(q, h, at, part, core)
        recv = (r_sem if q == 0 else r2_sem).at[h, slot]
        remote(ref, ref, sem["r_send"] if q == 0 else sem["r2_send"], recv, device_of(to[0], to[1], core), x).start()

    def r_wait(q, h, at, slot):
        ref = r_ref(q, h, at, None, core)
        recv = (r_sem if q == 0 else r2_sem).at[h, slot]
        remote(ref, ref, sem["r_send"], recv, partner, x).wait_recv()

    def to_partner(q, h, at, late):
        ref = r_ref(q, h, at, None, core)
        recv = sem["p_recv"] if q == 0 else sem["p_recv%d%d" % (h, late)]
        remote(ref, ref, sem["p_send"] if q == 0 else sem["p2_send"], recv, partner, x).start()

    places = {0: 0, -1: 1, 1: 2, 2: 3}

    def slot_of(first, kind):
        return 3 + 3 * places[first] + kind

    def along_second(q, h, at, first):
        for direction in (0, 1):
            r_start(q, h, at, None, slot_of(first, direction), place(h, 0, 1 - 2 * direction))

    def r_own_first(q):
        for h in (0, 1):
            for direction in (0, 1):
                r_start(q, h, own, None, direction, place(h, 1 - 2 * direction, 0))

    def r_own_second(q):
        for h in (0, 1):
            along_second(q, h, own, 0)
            to_partner(q, h, own, 0)

    def r_first(q):
        for direction in (0, 1):
            by = 1 - 2 * direction
            for h in (0, 1):
                at = place(h, -by, 0)
                r_wait(q, h, at, direction)
                r_start(q, h, at, direction, 2, place(h, by, 0))
        for by in (1, -1):
            for h in (0, 1):
                at = place(h, -by, 0)
                along_second(q, h, at, -by)
                to_partner(q, h, at, 0)

    def r_opposite(q, h):
        at = place(h, 2, 0)
        r_wait(q, h, at, 2)
        along_second(q, h, at, 2)
        to_partner(q, h, at, 0)

    def r_second(q, first, direction, h):
        by = 1 - 2 * direction
        at = place(h, first, -by)
        r_wait(q, h, at, slot_of(first, direction))
        r_start(q, h, at, direction, slot_of(first, 2), place(h, 0, by))
        to_partner(q, h, at, 0)

    def r_second_opposite(q, first, h):
        at = place(h, first, 2)
        r_wait(q, h, at, slot_of(first, 2))
        to_partner(q, h, at, 1)

    FIRSTS = (0, -1, 1, 2)

    def product(k, by, start, size, columns):
        return jnp.dot(
            a_buf[a_part(shift(x, k), by, start, size), :],
            r_buf[rows_at(shift(x, k) * depth, depth), columns],
            preferred_element_type=jnp.float32,
        )

    def unit(k, by, mode, start=0, size=None):
        size = quarter if size is None else size
        out_rows = rows_at(shift(x, by) * quarter + start, size, 32)

        def step(j, carry):
            columns = pl.ds(pl.multiple_of(j * TILE_N, TILE_N), TILE_N)
            value = product(k, by, start, size, columns)
            if mode != "set":
                value = value + c_buf[out_rows, columns]
            c_buf[out_rows, columns] = value
            if mode == "last":
                sq_sum[:, columns] += jnp.sum(value * value, axis=0, keepdims=True)
            return carry

        lax.fori_loop(0, cols // TILE_N, step, 0)

    delta = (x + 2 - z + SIDE) % SIDE
    low = 1 - delta // 2
    early_blocks = ((3 - delta) // 3, 1 + 2 * low)
    late_blocks = (delta * low + 3 * (1 - low), 2)

    def ext_dot_0(start, block):
        return jnp.dot(
            a_buf[a_part(block, -1, start, EXT_M), :],
            r2_buf[rows_at(block * depth, depth), :],
            preferred_element_type=jnp.float32,
        )

    def ext_dot_1(start, pairs):
        total = None
        for zz, yy in pairs:
            value = jnp.dot(
                a_buf[a_part(zz, 1, start, EXT_M), pl.ds(pl.multiple_of(yy * chip, 128), chip)],
                r2_buf[rows_at(k_all + (zz * SIDE + yy) * chip, chip), :],
                preferred_element_type=jnp.float32,
            )
            total = value if total is None else total + value
        return total

    def ext_unit(h, dot, what, mode):
        def step(i, carry):
            start = pl.multiple_of(i * EXT_M, EXT_M)
            part = pl.ds(start, EXT_M)
            value = dot(start, what)
            if mode != "set":
                value = value + ext[h, part, :]
            ext[h, part, :] = value
            if mode == "last":
                columns = pl.ds(h * side_cols, side_cols)
                sq_out[:, columns] += jnp.sum(value * value, axis=0, keepdims=True)
            return carry

        lax.fori_loop(0, quarter // EXT_M, step, 0)

    def ext_early(h):
        if h == 0:
            for i, k in enumerate(early_blocks):
                ext_unit(0, ext_dot_0, shift(z, k), "set" if i == 0 else "add")
        else:
            for i, k in enumerate((0, -1, 1)):
                pairs = [(shift(x, b), shift(y, k)) for b in (0, -1, 1)]
                ext_unit(1, ext_dot_1, pairs, "set" if i == 0 else "add")

    def ext_middle():
        ext_unit(0, ext_dot_0, shift(z, late_blocks[0]), "add")
        ext_unit(1, ext_dot_1, [(shift(x, 2), shift(y, k)) for k in (0, -1, 1)], "add")

    def ext_late(h):
        if h == 0:
            ext_unit(0, ext_dot_0, shift(z, late_blocks[1]), "last")
        else:
            ext_unit(1, ext_dot_1, [(zz, shift(y, 2)) for zz in range(SIDE)], "last")

    def ext_copy(h, start, stop):
        by = 1 - 2 * h
        dst = c_buf.at[rows_at(shift(x, -by) * quarter + start, stop - start), pl.ds(h * side_cols, side_cols)]
        src = ext.at[h, pl.ds(start, stop - start), :]
        return remote(src, dst, sem["e_send"], sem["e_recv"], g, shift(x, by))

    def rounded(h, count=1):
        return r2_buf.at[pl.ds(h * (quarter - WIDE), count * (quarter - WIDE)), :]

    def rounded_copy(h):
        by = 1 - 2 * h
        dst = result.at[rows_at(shift(x, -by) * quarter + WIDE, quarter - WIDE), pl.ds(h * side_cols, side_cols)]
        return remote(rounded(h), dst, sem["b_send"], sem["b_recv"], g, shift(x, 1 - 2 * h))

    def scale_copy(h):
        columns = pl.ds(h * side_cols, side_cols)
        return remote(
            scale.at[:, columns], scale_in.at[:, columns], sem["n_send"], sem["n_recv"], g, shift(x, 2 * h - 1)
        )

    def sq_ext_copy(h):
        columns = pl.ds(h * side_cols, side_cols)
        return remote(
            sq_out.at[:, columns], sq_in.at[:, columns], sem["q_send"], sem["q_recv"], g, shift(x, 1 - 2 * h)
        )

    own_rot.wait()
    for h in (0, 1):
        remote(
            r_buf.at[piece_rows(own, core), pl.ds(h * side_cols, side_cols)], r_ref(1, h, own, None, core),
            sem["x_send"], sem["x_recv"], g, shift(x, 2 * h - 1),
        ).start()
    r_own_first(0)
    loaded = a_buf.at[rows_at(x * 3 * quarter, 3 * quarter, 32), :]
    pltpu.make_async_copy(loaded, loaded, load_sem.at[0]).wait()
    for i in range(3):
        for direction in (0, 1):
            a_start(direction, i)
    r_own_second(0)
    sq_sum[...] = jnp.zeros_like(sq_sum)
    sq_out[...] = jnp.zeros_like(sq_out)
    r_first(0)
    for h in (0, 1):
        r_opposite(0, h)
    for first in FIRSTS:
        for direction in (0, 1):
            for h in (0, 1):
                r_second(0, first, direction, h)
    two = r2_buf.at[pl.ds(0, 2 * piece), :]
    remote(two, two, sem["x_send"], sem["x_recv"], g, shift(x, 1)).wait()
    r_own_first(1)
    r_own_second(1)
    for direction in (0, 1):
        a_wait(direction, 0)
        relay_start(direction)
    for first in FIRSTS:
        for h in (0, 1):
            r_second_opposite(0, first, h)
    for direction in (0, 1):
        a_wait(direction, 1)
        for c in range(len(LAST)):
            last_start(direction, c)
    pieces = SIDE * SIDE * piece
    ref = r_buf.at[pl.ds(0, pieces), :]
    remote(ref, ref, sem["p_send"], sem["p_recv"], partner, x).wait()

    unit(0, 0, "set")
    unit(0, 1, "set")
    r_first(1)
    unit(0, -1, "set")
    for k in (-1, 1):
        unit(k, 0, "add")
    r_opposite(1, 0)
    for k in (-1, 1):
        unit(k, -k, "add")
    r_opposite(1, 1)
    for first in FIRSTS:
        for direction in (0, 1):
            for h in (0, 1):
                r_second(1, first, direction, h)
        if first == 0:
            for direction, k in enumerate((-1, 1)):
                a_wait(direction, 2)
                unit(k, k, "add")
    early = r2_buf.at[pl.ds(0, 12 * piece), :]
    for h in (0, 1):
        remote(early, early, sem["p2_send"], sem["p_recv%d0" % h], partner, x).wait_recv()
        ext_early(h)
    for direction, by in enumerate((-1, 1)):
        relay_wait(direction)
        unit(2, by, "last")
        for first in FIRSTS[2 * direction:2 * direction + 2]:
            for h in (0, 1):
                r_second_opposite(1, first, h)
    ext_middle()
    late = r2_buf.at[pl.ds(0, 4 * piece), :]
    for h in (0, 1):
        remote(late, late, sem["p2_send"], sem["p_recv%d1" % h], partner, x).wait_recv()
        ext_late(h)
        sq_ext_copy(h).start()
        ext_copy(h, 0, FIRST_WIDE).start()
    for c in range(len(LAST)):
        last_wait(c)
        unit(2, 0, "last", last_starts[c], LAST[c])
    remote(sq_out, sq_in, sem["q_send"], sem["q_recv"], g, shift(x, 1)).wait()

    sq_buf[g] = sq_sum[...] + sq_in[...]
    others = [(dz, dy, dc) for dz in range(-1, 3) for dy in range(-1, 3) for dc in (0, 1) if (dz, dy, dc) != (0, 0, 0)]
    for dz, dy, dc in sorted(others, key=lambda by: -(abs(by[0]) + abs(by[1]))):
        peer = device_of(shift(z, dz), shift(y, dy), (core + dc) % 2)
        remote(sq_buf.at[g], sq_buf.at[g], sem["s_send"], sem["s_recv"], peer, x).start()
    ref = a_buf.at[pl.ds(0, 9 * quarter), :]
    remote(ref, ref, sem["a_send"], sem["e_recv"], g, shift(x, 1)).wait_send()
    ref = r_buf.at[pl.ds(0, 15 * piece), :]
    remote(ref, ref, sem["r_send"], sem["e_recv"], partner, x).wait_send()
    ref = r2_buf.at[pl.ds(0, 30 * piece), :]
    remote(ref, ref, sem["r2_send"], sem["e_recv"], partner, x).wait_send()
    ref = r2_buf.at[pl.ds(0, 32 * piece), :]
    remote(ref, ref, sem["p2_send"], sem["e_recv"], partner, x).wait_send()
    ref = sq_buf.at[pl.ds(0, peers - 1)]
    remote(ref, ref, sem["s_send"], sem["s_recv"], partner, x).wait()
    total = sq_buf[0]
    for i in range(1, peers):
        total = total + sq_buf[i]
    rms = jnp.sqrt(total / TOTAL_ROWS + 1e-06)
    rms_out[...] = rms
    scale[...] = 1.0 / rms
    for h in (0, 1):
        scale_copy(h).start()
    for h in (0, 1):
        ext_copy(h, FIRST_WIDE, WIDE).start()
    remote(scale, scale_in, sem["n_send"], sem["n_recv"], g, shift(x, 1)).wait()
    for h in (0, 1):
        rounded(h)[...] = (ext[h, WIDE:, :] * scale_in[:, h * side_cols:(h + 1) * side_cols]).astype(jnp.bfloat16)
        rounded_copy(h).start()
    ref = ext.at[:, pl.ds(0, WIDE), :]
    remote(ref, ref, sem["e_send"], sem["e_recv"], g, shift(x, 1)).wait()

    def normalize(part):
        result[part, :] = (c_buf[part, :] * scale[...]).astype(jnp.bfloat16)

    normalize(rows_at(shift(x, 2) * quarter, WIDE))
    for by in (-1, 0, 1):
        normalize(rows_at(shift(x, by) * quarter, quarter))
    remote(rounded(0, 2), rounded(0, 2), sem["b_send"], sem["b_recv"], g, shift(x, 1)).wait()


def put(result, rms_in, out, rms_out, rms, out_sem):
    rows = result.shape[0]
    copies = []
    for i in range(4):
        part = pl.ds(i * rows // 4, rows // 4)
        copies.append(pltpu.make_async_copy(result.at[part, :], out.at[part, :], out_sem.at[i]))
        copies[-1].start()
    rms[...] = rms_in[...].reshape(rms.shape)
    copies.append(pltpu.make_async_copy(rms, rms_out, out_sem.at[4]))
    copies[-1].start()
    for copy in copies:
        copy.wait()


def body(coefficients, rotation):
    rows, depth = coefficients.shape
    piece, cols = rotation.shape
    peers = lax.axis_size("ga")
    dma = pltpu.SemaphoreType.DMA
    row = pltpu.VMEM((1, cols), jnp.float32)
    parts = pl.pallas_call(
        gather_multiply,
        out_shape=(pltpu.VMEM((rows, cols), jnp.bfloat16), row),
        in_specs=[pl.BlockSpec(memory_space=pl.ANY)] * 2,
        out_specs=(pl.BlockSpec(memory_space=pltpu.VMEM),) * 2,
        scratch_shapes=[
            pltpu.VMEM((rows, cols), jnp.float32),
            row,
            pltpu.VMEM((3 * rows, depth), jnp.bfloat16),
            pltpu.VMEM((SIDE * depth, cols), jnp.bfloat16),
            pltpu.VMEM((2 * SIDE * depth, cols // 2), jnp.bfloat16),
            pltpu.VMEM((2, rows // SIDE, cols // 2), jnp.float32),
            pltpu.VMEM((peers, 1, cols), jnp.float32),
            row,
            row,
            row,
            row,
            dma((2,)),
            dma((2, 3)),
            dma((2,)),
            dma((len(LAST),)),
            dma((2, 15)),
            dma((2, 15)),
            dma((len(SEMS),)),
        ],
        compiler_params=pltpu.CompilerParams(
            collective_id=0, has_side_effects=True, vmem_limit_bytes=60 * 1024 * 1024
        ),
        cost_estimate=pl.CostEstimate(
            flops=2 * rows * depth * SIDE * cols, bytes_accessed=4 * rows * depth, transcendentals=0
        ),
    )(coefficients, rotation)
    return pl.pallas_call(
        put,
        out_shape=(
            jax.ShapeDtypeStruct((rows, cols), jnp.bfloat16),
            jax.ShapeDtypeStruct((cols,), jnp.float32),
        ),
        in_specs=[pl.BlockSpec(memory_space=pltpu.VMEM)] * 2,
        out_specs=(pl.BlockSpec(memory_space=pl.ANY),) * 2,
        scratch_shapes=[
            pltpu.VMEM((cols,), jnp.float32),
            dma((5,)),
        ],
        compiler_params=pltpu.CompilerParams(vmem_limit_bytes=4 * 1024 * 1024),
        cost_estimate=pl.CostEstimate(flops=rows * cols, bytes_accessed=6 * rows * cols, transcendentals=0),
    )(*parts)


def solution(mesh):
    return jax.shard_map(
        body, mesh=mesh, in_specs=(P("ga", "ba"), P("ga", "ba")), out_specs=(P("ga", "ba"), P("ba")), check_vma=False
    )
```

```python
import jax
import jax.numpy as jnp
from jax import lax
from jax.experimental import pallas as pl
from jax.experimental.pallas import tpu as pltpu
from jax.sharding import PartitionSpec as P

MESH = pl.DeviceIdType.MESH
SIDE = 4
LAST = (192, 128)
FIRST_WIDE, WIDE = 144, 176
TILE_N = 768
EXT_M = 160
TOTAL_ROWS = 40960
SENDS = ("a_send", "r_send", "r2_send", "p_send", "p2_send", "x_send", "e_send", "q_send", "s_send", "n_send", "b_send")
ARRIVALS = ("x_recv", "e_recv", "q_recv", "s_recv", "n_recv", "b_recv", "p_recv", "p_recv00", "p_recv01", "p_recv10", "p_recv11")
SEMS = {name: i for i, name in enumerate(SENDS + ARRIVALS)}


def gather_multiply(
    coef, rot, result, rms_out, c_buf, scale, a_buf, r_buf, r2_buf, ext, sq_buf, sq_sum, sq_out, sq_in, scale_in,
    load_sem, a_sem, relay_sem, last_sem, r_sem, r2_sem, sems,
):
    rows, depth = coef.shape
    piece, cols = rot.shape
    peers = 2 * SIDE * SIDE
    quarter = rows // SIDE
    side_cols = cols // 2
    k_all = peers * piece
    chip = 2 * piece

    g = lax.axis_index("ga")
    x = lax.axis_index("ba")
    core = g % 2
    y = (g // 2) % SIDE
    z = g // (2 * SIDE)
    sem = {name: sems.at[i] for name, i in SEMS.items()}

    def shift(value, by):
        return (value + by + SIDE) % SIDE

    def device_of(zz, yy, cc):
        return (zz * SIDE + yy) * 2 + cc

    partner = device_of(z, y, 1 - core)

    def rows_at(start, size, align=16):
        return pl.ds(pl.multiple_of(start, align), size)

    def a_part(block, by, start=0, size=None):
        at = (block * 3 + by + 1) * quarter + start
        return rows_at(at, quarter if size is None else size, 32)

    def piece_rows(at, cc, start=0, size=None):
        return rows_at(device_of(at[0], at[1], cc) * piece + start, piece if size is None else size)

    own = (z, y)

    own_rot = pltpu.make_async_copy(rot, r_buf.at[piece_rows(own, core), :], load_sem.at[1])
    own_rot.start()

    def own_part(by):
        return coef.at[rows_at(shift(x, by) * quarter, quarter, 32), :]

    for by in (-1, 0, 1):
        pltpu.make_async_copy(own_part(by), a_buf.at[a_part(x, by), :], load_sem.at[0]).start()

    barrier = pltpu.get_barrier_semaphore()
    near = [(device_of(shift(z, by), y, core), x) for by in (1, -1)]
    near += [(device_of(z, shift(y, by), core), x) for by in (1, -1)]
    near += [(g, shift(x, by)) for by in (1, -1)]
    near += [(partner, x)]
    for ga, ba in near:
        pl.semaphore_signal(barrier, inc=1, device_id={"ga": ga, "ba": ba}, device_id_type=MESH)
    pl.semaphore_wait(barrier, len(near))

    def remote(src, dst, send, recv, ga, ba):
        return pltpu.make_async_remote_copy(
            src_ref=src, dst_ref=dst, send_sem=send, recv_sem=recv,
            device_id={"ga": ga, "ba": ba}, device_id_type=MESH,
        )

    def a_move(src, dst, recv, to):
        src = src if isinstance(src, tuple) else (a_buf.at[src, :],)
        return remote(src[0], a_buf.at[dst, :], sem["a_send"], recv, g, to)

    def a_start(direction, i):
        by = 1 - 2 * direction
        src = (a_part(x, by), (own_part(2),), a_part(x, 0))[i]
        a_move(src, a_part(x, (0, by, -by)[i]), a_sem.at[direction, i], shift(x, by)).start()

    def a_wait(direction, i):
        by = 1 - 2 * direction
        part = a_part(shift(x, -by), (0, by, -by)[i])
        a_move(part, part, a_sem.at[direction, i], shift(x, by)).wait_recv()

    def relay_start(direction):
        by = 1 - 2 * direction
        origin = shift(x, -by)
        a_move(a_part(origin, 0), a_part(origin, -by), relay_sem.at[direction], shift(x, by)).start()

    def relay_wait(direction):
        by = 1 - 2 * direction
        part = a_part(shift(x, 2), -by)
        a_move(part, part, relay_sem.at[direction], shift(x, by)).wait_recv()

    last_starts = [sum(LAST[:c]) for c in range(len(LAST))]

    def last_start(direction, c):
        by = 1 - 2 * direction
        size = LAST[c] // 2
        start = last_starts[c] + direction * size
        origin = shift(x, -by)
        a_move(a_part(origin, by, start, size), a_part(origin, 0, start, size), last_sem.at[c], shift(x, by)).start()

    def last_wait(c):
        part = a_part(shift(x, 2), 0, last_starts[c], LAST[c])
        a_move(part, part, last_sem.at[c], shift(x, 1)).wait_recv()

    def place(h, first, second):
        return (shift(z, second), shift(y, first)) if h == 0 else (shift(z, first), shift(y, second))

    def r_ref(q, h, at, part, cc):
        if q == 0:
            size = piece // 2
            start = h * size
            ref = r_buf
            if part is not None:
                size = size // 2
                start = start + part * size
            return ref.at[piece_rows(at, cc, start, size), :]
        size, start = piece, h * k_all
        if part is not None:
            size = size // 2
            start = start + part * size
        return r2_buf.at[piece_rows(at, cc, start, size), :]

    def r_start(q, h, at, part, slot, to):
        ref = r_ref(q, h, at, part, core)
        recv = (r_sem if q == 0 else r2_sem).at[h, slot]
        remote(ref, ref, sem["r_send"] if q == 0 else sem["r2_send"], recv, device_of(to[0], to[1], core), x).start()

    def r_wait(q, h, at, slot):
        ref = r_ref(q, h, at, None, core)
        recv = (r_sem if q == 0 else r2_sem).at[h, slot]
        remote(ref, ref, sem["r_send"], recv, partner, x).wait_recv()

    def to_partner(q, h, at, late):
        ref = r_ref(q, h, at, None, core)
        recv = sem["p_recv"] if q == 0 else sem["p_recv%d%d" % (h, late)]
        remote(ref, ref, sem["p_send"] if q == 0 else sem["p2_send"], recv, partner, x).start()

    places = {0: 0, -1: 1, 1: 2, 2: 3}

    def slot_of(first, kind):
        return 3 + 3 * places[first] + kind

    def along_second(q, h, at, first):
        for direction in (0, 1):
            r_start(q, h, at, None, slot_of(first, direction), place(h, 0, 1 - 2 * direction))

    def r_own_first(q):
        for h in (0, 1):
            for direction in (0, 1):
                r_start(q, h, own, None, direction, place(h, 1 - 2 * direction, 0))

    def r_own_second(q):
        for h in (0, 1):
            along_second(q, h, own, 0)
            to_partner(q, h, own, 0)

    def r_first(q):
        for direction in (0, 1):
            by = 1 - 2 * direction
            for h in (0, 1):
                at = place(h, -by, 0)
                r_wait(q, h, at, direction)
                r_start(q, h, at, direction, 2, place(h, by, 0))
        for by in (1, -1):
            for h in (0, 1):
                at = place(h, -by, 0)
                along_second(q, h, at, -by)
                to_partner(q, h, at, 0)

    def r_opposite(q, h):
        at = place(h, 2, 0)
        r_wait(q, h, at, 2)
        along_second(q, h, at, 2)
        to_partner(q, h, at, 0)

    def r_second(q, first, direction, h):
        by = 1 - 2 * direction
        at = place(h, first, -by)
        r_wait(q, h, at, slot_of(first, direction))
        r_start(q, h, at, direction, slot_of(first, 2), place(h, 0, by))
        to_partner(q, h, at, 0)

    def r_second_opposite(q, first, h):
        at = place(h, first, 2)
        r_wait(q, h, at, slot_of(first, 2))
        to_partner(q, h, at, 1)

    FIRSTS = (0, -1, 1, 2)

    def product(k, by, start, size, columns):
        return jnp.dot(
            a_buf[a_part(shift(x, k), by, start, size), :],
            r_buf[rows_at(shift(x, k) * depth, depth), columns],
            preferred_element_type=jnp.float32,
        )

    def unit(k, by, mode, start=0, size=None):
        size = quarter if size is None else size
        out_rows = rows_at(shift(x, by) * quarter + start, size, 32)

        tile = cols if mode == "last" else TILE_N

        def step(j, carry):
            columns = pl.ds(pl.multiple_of(j * tile, tile), tile)
            value = product(k, by, start, size, columns)
            if mode != "set":
                value = value + c_buf[out_rows, columns]
            c_buf[out_rows, columns] = value
            if mode == "last":
                sq_sum[:, columns] += jnp.sum(value * value, axis=0, keepdims=True)
            return carry

        lax.fori_loop(0, cols // tile, step, 0)

    delta = (x + 2 - z + SIDE) % SIDE
    low = 1 - delta // 2
    early_blocks = ((3 - delta) // 3, 1 + 2 * low)
    late_blocks = (delta * low + 3 * (1 - low), 2)

    def ext_dot_0(start, block):
        return jnp.dot(
            a_buf[a_part(block, -1, start, EXT_M), :],
            r2_buf[rows_at(block * depth, depth), :],
            preferred_element_type=jnp.float32,
        )

    def ext_dot_1(start, pairs):
        total = None
        for zz, yy in pairs:
            value = jnp.dot(
                a_buf[a_part(zz, 1, start, EXT_M), pl.ds(pl.multiple_of(yy * chip, 128), chip)],
                r2_buf[rows_at(k_all + (zz * SIDE + yy) * chip, chip), :],
                preferred_element_type=jnp.float32,
            )
            total = value if total is None else total + value
        return total

    def ext_unit(h, dot, what, mode):
        def step(i, carry):
            start = pl.multiple_of(i * EXT_M, EXT_M)
            part = pl.ds(start, EXT_M)
            value = dot(start, what)
            if mode != "set":
                value = value + ext[h, part, :]
            ext[h, part, :] = value
            if mode == "last":
                columns = pl.ds(h * side_cols, side_cols)
                sq_out[:, columns] += jnp.sum(value * value, axis=0, keepdims=True)
            return carry

        lax.fori_loop(0, quarter // EXT_M, step, 0)

    def ext_early(h):
        if h == 0:
            for i, k in enumerate(early_blocks):
                ext_unit(0, ext_dot_0, shift(z, k), "set" if i == 0 else "add")
        else:
            for i, k in enumerate((0, -1, 1)):
                pairs = [(shift(x, b), shift(y, k)) for b in (0, -1, 1)]
                ext_unit(1, ext_dot_1, pairs, "set" if i == 0 else "add")

    def ext_middle():
        ext_unit(0, ext_dot_0, shift(z, late_blocks[0]), "add")
        ext_unit(1, ext_dot_1, [(shift(x, 2), shift(y, k)) for k in (0, -1, 1)], "add")

    def ext_late(h):
        if h == 0:
            ext_unit(0, ext_dot_0, shift(z, late_blocks[1]), "last")
        else:
            ext_unit(1, ext_dot_1, [(zz, shift(y, 2)) for zz in range(SIDE)], "last")

    def ext_copy(h, start, stop):
        by = 1 - 2 * h
        dst = c_buf.at[rows_at(shift(x, -by) * quarter + start, stop - start), pl.ds(h * side_cols, side_cols)]
        src = ext.at[h, pl.ds(start, stop - start), :]
        return remote(src, dst, sem["e_send"], sem["e_recv"], g, shift(x, by))

    def rounded(h, count=1):
        return r2_buf.at[pl.ds(h * (quarter - WIDE), count * (quarter - WIDE)), :]

    def rounded_copy(h):
        by = 1 - 2 * h
        dst = result.at[rows_at(shift(x, -by) * quarter + WIDE, quarter - WIDE), pl.ds(h * side_cols, side_cols)]
        return remote(rounded(h), dst, sem["b_send"], sem["b_recv"], g, shift(x, 1 - 2 * h))

    def scale_copy(h):
        columns = pl.ds(h * side_cols, side_cols)
        return remote(
            scale.at[:, columns], scale_in.at[:, columns], sem["n_send"], sem["n_recv"], g, shift(x, 2 * h - 1)
        )

    def sq_ext_copy(h):
        columns = pl.ds(h * side_cols, side_cols)
        return remote(
            sq_out.at[:, columns], sq_in.at[:, columns], sem["q_send"], sem["q_recv"], g, shift(x, 1 - 2 * h)
        )

    own_rot.wait()
    for h in (0, 1):
        remote(
            r_buf.at[piece_rows(own, core), pl.ds(h * side_cols, side_cols)], r_ref(1, h, own, None, core),
            sem["x_send"], sem["x_recv"], g, shift(x, 2 * h - 1),
        ).start()
    r_own_first(0)
    loaded = a_buf.at[rows_at(x * 3 * quarter, 3 * quarter, 32), :]
    pltpu.make_async_copy(loaded, loaded, load_sem.at[0]).wait()
    for i in range(3):
        for direction in (0, 1):
            a_start(direction, i)
    r_own_second(0)
    sq_sum[...] = jnp.zeros_like(sq_sum)
    sq_out[...] = jnp.zeros_like(sq_out)
    r_first(0)
    for h in (0, 1):
        r_opposite(0, h)
    for first in FIRSTS:
        for direction in (0, 1):
            for h in (0, 1):
                r_second(0, first, direction, h)
    two = r2_buf.at[pl.ds(0, 2 * piece), :]
    remote(two, two, sem["x_send"], sem["x_recv"], g, shift(x, 1)).wait()
    r_own_first(1)
    r_own_second(1)
    for direction in (0, 1):
        a_wait(direction, 0)
        relay_start(direction)
    for first in FIRSTS:
        for h in (0, 1):
            r_second_opposite(0, first, h)
    for direction in (0, 1):
        a_wait(direction, 1)
        for c in range(len(LAST)):
            last_start(direction, c)
    pieces = SIDE * SIDE * piece
    ref = r_buf.at[pl.ds(0, pieces), :]
    remote(ref, ref, sem["p_send"], sem["p_recv"], partner, x).wait()

    unit(0, 0, "set")
    unit(0, 1, "set")
    r_first(1)
    unit(0, -1, "set")
    for k in (-1, 1):
        unit(k, 0, "add")
    r_opposite(1, 0)
    for k in (-1, 1):
        unit(k, -k, "add")
    r_opposite(1, 1)
    for first in FIRSTS:
        for direction in (0, 1):
            for h in (0, 1):
                r_second(1, first, direction, h)
        if first == 0:
            for direction, k in enumerate((-1, 1)):
                a_wait(direction, 2)
                unit(k, k, "add")
    early = r2_buf.at[pl.ds(0, 12 * piece), :]
    for h in (0, 1):
        remote(early, early, sem["p2_send"], sem["p_recv%d0" % h], partner, x).wait_recv()
        ext_early(h)
    for direction, by in enumerate((-1, 1)):
        relay_wait(direction)
        unit(2, by, "last")
        for first in FIRSTS[2 * direction:2 * direction + 2]:
            for h in (0, 1):
                r_second_opposite(1, first, h)
    ext_middle()
    late = r2_buf.at[pl.ds(0, 4 * piece), :]
    for h in (0, 1):
        remote(late, late, sem["p2_send"], sem["p_recv%d1" % h], partner, x).wait_recv()
        ext_late(h)
        sq_ext_copy(h).start()
        ext_copy(h, 0, FIRST_WIDE).start()
    for c in range(len(LAST)):
        last_wait(c)
        unit(2, 0, "last", last_starts[c], LAST[c])
    remote(sq_out, sq_in, sem["q_send"], sem["q_recv"], g, shift(x, 1)).wait()

    sq_buf[g] = sq_sum[...] + sq_in[...]
    others = [(dz, dy, dc) for dz in range(-1, 3) for dy in range(-1, 3) for dc in (0, 1) if (dz, dy, dc) != (0, 0, 0)]
    for dz, dy, dc in sorted(others, key=lambda by: -(abs(by[0]) + abs(by[1]))):
        peer = device_of(shift(z, dz), shift(y, dy), (core + dc) % 2)
        remote(sq_buf.at[g], sq_buf.at[g], sem["s_send"], sem["s_recv"], peer, x).start()
    ref = a_buf.at[pl.ds(0, 9 * quarter), :]
    remote(ref, ref, sem["a_send"], sem["e_recv"], g, shift(x, 1)).wait_send()
    ref = r_buf.at[pl.ds(0, 15 * piece), :]
    remote(ref, ref, sem["r_send"], sem["e_recv"], partner, x).wait_send()
    ref = r2_buf.at[pl.ds(0, 30 * piece), :]
    remote(ref, ref, sem["r2_send"], sem["e_recv"], partner, x).wait_send()
    ref = r2_buf.at[pl.ds(0, 32 * piece), :]
    remote(ref, ref, sem["p2_send"], sem["e_recv"], partner, x).wait_send()
    ref = sq_buf.at[pl.ds(0, peers - 1)]
    remote(ref, ref, sem["s_send"], sem["s_recv"], partner, x).wait()
    total = sq_buf[0]
    for i in range(1, peers):
        total = total + sq_buf[i]
    rms = jnp.sqrt(total / TOTAL_ROWS + 1e-06)
    rms_out[...] = rms
    scale[...] = 1.0 / rms
    for h in (0, 1):
        scale_copy(h).start()
    for h in (0, 1):
        ext_copy(h, FIRST_WIDE, WIDE).start()
    remote(scale, scale_in, sem["n_send"], sem["n_recv"], g, shift(x, 1)).wait()
    for h in (0, 1):
        rounded(h)[...] = (ext[h, WIDE:, :] * scale_in[:, h * side_cols:(h + 1) * side_cols]).astype(jnp.bfloat16)
        rounded_copy(h).start()
    ref = ext.at[:, pl.ds(0, WIDE), :]
    remote(ref, ref, sem["e_send"], sem["e_recv"], g, shift(x, 1)).wait()

    def normalize(part):
        result[part, :] = (c_buf[part, :] * scale[...]).astype(jnp.bfloat16)

    normalize(rows_at(shift(x, 2) * quarter, WIDE))
    for by in (-1, 0, 1):
        normalize(rows_at(shift(x, by) * quarter, quarter))
    remote(rounded(0, 2), rounded(0, 2), sem["b_send"], sem["b_recv"], g, shift(x, 1)).wait()


def put(result, rms_in, out, rms_out, rms, out_sem):
    rows = result.shape[0]
    copies = []
    for i in range(4):
        part = pl.ds(i * rows // 4, rows // 4)
        copies.append(pltpu.make_async_copy(result.at[part, :], out.at[part, :], out_sem.at[i]))
        copies[-1].start()
    rms[...] = rms_in[...].reshape(rms.shape)
    copies.append(pltpu.make_async_copy(rms, rms_out, out_sem.at[4]))
    copies[-1].start()
    for copy in copies:
        copy.wait()


def body(coefficients, rotation):
    rows, depth = coefficients.shape
    piece, cols = rotation.shape
    peers = lax.axis_size("ga")
    dma = pltpu.SemaphoreType.DMA
    row = pltpu.VMEM((1, cols), jnp.float32)
    parts = pl.pallas_call(
        gather_multiply,
        out_shape=(pltpu.VMEM((rows, cols), jnp.bfloat16), row),
        in_specs=[pl.BlockSpec(memory_space=pl.ANY)] * 2,
        out_specs=(pl.BlockSpec(memory_space=pltpu.VMEM),) * 2,
        scratch_shapes=[
            pltpu.VMEM((rows, cols), jnp.float32),
            row,
            pltpu.VMEM((3 * rows, depth), jnp.bfloat16),
            pltpu.VMEM((SIDE * depth, cols), jnp.bfloat16),
            pltpu.VMEM((2 * SIDE * depth, cols // 2), jnp.bfloat16),
            pltpu.VMEM((2, rows // SIDE, cols // 2), jnp.float32),
            pltpu.VMEM((peers, 1, cols), jnp.float32),
            row,
            row,
            row,
            row,
            dma((2,)),
            dma((2, 3)),
            dma((2,)),
            dma((len(LAST),)),
            dma((2, 15)),
            dma((2, 15)),
            dma((len(SEMS),)),
        ],
        compiler_params=pltpu.CompilerParams(
            collective_id=0, has_side_effects=True, vmem_limit_bytes=60 * 1024 * 1024
        ),
        cost_estimate=pl.CostEstimate(
            flops=2 * rows * depth * SIDE * cols, bytes_accessed=4 * rows * depth, transcendentals=0
        ),
    )(coefficients, rotation)
    return pl.pallas_call(
        put,
        out_shape=(
            jax.ShapeDtypeStruct((rows, cols), jnp.bfloat16),
            jax.ShapeDtypeStruct((cols,), jnp.float32),
        ),
        in_specs=[pl.BlockSpec(memory_space=pltpu.VMEM)] * 2,
        out_specs=(pl.BlockSpec(memory_space=pl.ANY),) * 2,
        scratch_shapes=[
            pltpu.VMEM((cols,), jnp.float32),
            dma((5,)),
        ],
        compiler_params=pltpu.CompilerParams(vmem_limit_bytes=4 * 1024 * 1024),
        cost_estimate=pl.CostEstimate(flops=rows * cols, bytes_accessed=6 * rows * cols, transcendentals=0),
    )(*parts)


def solution(mesh):
    return jax.shard_map(
        body, mesh=mesh, in_specs=(P("ga", "ba"), P("ga", "ba")), out_specs=(P("ga", "ba"), P("ba")), check_vma=False
    )
```

```python
import jax
import jax.numpy as jnp
from jax import lax
from jax.experimental import pallas as pl
from jax.experimental.pallas import tpu as pltpu
from jax.sharding import PartitionSpec as P

MESH = pl.DeviceIdType.MESH
SIDE = 4
LAST = (192, 128)
FIRST_WIDE, WIDE = 144, 176
TILE_N = 768
EXT_M = 160
TOTAL_ROWS = 40960
SENDS = ("a_send", "r_send", "r2_send", "p_send", "p2_send", "x_send", "e_send", "q_send", "s_send", "n_send", "b_send")
ARRIVALS = ("x_recv", "e_recv", "q_recv", "s_recv", "n_recv", "b_recv", "p_recv", "p_recv00", "p_recv01", "p_recv10", "p_recv11")
SEMS = {name: i for i, name in enumerate(SENDS + ARRIVALS)}


def gather_multiply(
    coef, rot, result, rms_out, c_buf, scale, a_buf, r_buf, r2_buf, ext, sq_buf, sq_sum, sq_out, sq_in, scale_in,
    load_sem, a_sem, relay_sem, last_sem, r_sem, r2_sem, sems,
):
    rows, depth = coef.shape
    piece, cols = rot.shape
    peers = 2 * SIDE * SIDE
    quarter = rows // SIDE
    side_cols = cols // 2
    k_all = peers * piece
    chip = 2 * piece

    g = lax.axis_index("ga")
    x = lax.axis_index("ba")
    core = g % 2
    y = (g // 2) % SIDE
    z = g // (2 * SIDE)
    sem = {name: sems.at[i] for name, i in SEMS.items()}

    def shift(value, by):
        return (value + by + SIDE) % SIDE

    def device_of(zz, yy, cc):
        return (zz * SIDE + yy) * 2 + cc

    partner = device_of(z, y, 1 - core)

    def rows_at(start, size, align=16):
        return pl.ds(pl.multiple_of(start, align), size)

    def a_part(block, by, start=0, size=None):
        at = (block * 3 + by + 1) * quarter + start
        return rows_at(at, quarter if size is None else size, 32)

    def piece_rows(at, cc, start=0, size=None):
        return rows_at(device_of(at[0], at[1], cc) * piece + start, piece if size is None else size)

    own = (z, y)

    own_rot = pltpu.make_async_copy(rot, r_buf.at[piece_rows(own, core), :], load_sem.at[1])
    own_rot.start()

    def own_part(by):
        return coef.at[rows_at(shift(x, by) * quarter, quarter, 32), :]

    for by in (-1, 0, 1):
        pltpu.make_async_copy(own_part(by), a_buf.at[a_part(x, by), :], load_sem.at[0]).start()

    barrier = pltpu.get_barrier_semaphore()
    near = [(device_of(shift(z, by), y, core), x) for by in (1, -1)]
    near += [(device_of(z, shift(y, by), core), x) for by in (1, -1)]
    near += [(g, shift(x, by)) for by in (1, -1)]
    near += [(partner, x)]
    for ga, ba in near:
        pl.semaphore_signal(barrier, inc=1, device_id={"ga": ga, "ba": ba}, device_id_type=MESH)
    pl.semaphore_wait(barrier, len(near))

    def remote(src, dst, send, recv, ga, ba):
        return pltpu.make_async_remote_copy(
            src_ref=src, dst_ref=dst, send_sem=send, recv_sem=recv,
            device_id={"ga": ga, "ba": ba}, device_id_type=MESH,
        )

    def a_move(src, dst, recv, to):
        src = src if isinstance(src, tuple) else (a_buf.at[src, :],)
        return remote(src[0], a_buf.at[dst, :], sem["a_send"], recv, g, to)

    def a_start(direction, i):
        by = 1 - 2 * direction
        src = (a_part(x, by), (own_part(2),), a_part(x, 0))[i]
        a_move(src, a_part(x, (0, by, -by)[i]), a_sem.at[direction, i], shift(x, by)).start()

    def a_wait(direction, i):
        by = 1 - 2 * direction
        part = a_part(shift(x, -by), (0, by, -by)[i])
        a_move(part, part, a_sem.at[direction, i], shift(x, by)).wait_recv()

    def relay_start(direction):
        by = 1 - 2 * direction
        origin = shift(x, -by)
        a_move(a_part(origin, 0), a_part(origin, -by), relay_sem.at[direction], shift(x, by)).start()

    def relay_wait(direction):
        by = 1 - 2 * direction
        part = a_part(shift(x, 2), -by)
        a_move(part, part, relay_sem.at[direction], shift(x, by)).wait_recv()

    last_starts = [sum(LAST[:c]) for c in range(len(LAST))]

    def last_start(direction, c):
        by = 1 - 2 * direction
        size = LAST[c] // 2
        start = last_starts[c] + direction * size
        origin = shift(x, -by)
        a_move(a_part(origin, by, start, size), a_part(origin, 0, start, size), last_sem.at[c], shift(x, by)).start()

    def last_wait(c):
        part = a_part(shift(x, 2), 0, last_starts[c], LAST[c])
        a_move(part, part, last_sem.at[c], shift(x, 1)).wait_recv()

    def place(h, first, second):
        return (shift(z, second), shift(y, first)) if h == 0 else (shift(z, first), shift(y, second))

    def r_ref(q, h, at, part, cc):
        if q == 0:
            size = piece // 2
            start = h * size
            ref = r_buf
            if part is not None:
                size = size // 2
                start = start + part * size
            return ref.at[piece_rows(at, cc, start, size), :]
        size, start = piece, h * k_all
        if part is not None:
            size = size // 2
            start = start + part * size
        return r2_buf.at[piece_rows(at, cc, start, size), :]

    def r_start(q, h, at, part, slot, to):
        ref = r_ref(q, h, at, part, core)
        recv = (r_sem if q == 0 else r2_sem).at[h, slot]
        remote(ref, ref, sem["r_send"] if q == 0 else sem["r2_send"], recv, device_of(to[0], to[1], core), x).start()

    def r_wait(q, h, slot, count):
        if q == 0:
            ref, recv = r_buf.at[pl.ds(0, count * (piece // 2)), :], r_sem.at[h, slot]
        else:
            ref, recv = r2_buf.at[pl.ds(0, count * piece), :], r2_sem.at[h, slot]
        remote(ref, ref, sem["r_send"], recv, partner, x).wait_recv()

    def to_partner(q, h, at, late):
        ref = r_ref(q, h, at, None, core)
        recv = sem["p_recv"] if q == 0 else sem["p_recv%d%d" % (h, late)]
        remote(ref, ref, sem["p_send"] if q == 0 else sem["p2_send"], recv, partner, x).start()

    places = {0: 0, -1: 1, 1: 2, 2: 3}

    def slot_of(first, opposite):
        return 2 + 4 * opposite + places[first]

    def along_second(q, h, at, first):
        for direction in (0, 1):
            r_start(q, h, at, None, slot_of(first, 0), place(h, 0, 1 - 2 * direction))

    def r_own_first(q):
        for h in (0, 1):
            for direction in (0, 1):
                r_start(q, h, own, None, 0, place(h, 1 - 2 * direction, 0))

    def r_own_second(q):
        for h in (0, 1):
            along_second(q, h, own, 0)
            to_partner(q, h, own, 0)

    def r_first(q):
        for h in (0, 1):
            r_wait(q, h, 0, 2)
            for direction, by in ((0, 1), (1, -1)):
                r_start(q, h, place(h, -by, 0), direction, 1, place(h, by, 0))
        for by in (1, -1):
            for h in (0, 1):
                at = place(h, -by, 0)
                along_second(q, h, at, -by)
                to_partner(q, h, at, 0)

    def r_opposite(q, h):
        at = place(h, 2, 0)
        r_wait(q, h, 1, 1)
        along_second(q, h, at, 2)
        to_partner(q, h, at, 0)

    def r_second(q, first, h):
        r_wait(q, h, slot_of(first, 0), 2)
        for direction, by in ((0, 1), (1, -1)):
            at = place(h, first, -by)
            r_start(q, h, at, direction, slot_of(first, 1), place(h, 0, by))
            to_partner(q, h, at, 0)

    def r_second_opposite(q, first, h):
        at = place(h, first, 2)
        r_wait(q, h, slot_of(first, 1), 1)
        to_partner(q, h, at, 1)

    FIRSTS = (0, -1, 1, 2)

    def product(k, by, start, size, columns):
        return jnp.dot(
            a_buf[a_part(shift(x, k), by, start, size), :],
            r_buf[rows_at(shift(x, k) * depth, depth), columns],
            preferred_element_type=jnp.float32,
        )

    def unit(k, by, mode, start=0, size=None):
        size = quarter if size is None else size
        out_rows = rows_at(shift(x, by) * quarter + start, size, 32)

        tile = cols if mode == "last" else TILE_N

        def step(j, carry):
            columns = pl.ds(pl.multiple_of(j * tile, tile), tile)
            value = product(k, by, start, size, columns)
            if mode != "set":
                value = value + c_buf[out_rows, columns]
            c_buf[out_rows, columns] = value
            if mode == "last":
                sq_sum[:, columns] += jnp.sum(value * value, axis=0, keepdims=True)
            return carry

        lax.fori_loop(0, cols // tile, step, 0)

    delta = (x + 2 - z + SIDE) % SIDE
    low = 1 - delta // 2
    early_blocks = ((3 - delta) // 3, 1 + 2 * low)
    late_blocks = (delta * low + 3 * (1 - low), 2)

    def ext_dot_0(start, block):
        return jnp.dot(
            a_buf[a_part(block, -1, start, EXT_M), :],
            r2_buf[rows_at(block * depth, depth), :],
            preferred_element_type=jnp.float32,
        )

    def ext_dot_1(start, pairs):
        total = None
        for zz, yy in pairs:
            value = jnp.dot(
                a_buf[a_part(zz, 1, start, EXT_M), pl.ds(pl.multiple_of(yy * chip, 128), chip)],
                r2_buf[rows_at(k_all + (zz * SIDE + yy) * chip, chip), :],
                preferred_element_type=jnp.float32,
            )
            total = value if total is None else total + value
        return total

    def ext_unit(h, dot, what, mode):
        def step(i, carry):
            start = pl.multiple_of(i * EXT_M, EXT_M)
            part = pl.ds(start, EXT_M)
            value = dot(start, what)
            if mode != "set":
                value = value + ext[h, part, :]
            ext[h, part, :] = value
            if mode == "last":
                columns = pl.ds(h * side_cols, side_cols)
                sq_out[:, columns] += jnp.sum(value * value, axis=0, keepdims=True)
            return carry

        lax.fori_loop(0, quarter // EXT_M, step, 0)

    def ext_early(h):
        if h == 0:
            for i, k in enumerate(early_blocks):
                ext_unit(0, ext_dot_0, shift(z, k), "set" if i == 0 else "add")
        else:
            for i, k in enumerate((0, -1, 1)):
                pairs = [(shift(x, b), shift(y, k)) for b in (0, -1, 1)]
                ext_unit(1, ext_dot_1, pairs, "set" if i == 0 else "add")

    def ext_middle():
        ext_unit(0, ext_dot_0, shift(z, late_blocks[0]), "add")
        ext_unit(1, ext_dot_1, [(shift(x, 2), shift(y, k)) for k in (0, -1, 1)], "add")

    def ext_late(h):
        if h == 0:
            ext_unit(0, ext_dot_0, shift(z, late_blocks[1]), "last")
        else:
            ext_unit(1, ext_dot_1, [(zz, shift(y, 2)) for zz in range(SIDE)], "last")

    def ext_copy(h, start, stop):
        by = 1 - 2 * h
        dst = c_buf.at[rows_at(shift(x, -by) * quarter + start, stop - start), pl.ds(h * side_cols, side_cols)]
        src = ext.at[h, pl.ds(start, stop - start), :]
        return remote(src, dst, sem["e_send"], sem["e_recv"], g, shift(x, by))

    def rounded(h, count=1):
        return r2_buf.at[pl.ds(h * (quarter - WIDE), count * (quarter - WIDE)), :]

    def rounded_copy(h):
        by = 1 - 2 * h
        dst = result.at[rows_at(shift(x, -by) * quarter + WIDE, quarter - WIDE), pl.ds(h * side_cols, side_cols)]
        return remote(rounded(h), dst, sem["b_send"], sem["b_recv"], g, shift(x, 1 - 2 * h))

    def scale_copy(h):
        columns = pl.ds(h * side_cols, side_cols)
        return remote(
            scale.at[:, columns], scale_in.at[:, columns], sem["n_send"], sem["n_recv"], g, shift(x, 2 * h - 1)
        )

    def sq_ext_copy(h):
        columns = pl.ds(h * side_cols, side_cols)
        return remote(
            sq_out.at[:, columns], sq_in.at[:, columns], sem["q_send"], sem["q_recv"], g, shift(x, 1 - 2 * h)
        )

    own_rot.wait()
    for h in (0, 1):
        remote(
            r_buf.at[piece_rows(own, core), pl.ds(h * side_cols, side_cols)], r_ref(1, h, own, None, core),
            sem["x_send"], sem["x_recv"], g, shift(x, 2 * h - 1),
        ).start()
    r_own_first(0)
    loaded = a_buf.at[rows_at(x * 3 * quarter, 3 * quarter, 32), :]
    pltpu.make_async_copy(loaded, loaded, load_sem.at[0]).wait()
    for i in range(3):
        for direction in (0, 1):
            a_start(direction, i)
    r_own_second(0)
    sq_sum[...] = jnp.zeros_like(sq_sum)
    sq_out[...] = jnp.zeros_like(sq_out)
    r_first(0)
    for h in (0, 1):
        r_opposite(0, h)
    for first in FIRSTS:
        for h in (0, 1):
            r_second(0, first, h)
    two = r2_buf.at[pl.ds(0, 2 * piece), :]
    remote(two, two, sem["x_send"], sem["x_recv"], g, shift(x, 1)).wait()
    r_own_first(1)
    r_own_second(1)
    for direction in (0, 1):
        a_wait(direction, 0)
        relay_start(direction)
    for first in FIRSTS:
        for h in (0, 1):
            r_second_opposite(0, first, h)
    for direction in (0, 1):
        a_wait(direction, 1)
        for c in range(len(LAST)):
            last_start(direction, c)
    pieces = SIDE * SIDE * piece
    ref = r_buf.at[pl.ds(0, pieces), :]
    remote(ref, ref, sem["p_send"], sem["p_recv"], partner, x).wait()

    unit(0, 0, "set")
    unit(0, 1, "set")
    r_first(1)
    unit(0, -1, "set")
    for k in (-1, 1):
        unit(k, 0, "add")
    r_opposite(1, 0)
    for k in (-1, 1):
        unit(k, -k, "add")
    r_opposite(1, 1)
    for first in FIRSTS:
        for h in (0, 1):
            r_second(1, first, h)
        if first == 0:
            for direction, k in enumerate((-1, 1)):
                a_wait(direction, 2)
                unit(k, k, "add")
    early = r2_buf.at[pl.ds(0, 12 * piece), :]
    for h in (0, 1):
        remote(early, early, sem["p2_send"], sem["p_recv%d0" % h], partner, x).wait_recv()
        ext_early(h)
    for direction, by in enumerate((-1, 1)):
        relay_wait(direction)
        unit(2, by, "last")
        for first in FIRSTS[2 * direction:2 * direction + 2]:
            for h in (0, 1):
                r_second_opposite(1, first, h)
    ext_middle()
    late = r2_buf.at[pl.ds(0, 4 * piece), :]
    for h in (0, 1):
        remote(late, late, sem["p2_send"], sem["p_recv%d1" % h], partner, x).wait_recv()
        ext_late(h)
        sq_ext_copy(h).start()
        ext_copy(h, 0, FIRST_WIDE).start()
    for c in range(len(LAST)):
        last_wait(c)
        unit(2, 0, "last", last_starts[c], LAST[c])
    remote(sq_out, sq_in, sem["q_send"], sem["q_recv"], g, shift(x, 1)).wait()

    sq_buf[g] = sq_sum[...] + sq_in[...]
    others = [(dz, dy, dc) for dz in range(-1, 3) for dy in range(-1, 3) for dc in (0, 1) if (dz, dy, dc) != (0, 0, 0)]
    for dz, dy, dc in sorted(others, key=lambda by: -(abs(by[0]) + abs(by[1]))):
        peer = device_of(shift(z, dz), shift(y, dy), (core + dc) % 2)
        remote(sq_buf.at[g], sq_buf.at[g], sem["s_send"], sem["s_recv"], peer, x).start()
    ref = a_buf.at[pl.ds(0, 9 * quarter), :]
    remote(ref, ref, sem["a_send"], sem["e_recv"], g, shift(x, 1)).wait_send()
    ref = r_buf.at[pl.ds(0, 15 * piece), :]
    remote(ref, ref, sem["r_send"], sem["e_recv"], partner, x).wait_send()
    ref = r2_buf.at[pl.ds(0, 30 * piece), :]
    remote(ref, ref, sem["r2_send"], sem["e_recv"], partner, x).wait_send()
    ref = r2_buf.at[pl.ds(0, 32 * piece), :]
    remote(ref, ref, sem["p2_send"], sem["e_recv"], partner, x).wait_send()
    ref = sq_buf.at[pl.ds(0, peers - 1)]
    remote(ref, ref, sem["s_send"], sem["s_recv"], partner, x).wait()
    total = sq_buf[0]
    for i in range(1, peers):
        total = total + sq_buf[i]
    rms = jnp.sqrt(total / TOTAL_ROWS + 1e-06)
    rms_out[...] = rms
    scale[...] = 1.0 / rms
    for h in (0, 1):
        scale_copy(h).start()
    for h in (0, 1):
        ext_copy(h, FIRST_WIDE, WIDE).start()
    remote(scale, scale_in, sem["n_send"], sem["n_recv"], g, shift(x, 1)).wait()
    for h in (0, 1):
        rounded(h)[...] = (ext[h, WIDE:, :] * scale_in[:, h * side_cols:(h + 1) * side_cols]).astype(jnp.bfloat16)
        rounded_copy(h).start()
    ref = ext.at[:, pl.ds(0, WIDE), :]
    remote(ref, ref, sem["e_send"], sem["e_recv"], g, shift(x, 1)).wait()

    def normalize(part):
        result[part, :] = (c_buf[part, :] * scale[...]).astype(jnp.bfloat16)

    normalize(rows_at(shift(x, 2) * quarter, WIDE))
    for by in (-1, 0, 1):
        normalize(rows_at(shift(x, by) * quarter, quarter))
    remote(rounded(0, 2), rounded(0, 2), sem["b_send"], sem["b_recv"], g, shift(x, 1)).wait()


def put(result, rms_in, out, rms_out, rms, out_sem):
    rows = result.shape[0]
    copies = []
    for i in range(4):
        part = pl.ds(i * rows // 4, rows // 4)
        copies.append(pltpu.make_async_copy(result.at[part, :], out.at[part, :], out_sem.at[i]))
        copies[-1].start()
    rms[...] = rms_in[...].reshape(rms.shape)
    copies.append(pltpu.make_async_copy(rms, rms_out, out_sem.at[4]))
    copies[-1].start()
    for copy in copies:
        copy.wait()


def body(coefficients, rotation):
    rows, depth = coefficients.shape
    piece, cols = rotation.shape
    peers = lax.axis_size("ga")
    dma = pltpu.SemaphoreType.DMA
    row = pltpu.VMEM((1, cols), jnp.float32)
    parts = pl.pallas_call(
        gather_multiply,
        out_shape=(pltpu.VMEM((rows, cols), jnp.bfloat16), row),
        in_specs=[pl.BlockSpec(memory_space=pl.ANY)] * 2,
        out_specs=(pl.BlockSpec(memory_space=pltpu.VMEM),) * 2,
        scratch_shapes=[
            pltpu.VMEM((rows, cols), jnp.float32),
            row,
            pltpu.VMEM((3 * rows, depth), jnp.bfloat16),
            pltpu.VMEM((SIDE * depth, cols), jnp.bfloat16),
            pltpu.VMEM((2 * SIDE * depth, cols // 2), jnp.bfloat16),
            pltpu.VMEM((2, rows // SIDE, cols // 2), jnp.float32),
            pltpu.VMEM((peers, 1, cols), jnp.float32),
            row,
            row,
            row,
            row,
            dma((2,)),
            dma((2, 3)),
            dma((2,)),
            dma((len(LAST),)),
            dma((2, 10)),
            dma((2, 10)),
            dma((len(SEMS),)),
        ],
        compiler_params=pltpu.CompilerParams(
            collective_id=0, has_side_effects=True, vmem_limit_bytes=60 * 1024 * 1024
        ),
        cost_estimate=pl.CostEstimate(
            flops=2 * rows * depth * SIDE * cols, bytes_accessed=4 * rows * depth, transcendentals=0
        ),
    )(coefficients, rotation)
    return pl.pallas_call(
        put,
        out_shape=(
            jax.ShapeDtypeStruct((rows, cols), jnp.bfloat16),
            jax.ShapeDtypeStruct((cols,), jnp.float32),
        ),
        in_specs=[pl.BlockSpec(memory_space=pltpu.VMEM)] * 2,
        out_specs=(pl.BlockSpec(memory_space=pl.ANY),) * 2,
        scratch_shapes=[
            pltpu.VMEM((cols,), jnp.float32),
            dma((5,)),
        ],
        compiler_params=pltpu.CompilerParams(vmem_limit_bytes=4 * 1024 * 1024),
        cost_estimate=pl.CostEstimate(flops=rows * cols, bytes_accessed=6 * rows * cols, transcendentals=0),
    )(*parts)


def solution(mesh):
    return jax.shard_map(
        body, mesh=mesh, in_specs=(P("ga", "ba"), P("ga", "ba")), out_specs=(P("ga", "ba"), P("ba")), check_vma=False
    )
```

```python
import jax
import jax.numpy as jnp
from jax import lax
from jax.experimental import pallas as pl
from jax.experimental.pallas import tpu as pltpu
from jax.sharding import PartitionSpec as P

MESH = pl.DeviceIdType.MESH
SIDE = 4
LAST = (192, 128)
FIRST_WIDE, WIDE = 144, 176
EXT_M = 160
TOTAL_ROWS = 40960
SENDS = ("a_send", "r_send", "r2_send", "p_send", "p2_send", "x_send", "e_send", "q_send", "s_send", "n_send", "b_send")
ARRIVALS = ("x_recv", "e_recv", "q_recv", "s_recv", "n_recv", "b_recv", "p_recv", "p_recv00", "p_recv01", "p_recv10", "p_recv11")
SEMS = {name: i for i, name in enumerate(SENDS + ARRIVALS)}


def gather_multiply(
    coef, rot, result, rms_out, c_buf, scale, a_buf, r_buf, r2_buf, ext, sq_buf, sq_sum, sq_out, sq_in, scale_in,
    load_sem, a_sem, relay_sem, last_sem, r_sem, r2_sem, sems,
):
    rows, depth = coef.shape
    piece, cols = rot.shape
    peers = 2 * SIDE * SIDE
    quarter = rows // SIDE
    side_cols = cols // 2
    k_all = peers * piece
    chip = 2 * piece

    g = lax.axis_index("ga")
    x = lax.axis_index("ba")
    core = g % 2
    y = (g // 2) % SIDE
    z = g // (2 * SIDE)
    sem = {name: sems.at[i] for name, i in SEMS.items()}

    def shift(value, by):
        return (value + by + SIDE) % SIDE

    def device_of(zz, yy, cc):
        return (zz * SIDE + yy) * 2 + cc

    partner = device_of(z, y, 1 - core)

    def rows_at(start, size, align=16):
        return pl.ds(pl.multiple_of(start, align), size)

    def a_part(block, by, start=0, size=None):
        at = (block * 3 + by + 1) * quarter + start
        return rows_at(at, quarter if size is None else size, 32)

    def piece_rows(at, cc, start=0, size=None):
        return rows_at(device_of(at[0], at[1], cc) * piece + start, piece if size is None else size)

    own = (z, y)

    own_rot = pltpu.make_async_copy(rot, r_buf.at[piece_rows(own, core), :], load_sem.at[1])
    own_rot.start()

    def own_part(by):
        return coef.at[rows_at(shift(x, by) * quarter, quarter, 32), :]

    for by in (-1, 0, 1):
        pltpu.make_async_copy(own_part(by), a_buf.at[a_part(x, by), :], load_sem.at[0]).start()

    barrier = pltpu.get_barrier_semaphore()
    near = [(device_of(shift(z, by), y, core), x) for by in (1, -1)]
    near += [(device_of(z, shift(y, by), core), x) for by in (1, -1)]
    near += [(g, shift(x, by)) for by in (1, -1)]
    near += [(partner, x)]
    for ga, ba in near:
        pl.semaphore_signal(barrier, inc=1, device_id={"ga": ga, "ba": ba}, device_id_type=MESH)
    pl.semaphore_wait(barrier, len(near))

    def remote(src, dst, send, recv, ga, ba):
        return pltpu.make_async_remote_copy(
            src_ref=src, dst_ref=dst, send_sem=send, recv_sem=recv,
            device_id={"ga": ga, "ba": ba}, device_id_type=MESH,
        )

    def a_move(src, dst, recv, to):
        src = src if isinstance(src, tuple) else (a_buf.at[src, :],)
        return remote(src[0], a_buf.at[dst, :], sem["a_send"], recv, g, to)

    def a_start(direction, i):
        by = 1 - 2 * direction
        src = (a_part(x, by), (own_part(2),), a_part(x, 0))[i]
        a_move(src, a_part(x, (0, by, -by)[i]), a_sem.at[direction, i], shift(x, by)).start()

    def a_wait(direction, i):
        by = 1 - 2 * direction
        part = a_part(shift(x, -by), (0, by, -by)[i])
        a_move(part, part, a_sem.at[direction, i], shift(x, by)).wait_recv()

    def relay_start(direction):
        by = 1 - 2 * direction
        origin = shift(x, -by)
        a_move(a_part(origin, 0), a_part(origin, -by), relay_sem.at[direction], shift(x, by)).start()

    def relay_wait(direction):
        by = 1 - 2 * direction
        part = a_part(shift(x, 2), -by)
        a_move(part, part, relay_sem.at[direction], shift(x, by)).wait_recv()

    last_starts = [sum(LAST[:c]) for c in range(len(LAST))]

    def last_start(direction, c):
        by = 1 - 2 * direction
        size = LAST[c] // 2
        start = last_starts[c] + direction * size
        origin = shift(x, -by)
        a_move(a_part(origin, by, start, size), a_part(origin, 0, start, size), last_sem.at[c], shift(x, by)).start()

    def last_wait(c):
        part = a_part(shift(x, 2), 0, last_starts[c], LAST[c])
        a_move(part, part, last_sem.at[c], shift(x, 1)).wait_recv()

    def place(h, first, second):
        return (shift(z, second), shift(y, first)) if h == 0 else (shift(z, first), shift(y, second))

    def r_ref(q, h, at, part, cc):
        if q == 0:
            size = piece // 2
            start = h * size
            ref = r_buf
            if part is not None:
                size = size // 2
                start = start + part * size
            return ref.at[piece_rows(at, cc, start, size), :]
        size, start = piece, h * k_all
        if part is not None:
            size = size // 2
            start = start + part * size
        return r2_buf.at[piece_rows(at, cc, start, size), :]

    def r_start(q, h, at, part, slot, to):
        ref = r_ref(q, h, at, part, core)
        recv = (r_sem if q == 0 else r2_sem).at[h, slot]
        remote(ref, ref, sem["r_send"] if q == 0 else sem["r2_send"], recv, device_of(to[0], to[1], core), x).start()

    def r_wait(q, h, slot, count):
        if q == 0:
            ref, recv = r_buf.at[pl.ds(0, count * (piece // 2)), :], r_sem.at[h, slot]
        else:
            ref, recv = r2_buf.at[pl.ds(0, count * piece), :], r2_sem.at[h, slot]
        remote(ref, ref, sem["r_send"], recv, partner, x).wait_recv()

    def to_partner(q, h, at, late):
        ref = r_ref(q, h, at, None, core)
        recv = sem["p_recv"] if q == 0 else sem["p_recv%d%d" % (h, late)]
        remote(ref, ref, sem["p_send"] if q == 0 else sem["p2_send"], recv, partner, x).start()

    places = {0: 0, -1: 1, 1: 2, 2: 3}

    def slot_of(first, opposite):
        return 2 + 4 * opposite + places[first]

    def along_second(q, h, at, first):
        for direction in (0, 1):
            r_start(q, h, at, None, slot_of(first, 0), place(h, 0, 1 - 2 * direction))

    def r_own_first(q):
        for h in (0, 1):
            for direction in (0, 1):
                r_start(q, h, own, None, 0, place(h, 1 - 2 * direction, 0))

    def r_own_second(q):
        for h in (0, 1):
            along_second(q, h, own, 0)
            to_partner(q, h, own, 0)

    def r_first(q):
        for h in (0, 1):
            r_wait(q, h, 0, 2)
            for direction, by in ((0, 1), (1, -1)):
                r_start(q, h, place(h, -by, 0), direction, 1, place(h, by, 0))
        for by in (1, -1):
            for h in (0, 1):
                at = place(h, -by, 0)
                along_second(q, h, at, -by)
                to_partner(q, h, at, 0)

    def r_opposite(q, h):
        at = place(h, 2, 0)
        r_wait(q, h, 1, 1)
        along_second(q, h, at, 2)
        to_partner(q, h, at, 0)

    def r_second(q, first, h):
        r_wait(q, h, slot_of(first, 0), 2)
        for direction, by in ((0, 1), (1, -1)):
            at = place(h, first, -by)
            r_start(q, h, at, direction, slot_of(first, 1), place(h, 0, by))
            to_partner(q, h, at, 0)

    def r_second_opposite(q, first, h):
        at = place(h, first, 2)
        r_wait(q, h, slot_of(first, 1), 1)
        to_partner(q, h, at, 1)

    FIRSTS = (0, -1, 1, 2)

    def product(k, by, start, size, columns):
        return jnp.dot(
            a_buf[a_part(shift(x, k), by, start, size), :],
            r_buf[rows_at(shift(x, k) * depth, depth), columns],
            preferred_element_type=jnp.float32,
        )

    def unit(k, by, mode, start=0, size=None):
        size = quarter if size is None else size
        out_rows = rows_at(shift(x, by) * quarter + start, size, 32)

        tile = cols

        def step(j, carry):
            columns = pl.ds(pl.multiple_of(j * tile, tile), tile)
            value = product(k, by, start, size, columns)
            if mode != "set":
                value = value + c_buf[out_rows, columns]
            c_buf[out_rows, columns] = value
            if mode == "last":
                sq_sum[:, columns] += jnp.sum(value * value, axis=0, keepdims=True)
            return carry

        lax.fori_loop(0, cols // tile, step, 0)

    delta = (x + 2 - z + SIDE) % SIDE
    low = 1 - delta // 2
    early_blocks = ((3 - delta) // 3, 1 + 2 * low)
    late_blocks = (delta * low + 3 * (1 - low), 2)

    def ext_dot_0(start, block):
        return jnp.dot(
            a_buf[a_part(block, -1, start, EXT_M), :],
            r2_buf[rows_at(block * depth, depth), :],
            preferred_element_type=jnp.float32,
        )

    def ext_dot_1(start, pairs):
        total = None
        for zz, yy in pairs:
            value = jnp.dot(
                a_buf[a_part(zz, 1, start, EXT_M), pl.ds(pl.multiple_of(yy * chip, 128), chip)],
                r2_buf[rows_at(k_all + (zz * SIDE + yy) * chip, chip), :],
                preferred_element_type=jnp.float32,
            )
            total = value if total is None else total + value
        return total

    def ext_unit(h, dot, what, mode):
        def step(i, carry):
            start = pl.multiple_of(i * EXT_M, EXT_M)
            part = pl.ds(start, EXT_M)
            value = dot(start, what)
            if mode != "set":
                value = value + ext[h, part, :]
            ext[h, part, :] = value
            if mode == "last":
                columns = pl.ds(h * side_cols, side_cols)
                sq_out[:, columns] += jnp.sum(value * value, axis=0, keepdims=True)
            return carry

        lax.fori_loop(0, quarter // EXT_M, step, 0)

    def ext_early(h):
        if h == 0:
            for i, k in enumerate(early_blocks):
                ext_unit(0, ext_dot_0, shift(z, k), "set" if i == 0 else "add")
        else:
            for i, k in enumerate((0, -1, 1)):
                pairs = [(shift(x, b), shift(y, k)) for b in (0, -1, 1)]
                ext_unit(1, ext_dot_1, pairs, "set" if i == 0 else "add")

    def ext_middle():
        ext_unit(0, ext_dot_0, shift(z, late_blocks[0]), "add")
        ext_unit(1, ext_dot_1, [(shift(x, 2), shift(y, k)) for k in (0, -1, 1)], "add")

    def ext_late(h):
        if h == 0:
            ext_unit(0, ext_dot_0, shift(z, late_blocks[1]), "last")
        else:
            ext_unit(1, ext_dot_1, [(zz, shift(y, 2)) for zz in range(SIDE)], "last")

    def ext_copy(h, start, stop):
        by = 1 - 2 * h
        dst = c_buf.at[rows_at(shift(x, -by) * quarter + start, stop - start), pl.ds(h * side_cols, side_cols)]
        src = ext.at[h, pl.ds(start, stop - start), :]
        return remote(src, dst, sem["e_send"], sem["e_recv"], g, shift(x, by))

    def rounded(h, count=1):
        return r2_buf.at[pl.ds(h * (quarter - WIDE), count * (quarter - WIDE)), :]

    def rounded_copy(h):
        by = 1 - 2 * h
        dst = result.at[rows_at(shift(x, -by) * quarter + WIDE, quarter - WIDE), pl.ds(h * side_cols, side_cols)]
        return remote(rounded(h), dst, sem["b_send"], sem["b_recv"], g, shift(x, 1 - 2 * h))

    def scale_copy(h):
        columns = pl.ds(h * side_cols, side_cols)
        return remote(
            scale.at[:, columns], scale_in.at[:, columns], sem["n_send"], sem["n_recv"], g, shift(x, 2 * h - 1)
        )

    def sq_ext_copy(h):
        columns = pl.ds(h * side_cols, side_cols)
        return remote(
            sq_out.at[:, columns], sq_in.at[:, columns], sem["q_send"], sem["q_recv"], g, shift(x, 1 - 2 * h)
        )

    own_rot.wait()
    for h in (0, 1):
        remote(
            r_buf.at[piece_rows(own, core), pl.ds(h * side_cols, side_cols)], r_ref(1, h, own, None, core),
            sem["x_send"], sem["x_recv"], g, shift(x, 2 * h - 1),
        ).start()
    r_own_first(0)
    loaded = a_buf.at[rows_at(x * 3 * quarter, 3 * quarter, 32), :]
    pltpu.make_async_copy(loaded, loaded, load_sem.at[0]).wait()
    for i in range(3):
        for direction in (0, 1):
            a_start(direction, i)
    r_own_second(0)
    sq_sum[...] = jnp.zeros_like(sq_sum)
    sq_out[...] = jnp.zeros_like(sq_out)
    r_first(0)
    for h in (0, 1):
        r_opposite(0, h)
    for first in FIRSTS:
        for h in (0, 1):
            r_second(0, first, h)
    two = r2_buf.at[pl.ds(0, 2 * piece), :]
    remote(two, two, sem["x_send"], sem["x_recv"], g, shift(x, 1)).wait()
    r_own_first(1)
    r_own_second(1)
    for direction in (0, 1):
        a_wait(direction, 0)
        relay_start(direction)
    for first in FIRSTS:
        for h in (0, 1):
            r_second_opposite(0, first, h)
    for direction in (0, 1):
        a_wait(direction, 1)
        for c in range(len(LAST)):
            last_start(direction, c)
    pieces = SIDE * SIDE * piece
    ref = r_buf.at[pl.ds(0, pieces), :]
    remote(ref, ref, sem["p_send"], sem["p_recv"], partner, x).wait()

    unit(0, 0, "set")
    unit(0, 1, "set")
    r_first(1)
    unit(0, -1, "set")
    for k in (-1, 1):
        unit(k, 0, "add")
    r_opposite(1, 0)
    for k in (-1, 1):
        unit(k, -k, "add")
    r_opposite(1, 1)
    for first in FIRSTS:
        for h in (0, 1):
            r_second(1, first, h)
        if first == 0:
            for direction, k in enumerate((-1, 1)):
                a_wait(direction, 2)
                unit(k, k, "add")
    early = r2_buf.at[pl.ds(0, 12 * piece), :]
    for h in (0, 1):
        remote(early, early, sem["p2_send"], sem["p_recv%d0" % h], partner, x).wait_recv()
        ext_early(h)
    for direction, by in enumerate((-1, 1)):
        relay_wait(direction)
        unit(2, by, "last")
        for first in FIRSTS[2 * direction:2 * direction + 2]:
            for h in (0, 1):
                r_second_opposite(1, first, h)
    ext_middle()
    late = r2_buf.at[pl.ds(0, 4 * piece), :]
    for h in (0, 1):
        remote(late, late, sem["p2_send"], sem["p_recv%d1" % h], partner, x).wait_recv()
        ext_late(h)
        sq_ext_copy(h).start()
        ext_copy(h, 0, FIRST_WIDE).start()
    for c in range(len(LAST)):
        last_wait(c)
        unit(2, 0, "last", last_starts[c], LAST[c])
    remote(sq_out, sq_in, sem["q_send"], sem["q_recv"], g, shift(x, 1)).wait()

    sq_buf[g] = sq_sum[...] + sq_in[...]
    others = [(dz, dy, dc) for dz in range(-1, 3) for dy in range(-1, 3) for dc in (0, 1) if (dz, dy, dc) != (0, 0, 0)]
    for dz, dy, dc in sorted(others, key=lambda by: -(abs(by[0]) + abs(by[1]))):
        peer = device_of(shift(z, dz), shift(y, dy), (core + dc) % 2)
        remote(sq_buf.at[g], sq_buf.at[g], sem["s_send"], sem["s_recv"], peer, x).start()
    ref = a_buf.at[pl.ds(0, 9 * quarter), :]
    remote(ref, ref, sem["a_send"], sem["e_recv"], g, shift(x, 1)).wait_send()
    ref = r_buf.at[pl.ds(0, 15 * piece), :]
    remote(ref, ref, sem["r_send"], sem["e_recv"], partner, x).wait_send()
    ref = r2_buf.at[pl.ds(0, 30 * piece), :]
    remote(ref, ref, sem["r2_send"], sem["e_recv"], partner, x).wait_send()
    ref = r2_buf.at[pl.ds(0, 32 * piece), :]
    remote(ref, ref, sem["p2_send"], sem["e_recv"], partner, x).wait_send()
    ref = sq_buf.at[pl.ds(0, peers - 1)]
    remote(ref, ref, sem["s_send"], sem["s_recv"], partner, x).wait()
    total = sq_buf[0]
    for i in range(1, peers):
        total = total + sq_buf[i]
    rms = jnp.sqrt(total / TOTAL_ROWS + 1e-06)
    rms_out[...] = rms
    scale[...] = 1.0 / rms
    for h in (0, 1):
        scale_copy(h).start()
    for h in (0, 1):
        ext_copy(h, FIRST_WIDE, WIDE).start()
    remote(scale, scale_in, sem["n_send"], sem["n_recv"], g, shift(x, 1)).wait()
    for h in (0, 1):
        rounded(h)[...] = (ext[h, WIDE:, :] * scale_in[:, h * side_cols:(h + 1) * side_cols]).astype(jnp.bfloat16)
        rounded_copy(h).start()
    ref = ext.at[:, pl.ds(0, WIDE), :]
    remote(ref, ref, sem["e_send"], sem["e_recv"], g, shift(x, 1)).wait()

    def normalize(part):
        result[part, :] = (c_buf[part, :] * scale[...]).astype(jnp.bfloat16)

    normalize(rows_at(shift(x, 2) * quarter, WIDE))
    for by in (-1, 0, 1):
        normalize(rows_at(shift(x, by) * quarter, quarter))
    remote(rounded(0, 2), rounded(0, 2), sem["b_send"], sem["b_recv"], g, shift(x, 1)).wait()


def put(result, rms_in, out, rms_out, rms, out_sem):
    rows = result.shape[0]
    copies = []
    for i in range(4):
        part = pl.ds(i * rows // 4, rows // 4)
        copies.append(pltpu.make_async_copy(result.at[part, :], out.at[part, :], out_sem.at[i]))
        copies[-1].start()
    rms[...] = rms_in[...].reshape(rms.shape)
    copies.append(pltpu.make_async_copy(rms, rms_out, out_sem.at[4]))
    copies[-1].start()
    for copy in copies:
        copy.wait()


def body(coefficients, rotation):
    rows, depth = coefficients.shape
    piece, cols = rotation.shape
    peers = lax.axis_size("ga")
    dma = pltpu.SemaphoreType.DMA
    row = pltpu.VMEM((1, cols), jnp.float32)
    parts = pl.pallas_call(
        gather_multiply,
        out_shape=(pltpu.VMEM((rows, cols), jnp.bfloat16), row),
        in_specs=[pl.BlockSpec(memory_space=pl.ANY)] * 2,
        out_specs=(pl.BlockSpec(memory_space=pltpu.VMEM),) * 2,
        scratch_shapes=[
            pltpu.VMEM((rows, cols), jnp.float32),
            row,
            pltpu.VMEM((3 * rows, depth), jnp.bfloat16),
            pltpu.VMEM((SIDE * depth, cols), jnp.bfloat16),
            pltpu.VMEM((2 * SIDE * depth, cols // 2), jnp.bfloat16),
            pltpu.VMEM((2, rows // SIDE, cols // 2), jnp.float32),
            pltpu.VMEM((peers, 1, cols), jnp.float32),
            row,
            row,
            row,
            row,
            dma((2,)),
            dma((2, 3)),
            dma((2,)),
            dma((len(LAST),)),
            dma((2, 10)),
            dma((2, 10)),
            dma((len(SEMS),)),
        ],
        compiler_params=pltpu.CompilerParams(
            collective_id=0, has_side_effects=True, vmem_limit_bytes=60 * 1024 * 1024
        ),
        cost_estimate=pl.CostEstimate(
            flops=2 * rows * depth * SIDE * cols, bytes_accessed=4 * rows * depth, transcendentals=0
        ),
    )(coefficients, rotation)
    return pl.pallas_call(
        put,
        out_shape=(
            jax.ShapeDtypeStruct((rows, cols), jnp.bfloat16),
            jax.ShapeDtypeStruct((cols,), jnp.float32),
        ),
        in_specs=[pl.BlockSpec(memory_space=pltpu.VMEM)] * 2,
        out_specs=(pl.BlockSpec(memory_space=pl.ANY),) * 2,
        scratch_shapes=[
            pltpu.VMEM((cols,), jnp.float32),
            dma((5,)),
        ],
        compiler_params=pltpu.CompilerParams(vmem_limit_bytes=4 * 1024 * 1024),
        cost_estimate=pl.CostEstimate(flops=rows * cols, bytes_accessed=6 * rows * cols, transcendentals=0),
    )(*parts)


def solution(mesh):
    return jax.shard_map(
        body, mesh=mesh, in_specs=(P("ga", "ba"), P("ga", "ba")), out_specs=(P("ga", "ba"), P("ba")), check_vma=False
    )
```
